128 devices in a mesh: dom: 128 (over x, z, y, core).
Axes of the slice: x: 4, y: 4, z: 4, core: 2. Of those that a mesh axis runs over, the one named last changes fastest.
Arguments:
- features: bfloat16 [32768, 512], P('dom'), may hold values from -6 to 6
- w_one: bfloat16 [9, 512, 512], replicated, may hold values from -0.25 to 0.25
- w_two: bfloat16 [8, 512, 349], replicated, may hold values from -0.25 to 0.25
- self_two: bfloat16 [512, 349], replicated, may hold values from -80 to 80
- edge_src: int32 [8, 256, 256], P(None, 'dom'), may hold values from 0 to 1279, as said below
- edge_dst: int32 [8, 256, 256], P(None, 'dom'), may hold values from -1 to 127, as said below
- send_rows: int32 [128, 128, 8], P('dom'), may hold values from 0 to 255
- send_count: int32 [128, 128], P('dom'), may hold values from 1 to 8, as said below
- labels: int32 [32768], P('dom'), may hold values from -1 to 348
Outputs:
- logits: float32 [32768, 349], P('dom')
- loss: float32 [], replicated
- grad_one: float32 [4608, 512], P('dom')
- grad_two: float32 [4608, 349], P('dom')
The draws below stay inside these ranges and needn't reach their ends.
Inputs may be any that keep to these rules, and one draw needn't show every extreme that they name: `send_rows`: entry [p, q, s] is a row of partition p's own nodes, rows may repeat. `send_count`: entry [p, q] counts the live slots p sends to q; every row reaches 8 at some q. `edge_src`: index into the destination partition's table: its 256 own rows, then 8 slots from each partition in order. `edge_dst`: -1 marks an empty edge slot.
All inputs are finite; a program needn't handle non-finite values.
Results may differ from the reference program's by a relative error of at most 0.0085.
The reference program's roundings to bfloat16 on the way count: a program that leaves them out, or rounds other values in their place, can miss the bound.
Values may be sent and summed in bfloat16 or wider, within the bound.
A program may use at most 128 MiB of HBM per device.

```python
import jax
import jax.numpy as jnp
from jax import lax

D = 512
CLASSES = 349
RELATIONS = 8
NODES_DEV = 256
SLOTS = 8
EDGES_BLOCK = 256
NODES = 32768
N_DOM = 128


def slot_counts(key):
    base_key = jax.random.fold_in(key, 7)
    limits = jax.random.randint(jax.random.fold_in(base_key, 1), (N_DOM, 1), 1, SLOTS + 1)
    counts = jax.random.randint(jax.random.fold_in(base_key, 2), (N_DOM, N_DOM), 1, SLOTS + 1)
    counts = jnp.minimum(counts, limits)
    full_peer = jax.random.randint(jax.random.fold_in(base_key, 3), (N_DOM, 1), 0, N_DOM)
    peer_ids = jnp.arange(N_DOM, dtype=jnp.int32)[None, :]
    return jnp.where(peer_ids == full_peer, SLOTS, counts).astype(jnp.int32)


def edge_tables(key):
    counts = slot_counts(key)
    base_key = jax.random.fold_in(key, 11)
    blocks = NODES // 128
    edge_shape = (RELATIONS, blocks, EDGES_BLOCK)
    owner_dev = (jnp.arange(blocks, dtype=jnp.int32) // (NODES_DEV // 128))[None, :, None] * jnp.ones(edge_shape, jnp.int32)
    live_level = jax.random.randint(jax.random.fold_in(base_key, 1), (N_DOM,), 4, 11)
    live_edge = jax.random.randint(jax.random.fold_in(base_key, 2), edge_shape, 0, 10) < live_level[owner_dev]
    targets = jnp.where(live_edge, jax.random.randint(jax.random.fold_in(base_key, 3), edge_shape, 0, 128), -1)
    remote = jax.random.randint(jax.random.fold_in(base_key, 4), edge_shape, 0, 2) == 1
    peer_pick = jax.random.randint(jax.random.fold_in(base_key, 5), edge_shape, 0, N_DOM)
    slot_limit = counts[peer_pick, owner_dev]
    slot_pick = jax.random.randint(jax.random.fold_in(base_key, 6), edge_shape, 0, 1 << 20) % slot_limit
    remote_row = NODES_DEV + peer_pick * SLOTS + slot_pick
    local_row = jax.random.randint(jax.random.fold_in(base_key, 7), edge_shape, 0, NODES_DEV)
    sources = jnp.where(remote, remote_row, local_row)
    return (sources.astype(jnp.int32), targets.astype(jnp.int32))


def draw_send_count(key, part):
    return slot_counts(key)


def draw_edge_src(key, part):
    return edge_tables(key)[0]


def draw_edge_dst(key, part):
    return edge_tables(key)[1]


def draw_labels(key, part):
    base_key = jax.random.fold_in(key, 23)
    device_of = jnp.arange(NODES, dtype=jnp.int32) // NODES_DEV
    chance = jax.random.randint(jax.random.fold_in(base_key, 1), (NODES,), 0, 1000)
    labelled = chance < 250 + 500 * device_of // max(N_DOM - 1, 1)
    classes = jax.random.randint(jax.random.fold_in(base_key, 2), (NODES,), 0, CLASSES)
    return jnp.where(labelled, classes, -1).astype(jnp.int32)


def draw_self_two(key, part):
    base_key = jax.random.fold_in(key, 31)
    values = jax.random.normal(jax.random.fold_in(base_key, 1), (D, CLASSES), jnp.float32) * D ** (-0.5)
    return jnp.clip(values, -80.0, 80.0).astype(jnp.bfloat16)


def set_ends(drawn, own_key, least, top_value):
    spot = [jax.random.randint(jax.random.fold_in(own_key, axis), (), 0, length) for axis, length in enumerate(drawn.shape)]
    widest = drawn.shape.index(max(drawn.shape))
    neighbour = spot[:widest] + [(spot[widest] + 1) % drawn.shape[widest]] + spot[widest + 1:]
    return drawn.at[tuple(spot)].set(least).at[tuple(neighbour)].set(top_value)


def level_of(rng, shape, shards, least, high):
    def one(position, shards_of):
        heights = jax.random.uniform(jax.random.fold_in(jax.random.fold_in(rng, 6), position), (shards_of,), jnp.float32, least / len(shards), high / len(shards))
        return jnp.repeat(jnp.exp(heights), shape[position] // shards_of).reshape((-1,) + (1,) * (len(shape) - position - 1))

    level = one(*shards[0])
    for cut in shards[1:]:
        level = level * one(*cut)
    return level


def scatter_about(key, shape, scale, bound, cuts=(), kind=jnp.bfloat16):
    factor_of = level_of(key, shape, cuts, -0.22, 0.18) if cuts else 1.0
    array = jax.random.normal(key, shape, jnp.float32) * scale * factor_of
    return jnp.minimum(jnp.maximum(array, -bound), bound).astype(kind)


def setup_inputs(seed: int = 0) -> dict:
    keys = jax.random.split(jax.random.key(seed), 10)
    return {
        "features": scatter_about(keys[0], (NODES, D), 1.0, 6.0, ((0, 128),)),
        "w_one": scatter_about(keys[1], (RELATIONS + 1, D, D), D ** -0.5, 0.25),
        "w_two": scatter_about(keys[2], (RELATIONS, D, CLASSES), D ** -0.5, 0.25),
        "self_two": draw_self_two(jax.random.fold_in(keys[9], 71), 0),
        "edge_src": draw_edge_src(jax.random.fold_in(keys[9], 71), 0),
        "edge_dst": draw_edge_dst(jax.random.fold_in(keys[9], 71), 0),
        "send_rows": set_ends(jax.random.randint(keys[6], (N_DOM, N_DOM, SLOTS), 0, NODES_DEV), jax.random.fold_in(keys[6], 1), 0, NODES_DEV - 1).astype(jnp.int32),
        "send_count": draw_send_count(jax.random.fold_in(keys[9], 71), 0),
        "labels": draw_labels(jax.random.fold_in(keys[9], 71), 0),
    }


loss_scale = 256.0


def slot_rows(values, send_rows, send_count, device):
    picks = send_rows[:, device, :]
    owners = jnp.arange(N_DOM, dtype=jnp.int32)[:, None] * NODES_DEV + picks
    chosen = values[owners.reshape(-1)]
    live_slot = (jnp.arange(SLOTS, dtype=jnp.int32)[None, :] < send_count[:, device][:, None]).reshape(-1)
    return jnp.where(live_slot[:, None], chosen, jnp.zeros_like(chosen))


def device_edges(edge_src, edge_dst, device):
    blocks = NODES_DEV // 128
    start = (device * blocks).astype(jnp.int32)
    return (lax.dynamic_slice_in_dim(edge_src, start, blocks, 1), lax.dynamic_slice_in_dim(edge_dst, start, blocks, 1))


def edge_targets(targets):
    blocks = NODES_DEV // 128
    live_edge = targets >= 0
    node_of = jnp.arange(blocks, dtype=jnp.int32)[None, :, None] * 128 + jnp.where(live_edge, targets, 0)
    segment = jnp.arange(RELATIONS, dtype=jnp.int32)[:, None, None] * NODES_DEV + node_of
    return jnp.where(live_edge, segment, RELATIONS * NODES_DEV).reshape(-1).astype(jnp.int32)


def aggregate(node_table, sources, targets):
    segment = edge_targets(targets)
    slots_all = RELATIONS * NODES_DEV + 1
    gathered = node_table[sources.reshape(-1)].astype(jnp.float32)
    sums = jax.ops.segment_sum(gathered, segment, num_segments=slots_all)[:-1]
    counts = jax.ops.segment_sum(jnp.ones(segment.shape, jnp.float32), segment, num_segments=slots_all)[:-1]
    norm_rows = 1.0 / jnp.maximum(counts, 1.0)
    averaged = (sums * norm_rows[:, None]).astype(jnp.bfloat16)
    return averaged.reshape(RELATIONS, NODES_DEV, -1), norm_rows.reshape(RELATIONS, NODES_DEV)


def layer(device, values, weights, self_weight, send_rows, send_count, edge_src, edge_dst):
    own_rows = lax.dynamic_slice_in_dim(values, (device * NODES_DEV).astype(jnp.int32), NODES_DEV, 0)
    node_table = jnp.concatenate([own_rows, slot_rows(values, send_rows, send_count, device)], axis=0)
    sources, targets = device_edges(edge_src, edge_dst, device)
    averaged, norm_rows = aggregate(node_table, sources, targets)
    output = jnp.einsum('rnd,rde->ne', averaged.astype(jnp.float32), weights.astype(jnp.float32))
    output = output + jnp.dot(own_rows, self_weight, preferred_element_type=jnp.float32)
    return own_rows, averaged, norm_rows, sources, targets, output


def reference(features, w_one, w_two, self_two, edge_src, edge_dst, send_rows, send_count, labels):
    devices = jnp.arange(N_DOM, dtype=jnp.int32)

    def first(device):
        return layer(device, features, w_one[:RELATIONS], w_one[RELATIONS], send_rows, send_count, edge_src, edge_dst)

    def second(device, hidden):
        return layer(device, hidden, w_two, self_two, send_rows, send_count, edge_src, edge_dst)

    hidden = lax.map(lambda device: jnp.maximum(first(device)[5], 0.0).astype(jnp.bfloat16), devices).reshape(NODES, D)
    logits = lax.map(lambda device: second(device, hidden)[5], devices).reshape(NODES, CLASSES)

    labelled = labels >= 0
    log_total = jax.nn.logsumexp(logits, axis=1)
    one_hot = (jnp.arange(CLASSES, dtype=jnp.int32)[None, :] == labels[:, None]).astype(jnp.float32)
    picked = jnp.sum(logits * one_hot, axis=1)
    total = jnp.sum(jnp.where(labelled, log_total - picked, 0.0))
    label_count = jnp.sum(labelled.astype(jnp.float32))
    loss = total / label_count
    softmax_out = jnp.exp(logits - log_total[:, None])
    grad_logits = (loss_scale * (softmax_out - one_hot) * labelled[:, None].astype(jnp.float32) / label_count).astype(jnp.bfloat16)

    table_rows = NODES_DEV + N_DOM * SLOTS

    def back_two(carry, device):
        own_rows, averaged, norm_rows, sources, targets, unused = second(device, hidden)
        grad_rows = lax.dynamic_slice_in_dim(grad_logits, (device * NODES_DEV).astype(jnp.int32), NODES_DEV, 0)
        grad_term = jnp.concatenate([
            jnp.einsum('rnd,nc->rdc', averaged.astype(jnp.float32), grad_rows.astype(jnp.float32)),
            jnp.dot(own_rows.T, grad_rows, preferred_element_type=jnp.float32)[None]], axis=0)
        spread = (jnp.einsum('nc,rdc->rnd', grad_rows.astype(jnp.float32), w_two.astype(jnp.float32)) * norm_rows[:, :, None]).astype(jnp.bfloat16)
        segment = edge_targets(targets)
        padded = jnp.concatenate([spread.reshape(RELATIONS * NODES_DEV, D), jnp.zeros((1, D), jnp.bfloat16)], axis=0)
        per_edge = padded[segment].astype(jnp.float32)
        table_grad = jax.ops.segment_sum(per_edge, sources.reshape(-1), num_segments=table_rows)
        local_grad = table_grad[:NODES_DEV] + jnp.dot(grad_rows, self_two.T, preferred_element_type=jnp.float32)
        return carry + grad_term, (local_grad, table_grad[NODES_DEV:].astype(jnp.bfloat16))

    grad_two, outputs = lax.scan(back_two, jnp.zeros((RELATIONS + 1, D, CLASSES), jnp.float32), devices)
    local_grads, backs = outputs

    owners = jnp.arange(N_DOM, dtype=jnp.int32)[None, :, None] * NODES_DEV + jnp.swapaxes(send_rows, 0, 1)
    live_slot = jnp.arange(SLOTS, dtype=jnp.int32)[None, None, :] < jnp.swapaxes(send_count, 0, 1)[:, :, None]
    back_values = jnp.where(live_slot[..., None], backs.reshape(N_DOM, N_DOM, SLOTS, D).astype(jnp.float32), 0.0)
    returned = jax.ops.segment_sum(back_values.reshape(-1, D), owners.reshape(-1), num_segments=NODES)
    grad_hidden = local_grads.reshape(NODES, D) + returned

    def back_one(carry, device):
        own_rows, averaged, norm_rows, sources, targets, before_relu = first(device)
        grad_rows = lax.dynamic_slice_in_dim(grad_hidden, (device * NODES_DEV).astype(jnp.int32), NODES_DEV, 0)
        grad_pre = jnp.where(before_relu > 0.0, grad_rows, 0.0).astype(jnp.bfloat16)
        grad_term = jnp.concatenate([
            jnp.einsum('rnd,ne->rde', averaged.astype(jnp.float32), grad_pre.astype(jnp.float32)),
            jnp.dot(own_rows.T, grad_pre, preferred_element_type=jnp.float32)[None]], axis=0)
        return carry + grad_term, None

    grad_one, unused = lax.scan(back_one, jnp.zeros((RELATIONS + 1, D, D), jnp.float32), devices)
    return (logits, loss, grad_one.reshape((RELATIONS + 1) * D, D), grad_two.reshape((RELATIONS + 1) * D, CLASSES))
```

```python
import functools

import jax
import jax.numpy as jnp
from jax import lax
from jax.experimental import pallas as pl
from jax.experimental.pallas import tpu as pltpu
from jax.sharding import Mesh
from jax.sharding import PartitionSpec as P

DOM = ("dom_0", "dom_1", "dom_2", "dom_3")
BF = jnp.bfloat16
F32 = jnp.float32
I32 = jnp.int32
loss_scale = 256.0
MB = 1 << 20


def copy_for_each(value, axis):
    count = lax.axis_size(axis)
    return lax.all_to_all(
        jnp.broadcast_to(value[None], (count, *value.shape)), axis, 0, 0, tiled=True
    )


def taken_together(value, axis):
    return jnp.sum(copy_for_each(value, axis), axis=0)


def one_axis_at_a_time(value, axes):
    far, near = axes
    return taken_together(taken_together(value, near), far)


def in_blocks(value, dim, count):
    shape = value.shape
    parts = value.reshape(*shape[:dim], count, shape[dim] // count, *shape[dim + 1 :])
    return jnp.moveaxis(parts, dim, 0)


def summed_on_arrival(value, axis, dim):
    parts = in_blocks(value, dim, lax.axis_size(axis))
    arrived = lax.all_to_all(parts, axis, split_axis=0, concat_axis=0, tiled=True)
    return arrived.astype(F32).sum(axis=0)


def summed_rows(value, axes, dim):
    far, near = axes
    own = summed_on_arrival(in_blocks(value, dim, lax.axis_size(far)), near, dim + 1)
    return jnp.sum(
        lax.all_to_all(own.astype(BF), far, 0, 0, tiled=True).astype(F32), axis=0
    )


def dot(a, b):
    return jnp.dot(a, b, preferred_element_type=F32)


def dot_nt(a, b):
    return lax.dot_general(a, b, (((1,), (1,)), ((), ())), preferred_element_type=F32)


def dot_tn(a, b):
    return lax.dot_general(a, b, (((0,), (0,)), ((), ())), preferred_element_type=F32)


def iota(shape, dim):
    return lax.broadcasted_iota(I32, shape, dim)


def one_hot_cols(col, count):
    return jnp.where(col == iota((col.shape[0], count), 1), 1.0, 0.0).astype(BF)


def one_hot_rows(row, count):
    return jnp.where(row == iota((count, row.shape[1]), 0), 1.0, 0.0).astype(BF)


def pack_body(values, picks, packed):
    hot = one_hot_cols(picks[...], values.shape[0])
    packed[...] = dot(hot, values[...]).astype(BF)


def adjacency_body(src_row, dst_row, src_col, dst_col, adj, adj_t, norm):
    table_rows = adj.shape[2]
    for b in range(2):
        dst_hot = one_hot_rows(dst_row[0, b : b + 1, :], 128)
        src_hot = one_hot_cols(src_col[0, :, b : b + 1], table_rows)
        adj[0, b * 128 : (b + 1) * 128, :] = dot(dst_hot, src_hot).astype(BF)
        counts = jnp.sum(dst_hot.astype(F32), axis=1, keepdims=True)
        norm[0, b * 128 : (b + 1) * 128, :] = jnp.broadcast_to(
            1.0 / jnp.maximum(counts, 1.0), (128, 128)
        )
        src_hot_t = one_hot_rows(src_row[0, b : b + 1, :], table_rows)
        dst_hot_t = one_hot_cols(dst_col[0, :, b : b + 1], 128)
        adj_t[0, :, b * 128 : (b + 1) * 128] = dot(src_hot_t, dst_hot_t).astype(BF)


def averaged_rows(adj, norm, own, arrived):
    rows = own.shape[0]
    sums = dot(adj[0, :, :rows], own[...]) + dot(adj[0, :, rows:], arrived[...])
    return (sums * norm[0, :, :1]).astype(BF)


def first_body(own, arrived, adj, norm, w, w_self, picks, avg, pre, hidden, packed, acc):
    r = pl.program_id(0)

    @pl.when(r == 0)
    def _():
        acc[...] = dot(own[...], w_self[0])

    a = averaged_rows(adj, norm, own, arrived)
    avg[0] = a
    acc[...] += dot(a, w[0])

    @pl.when(r == pl.num_programs(0) - 1)
    def _():
        total = acc[...]
        pre[...] = total
        h = jnp.maximum(total, 0.0).astype(BF)
        hidden[...] = h
        packed[...] = dot(one_hot_cols(picks[...], h.shape[0]), h).astype(BF)


def second_body(count, own, arrived, adj, norm, w, w_self, labels, avg, logits, grad, part, acc):
    r = pl.program_id(0)

    @pl.when(r == 0)
    def _():
        acc[...] = dot(own[...], w_self[...])

    a = averaged_rows(adj, norm, own, arrived)
    avg[0] = a
    acc[...] += dot(a, w[0])

    @pl.when(r == pl.num_programs(0) - 1)
    def _():
        out = acc[...]
        logits[...] = out
        lab = labels[...]
        labelled = lab >= 0
        top = jnp.max(out, axis=1, keepdims=True)
        log_total = jnp.log(jnp.sum(jnp.exp(out - top), axis=1, keepdims=True)) + top
        hot = jnp.where(lab == iota(out.shape, 1), 1.0, 0.0)
        picked = jnp.sum(out * hot, axis=1, keepdims=True)
        part[...] = jnp.sum(
            jnp.where(labelled, log_total - picked, 0.0), axis=0, keepdims=True
        )
        soft = jnp.exp(out - log_total)
        mask = jnp.where(labelled, 1.0, 0.0)
        grad[...] = (loss_scale * (soft - hot) * mask / count[0, 0]).astype(BF)


def spread_body(grad, w, w_self, adj_t, norm, back, local, acc):
    r = pl.program_id(0)
    rows = local.shape[0]

    @pl.when(r == 0)
    def _():
        acc[...] = jnp.zeros_like(acc)

    spread = (dot_nt(grad[...], w[0]) * norm[0, :, :1]).astype(BF)
    acc[...] += dot(adj_t[0], spread)

    @pl.when(r == pl.num_programs(0) - 1)
    def _():
        back[...] = acc[rows:, :].astype(BF)
        local[...] = acc[:rows, :] + dot_nt(grad[...], w_self[...])


def two_body(avg, own, grad, out):
    r = pl.program_id(0)
    last = pl.num_programs(0) - 1

    @pl.when(r < last)
    def _():
        out[...] = dot_tn(avg[0], grad[...]).astype(BF)

    @pl.when(r == last)
    def _():
        out[...] = dot_tn(own[...], grad[...]).astype(BF)


def one_body(avg, own, local, returned, picks, pre, out, grad_pre):
    r = pl.program_id(0)
    last = pl.num_programs(0) - 1

    @pl.when(r == 0)
    def _():
        hot = one_hot_rows(picks[...], local.shape[0])
        grad = local[...] + dot(hot, returned[...])
        grad_pre[...] = jnp.where(pre[...] > 0.0, grad, 0.0).astype(BF)

    @pl.when(r < last)
    def _():
        out[...] = dot_tn(avg[0], grad_pre[...]).astype(BF)

    @pl.when(r == last)
    def _():
        out[...] = dot_tn(own[...], grad_pre[...]).astype(BF)


def whole(shape, space=None):
    n = len(shape)
    return pl.BlockSpec(shape, lambda *_: (0,) * n)


def per_r(shape, top=None):
    n = len(shape)
    if top is None:
        return pl.BlockSpec((1, *shape), lambda r: (r,) + (0,) * n)
    return pl.BlockSpec((1, *shape), lambda r: (jnp.minimum(r, top),) + (0,) * n)


def sds(shape, dtype):
    return jax.ShapeDtypeStruct(shape, dtype)


def call(body, name, grid, ins, outs, shapes, scratch, flops, args, vmem=32 * MB):
    return pl.pallas_call(
        body,
        name=name,
        grid=grid,
        in_specs=ins,
        out_specs=outs,
        out_shape=shapes,
        scratch_shapes=scratch,
        compiler_params=pltpu.CompilerParams(
            vmem_limit_bytes=vmem, dimension_semantics=("arbitrary",) * len(grid)
        ),
        cost_estimate=pl.CostEstimate(flops=flops, bytes_accessed=0, transcendentals=0),
    )(*args)


def on_device(features, w_one, w_two, self_two, edge_src, edge_dst, send_rows, send_count, labels):
    peers = lax.axis_size(DOM)
    n, d = features.shape
    rel = w_two.shape[0]
    classes = w_two.shape[2]
    slots = send_rows.shape[2]
    far = peers * slots
    table = n + far
    live_slot = jnp.arange(slots, dtype=I32)[None, :] < send_count[0][:, None]
    picks = jnp.where(live_slot, send_rows[0], -1)
    picks_col = picks.reshape(far, 1)
    picks_row = picks.reshape(1, far)

    local_count = jnp.sum((labels >= 0).astype(F32))
    label_count = one_axis_at_a_time(
        local_count.reshape(1), (("dom_0", "dom_1", "dom_2"), "dom_3")
    )[0]

    packed = call(
        pack_body, "pack", (1,), [whole((n, d)), whole((far, 1))], whole((far, d)),
        sds((far, d), BF), [], 2 * far * n * d, (features, picks_col),
    )

    def exchange(v):
        return lax.all_to_all(
            v.reshape(peers, slots, d), DOM, split_axis=0, concat_axis=0, tiled=True
        ).reshape(far, d)

    arrived = exchange(packed)
    adj, adj_t, norm = call(
        adjacency_body, "adjacency", (rel,),
        [per_r((2, 256)), per_r((2, 256)), per_r((256, 2)), per_r((256, 2))],
        [per_r((n, table)), per_r((table, n)), per_r((n, 128))],
        [sds((rel, n, table), BF), sds((rel, table, n), BF), sds((rel, n, 128), F32)],
        [], 4 * rel * 2 * 128 * 256 * table,
        (edge_src, edge_dst, jnp.swapaxes(edge_src, 1, 2), jnp.swapaxes(edge_dst, 1, 2)),
    )
    w_last = pl.BlockSpec((1, d, d), lambda r: (rel, 0, 0))
    avg_one, pre, hidden, packed_hidden = call(
        first_body, "first", (rel,),
        [whole((n, d)), whole((far, d)), per_r((n, table)), per_r((n, 128)), per_r((d, d)), w_last,
         whole((far, 1))],
        [per_r((n, d)), whole((n, d)), whole((n, d)), whole((far, d))],
        [sds((rel, n, d), BF), sds((n, d), F32), sds((n, d), BF), sds((far, d), BF)],
        [pltpu.VMEM((n, d), F32)], 2 * rel * n * d * (table + d),
        (features, arrived, adj, norm, w_one, w_one, picks_col),
    )
    arrived_hidden = exchange(packed_hidden)
    avg_two, logits, grad_logits, part = call(
        second_body, "second", (rel,),
        [pl.BlockSpec(memory_space=pltpu.SMEM), whole((n, d)), whole((far, d)), per_r((n, table)),
         per_r((n, 128)), per_r((d, classes)), whole((d, classes)), whole((n, 1))],
        [per_r((n, d)), whole((n, classes)), whole((n, classes)), whole((1, 1))],
        [sds((rel, n, d), BF), sds((n, classes), F32), sds((n, classes), BF), sds((1, 1), F32)],
        [pltpu.VMEM((n, classes), F32)], 2 * rel * n * d * (table + classes),
        (label_count.reshape(1, 1), hidden, arrived_hidden, adj, norm, w_two, self_two,
         labels.reshape(n, 1)),
    )
    back, local = call(
        spread_body, "spread", (rel,),
        [whole((n, classes)), per_r((d, classes)), whole((d, classes)), per_r((table, n)),
         per_r((n, 128))],
        [whole((far, d)), whole((n, d))],
        [sds((far, d), BF), sds((n, d), F32)],
        [pltpu.VMEM((table, d), F32)], 2 * rel * n * d * (table + classes),
        (grad_logits, w_two, self_two, adj_t, norm),
    )
    returned = exchange(back)
    total = one_axis_at_a_time(part.reshape(1), (("dom_0", "dom_1", "dom_2"), "dom_3"))[0]
    loss = total / label_count
    g_two = call(
        two_body, "two", (rel + 1,),
        [per_r((n, d), rel - 1), whole((n, d)), whole((n, classes))],
        pl.BlockSpec((d, classes), lambda r: (r, 0)),
        sds(((rel + 1) * d, classes), BF), [], 2 * (rel + 1) * n * d * classes,
        (avg_two, hidden, grad_logits),
    )
    g_one = call(
        one_body, "one", (rel + 1,),
        [per_r((n, d), rel - 1), whole((n, d)), whole((n, d)), whole((far, d)), whole((1, far)),
         whole((n, d))],
        pl.BlockSpec((d, d), lambda r: (r, 0)),
        sds(((rel + 1) * d, d), BF), [pltpu.VMEM((n, d), BF)], 2 * (rel + 1) * n * d * d,
        (avg_one, features, local, returned, picks_row, pre),
    )
    joined = summed_rows(
        jnp.concatenate([g_one, g_two], axis=1), (("dom_0", "dom_1", "dom_2"), "dom_3"), 0
    )
    return (logits, loss, joined[:, :d], joined[:, d:])


def solution(mesh):
    split = Mesh(mesh.devices.reshape(4, 4, 4, 2), DOM)
    return jax.shard_map(
        on_device,
        mesh=split,
        in_specs=(
            P(DOM, None),
            P(),
            P(),
            P(),
            P(None, DOM, None),
            P(None, DOM, None),
            P(DOM, None, None),
            P(DOM, None),
            P(DOM),
        ),
        out_specs=(P(DOM, None), P(), P(DOM, None), P(DOM, None)),
        check_vma=False,
    )
```

```python
import functools

import jax
import jax.numpy as jnp
from jax import lax
from jax.experimental import pallas as pl
from jax.experimental.pallas import tpu as pltpu
from jax.sharding import Mesh
from jax.sharding import PartitionSpec as P

DOM = ("dom_0", "dom_1", "dom_2", "dom_3")
BF = jnp.bfloat16
F32 = jnp.float32
I32 = jnp.int32
loss_scale = 256.0
MB = 1 << 20


def copy_for_each(value, axis):
    count = lax.axis_size(axis)
    return lax.all_to_all(
        jnp.broadcast_to(value[None], (count, *value.shape)), axis, 0, 0, tiled=True
    )


def taken_together(value, axis):
    return jnp.sum(copy_for_each(value, axis), axis=0)


def one_axis_at_a_time(value, axes):
    far, near = axes
    return taken_together(taken_together(value, near), far)


def in_blocks(value, dim, count):
    shape = value.shape
    parts = value.reshape(*shape[:dim], count, shape[dim] // count, *shape[dim + 1 :])
    return jnp.moveaxis(parts, dim, 0)


def summed_on_arrival(value, axis, dim):
    parts = in_blocks(value, dim, lax.axis_size(axis))
    arrived = lax.all_to_all(parts, axis, split_axis=0, concat_axis=0, tiled=True)
    return arrived.astype(F32).sum(axis=0)


def summed_rows(value, axes, dim):
    far, near = axes
    own = summed_on_arrival(in_blocks(value, dim, lax.axis_size(far)), near, dim + 1)
    return jnp.sum(
        lax.all_to_all(own.astype(BF), far, 0, 0, tiled=True).astype(F32), axis=0
    )


def dot(a, b):
    return jnp.dot(a, b, preferred_element_type=F32)


def dot_nt(a, b):
    return lax.dot_general(a, b, (((1,), (1,)), ((), ())), preferred_element_type=F32)


def dot_tn(a, b):
    return lax.dot_general(a, b, (((0,), (0,)), ((), ())), preferred_element_type=F32)


def iota(shape, dim):
    return lax.broadcasted_iota(I32, shape, dim)


def one_hot_cols(col, count):
    return jnp.where(col == iota((col.shape[0], count), 1), 1.0, 0.0).astype(BF)


def one_hot_rows(row, count):
    return jnp.where(row == iota((count, row.shape[1]), 0), 1.0, 0.0).astype(BF)


def pack_body(values, picks, packed):
    hot = one_hot_cols(picks[...], values.shape[0])
    packed[...] = dot(hot, values[...]).astype(BF)


def adjacency_body(src_row, dst_row, src_col, dst_col, adj, adj_t, norm):
    table_rows = adj.shape[2]
    for b in range(2):
        dst_hot = one_hot_rows(dst_row[0, b : b + 1, :], 128)
        src_hot = one_hot_cols(src_col[0, :, b : b + 1], table_rows)
        adj[0, b * 128 : (b + 1) * 128, :] = dot(dst_hot, src_hot).astype(BF)
        counts = jnp.sum(dst_hot.astype(F32), axis=1, keepdims=True)
        norm[0, b * 128 : (b + 1) * 128, :] = jnp.broadcast_to(
            1.0 / jnp.maximum(counts, 1.0), (128, 128)
        )
        src_hot_t = one_hot_rows(src_row[0, b : b + 1, :], table_rows)
        dst_hot_t = one_hot_cols(dst_col[0, :, b : b + 1], 128)
        adj_t[0, :, b * 128 : (b + 1) * 128] = dot(src_hot_t, dst_hot_t).astype(BF)


def averaged_rows(adj, norm, own, arrived):
    rows = own.shape[0]
    sums = dot(adj[0, :, :rows], own[...]) + dot(adj[0, :, rows:], arrived[...])
    return (sums * norm[0, :, :1]).astype(BF)


def first_body(own, arrived, adj, norm, w, w_self, picks, avg, pre, hidden, packed, acc):
    r = pl.program_id(0)

    @pl.when(r == 0)
    def _():
        acc[...] = dot(own[...], w_self[0])

    a = averaged_rows(adj, norm, own, arrived)
    avg[0] = a
    acc[...] += dot(a, w[0])

    @pl.when(r == pl.num_programs(0) - 1)
    def _():
        total = acc[...]
        pre[...] = total
        h = jnp.maximum(total, 0.0).astype(BF)
        hidden[...] = h
        packed[...] = dot(one_hot_cols(picks[...], h.shape[0]), h).astype(BF)


def second_body(count, own, arrived, adj, norm, w, w_self, labels, avg, logits, grad, part, acc):
    r = pl.program_id(0)

    @pl.when(r == 0)
    def _():
        acc[...] = dot(own[...], w_self[...])

    a = averaged_rows(adj, norm, own, arrived)
    avg[0] = a
    acc[...] += dot(a, w[0])

    @pl.when(r == pl.num_programs(0) - 1)
    def _():
        out = acc[...]
        logits[...] = out
        lab = labels[...]
        labelled = lab >= 0
        top = jnp.max(out, axis=1, keepdims=True)
        log_total = jnp.log(jnp.sum(jnp.exp(out - top), axis=1, keepdims=True)) + top
        hot = jnp.where(lab == iota(out.shape, 1), 1.0, 0.0)
        picked = jnp.sum(out * hot, axis=1, keepdims=True)
        part[...] = jnp.sum(
            jnp.where(labelled, log_total - picked, 0.0), axis=0, keepdims=True
        )
        soft = jnp.exp(out - log_total)
        mask = jnp.where(labelled, 1.0, 0.0)
        grad[...] = (loss_scale * (soft - hot) * mask / count[0, 0]).astype(BF)


def spread_body(grad, w, w_self, adj_t, norm, back, local, acc):
    r = pl.program_id(0)
    rows = local.shape[0]

    @pl.when(r == 0)
    def _():
        acc[...] = jnp.zeros_like(acc)

    spread = (dot_nt(grad[...], w[0]) * norm[0, :, :1]).astype(BF)
    acc[...] += dot(adj_t[0], spread)

    @pl.when(r == pl.num_programs(0) - 1)
    def _():
        back[...] = acc[rows:, :].astype(BF)
        local[...] = acc[:rows, :] + dot_nt(grad[...], w_self[...])


def two_body(avg, own, grad, out):
    r = pl.program_id(0)
    last = pl.num_programs(0) - 1

    @pl.when(r < last)
    def _():
        out[...] = dot_tn(avg[0], grad[...]).astype(BF)

    @pl.when(r == last)
    def _():
        out[...] = dot_tn(own[...], grad[...]).astype(BF)


def one_body(avg, own, local, returned, picks, pre, out, grad_pre):
    r = pl.program_id(0)
    last = pl.num_programs(0) - 1

    @pl.when(r == 0)
    def _():
        hot = one_hot_rows(picks[...], local.shape[0])
        grad = local[...] + dot(hot, returned[...])
        grad_pre[...] = jnp.where(pre[...] > 0.0, grad, 0.0).astype(BF)

    @pl.when(r < last)
    def _():
        out[...] = dot_tn(avg[0], grad_pre[...]).astype(BF)

    @pl.when(r == last)
    def _():
        out[...] = dot_tn(own[...], grad_pre[...]).astype(BF)


def a2a_body(x, y, send_sem, recv_sem):
    sizes = [lax.axis_size(a) for a in DOM]
    me = [lax.axis_index(a) for a in DOM]
    mine = ((me[0] * sizes[1] + me[1]) * sizes[2] + me[2]) * sizes[3] + me[3]
    count = x.shape[0]

    def send(k, carry):
        d0 = k % 4
        d1 = (k // 4 + d0) % 4
        d2 = (k // 16 + d1) % 4
        step = (d0, d1, d2, k // 64)
        to = [lax.rem(m + s, n) for m, s, n in zip(me, step, sizes)]
        peer = ((to[0] * sizes[1] + to[1]) * sizes[2] + to[2]) * sizes[3] + to[3]
        pltpu.make_async_remote_copy(
            src_ref=x.at[peer], dst_ref=y.at[mine], send_sem=send_sem, recv_sem=recv_sem,
            device_id=tuple(to), device_id_type=pl.DeviceIdType.MESH,
        ).start()
        return carry

    lax.fori_loop(1, count, send, 0)
    y[mine] = x[mine]
    rest = pl.ds(0, count - 1)
    pltpu.make_async_copy(x.at[rest], y.at[rest], send_sem).wait()
    pltpu.make_async_copy(x.at[rest], y.at[rest], recv_sem).wait()


def whole(shape, space=None):
    n = len(shape)
    return pl.BlockSpec(shape, lambda *_: (0,) * n)


def per_r(shape, top=None):
    n = len(shape)
    if top is None:
        return pl.BlockSpec((1, *shape), lambda r: (r,) + (0,) * n)
    return pl.BlockSpec((1, *shape), lambda r: (jnp.minimum(r, top),) + (0,) * n)


def sds(shape, dtype):
    return jax.ShapeDtypeStruct(shape, dtype)


def call(body, name, grid, ins, outs, shapes, scratch, flops, args, vmem=32 * MB):
    return pl.pallas_call(
        body,
        name=name,
        grid=grid,
        in_specs=ins,
        out_specs=outs,
        out_shape=shapes,
        scratch_shapes=scratch,
        compiler_params=pltpu.CompilerParams(
            vmem_limit_bytes=vmem, dimension_semantics=("arbitrary",) * len(grid)
        ),
        cost_estimate=pl.CostEstimate(flops=flops, bytes_accessed=0, transcendentals=0),
    )(*args)


def on_device(features, w_one, w_two, self_two, edge_src, edge_dst, send_rows, send_count, labels):
    peers = lax.axis_size(DOM)
    n, d = features.shape
    rel = w_two.shape[0]
    classes = w_two.shape[2]
    slots = send_rows.shape[2]
    far = peers * slots
    table = n + far
    live_slot = jnp.arange(slots, dtype=I32)[None, :] < send_count[0][:, None]
    picks = jnp.where(live_slot, send_rows[0], -1)
    picks_col = picks.reshape(far, 1)
    picks_row = picks.reshape(1, far)

    local_count = jnp.sum((labels >= 0).astype(F32))
    label_count = one_axis_at_a_time(
        local_count.reshape(1), (("dom_0", "dom_1", "dom_2"), "dom_3")
    )[0]

    packed = call(
        pack_body, "pack", (1,), [whole((n, d)), whole((far, 1))], whole((far, d)),
        sds((far, d), BF), [], 2 * far * n * d, (features, picks_col),
    )

    def exchange(v):
        return pl.pallas_call(
            a2a_body,
            name="boundary",
            in_specs=[pl.BlockSpec(memory_space=pltpu.VMEM)],
            out_specs=pl.BlockSpec(memory_space=pltpu.VMEM),
            out_shape=sds((peers, slots, d), BF),
            scratch_shapes=[pltpu.SemaphoreType.DMA, pltpu.SemaphoreType.DMA],
            compiler_params=pltpu.CompilerParams(has_side_effects=True, vmem_limit_bytes=4 * MB),
        )(v.reshape(peers, slots, d)).reshape(far, d)

    arrived = exchange(packed)
    adj, adj_t, norm = call(
        adjacency_body, "adjacency", (rel,),
        [per_r((2, 256)), per_r((2, 256)), per_r((256, 2)), per_r((256, 2))],
        [per_r((n, table)), per_r((table, n)), per_r((n, 128))],
        [sds((rel, n, table), BF), sds((rel, table, n), BF), sds((rel, n, 128), F32)],
        [], 4 * rel * 2 * 128 * 256 * table,
        (edge_src, edge_dst, jnp.swapaxes(edge_src, 1, 2), jnp.swapaxes(edge_dst, 1, 2)),
    )
    w_last = pl.BlockSpec((1, d, d), lambda r: (rel, 0, 0))
    avg_one, pre, hidden, packed_hidden = call(
        first_body, "first", (rel,),
        [whole((n, d)), whole((far, d)), per_r((n, table)), per_r((n, 128)), per_r((d, d)), w_last,
         whole((far, 1))],
        [per_r((n, d)), whole((n, d)), whole((n, d)), whole((far, d))],
        [sds((rel, n, d), BF), sds((n, d), F32), sds((n, d), BF), sds((far, d), BF)],
        [pltpu.VMEM((n, d), F32)], 2 * rel * n * d * (table + d),
        (features, arrived, adj, norm, w_one, w_one, picks_col),
    )
    arrived_hidden = exchange(packed_hidden)
    avg_two, logits, grad_logits, part = call(
        second_body, "second", (rel,),
        [pl.BlockSpec(memory_space=pltpu.SMEM), whole((n, d)), whole((far, d)), per_r((n, table)),
         per_r((n, 128)), per_r((d, classes)), whole((d, classes)), whole((n, 1))],
        [per_r((n, d)), whole((n, classes)), whole((n, classes)), whole((1, 1))],
        [sds((rel, n, d), BF), sds((n, classes), F32), sds((n, classes), BF), sds((1, 1), F32)],
        [pltpu.VMEM((n, classes), F32)], 2 * rel * n * d * (table + classes),
        (label_count.reshape(1, 1), hidden, arrived_hidden, adj, norm, w_two, self_two,
         labels.reshape(n, 1)),
    )
    back, local = call(
        spread_body, "spread", (rel,),
        [whole((n, classes)), per_r((d, classes)), whole((d, classes)), per_r((table, n)),
         per_r((n, 128))],
        [whole((far, d)), whole((n, d))],
        [sds((far, d), BF), sds((n, d), F32)],
        [pltpu.VMEM((table, d), F32)], 2 * rel * n * d * (table + classes),
        (grad_logits, w_two, self_two, adj_t, norm),
    )
    returned = exchange(back)
    total = one_axis_at_a_time(part.reshape(1), (("dom_0", "dom_1", "dom_2"), "dom_3"))[0]
    loss = total / label_count
    g_two = call(
        two_body, "two", (rel + 1,),
        [per_r((n, d), rel - 1), whole((n, d)), whole((n, classes))],
        pl.BlockSpec((d, classes), lambda r: (r, 0)),
        sds(((rel + 1) * d, classes), BF), [], 2 * (rel + 1) * n * d * classes,
        (avg_two, hidden, grad_logits),
    )
    g_one = call(
        one_body, "one", (rel + 1,),
        [per_r((n, d), rel - 1), whole((n, d)), whole((n, d)), whole((far, d)), whole((1, far)),
         whole((n, d))],
        pl.BlockSpec((d, d), lambda r: (r, 0)),
        sds(((rel + 1) * d, d), BF), [pltpu.VMEM((n, d), BF)], 2 * (rel + 1) * n * d * d,
        (avg_one, features, local, returned, picks_row, pre),
    )
    joined = summed_rows(
        jnp.concatenate([g_one, g_two], axis=1), (("dom_0", "dom_1", "dom_2"), "dom_3"), 0
    )
    return (logits, loss, joined[:, :d], joined[:, d:])


def solution(mesh):
    split = Mesh(mesh.devices.reshape(4, 4, 4, 2), DOM)
    return jax.shard_map(
        on_device,
        mesh=split,
        in_specs=(
            P(DOM, None),
            P(),
            P(),
            P(),
            P(None, DOM, None),
            P(None, DOM, None),
            P(DOM, None, None),
            P(DOM, None),
            P(DOM),
        ),
        out_specs=(P(DOM, None), P(), P(DOM, None), P(DOM, None)),
        check_vma=False,
    )
```

```python
import jax
import jax.numpy as jnp
from jax import lax
from jax.experimental import pallas as pl
from jax.experimental.pallas import tpu as pltpu
from jax.sharding import Mesh
from jax.sharding import PartitionSpec as P

DOM = ("dom_0", "dom_1", "dom_2", "dom_3")
SIZES = (4, 4, 4, 2)
BF = jnp.bfloat16
F32 = jnp.float32
I32 = jnp.int32
MESH = pl.DeviceIdType.MESH
loss_scale = 256.0
MB = 1 << 20

PEERS = 128
CHIPS = 64
SLOTS = 8
REL = 8
N = 256
D = 512
C = 349
CP = 384
FAR = PEERS * SLOTS
TABLE = N + FAR
ROWS = 36
WIDE = D + CP
BLOCK = 16 * ROWS

STREAMS = ((0, 256, (0, 1, 2)), (256, 256, (1, 2, 0)), (512, 384, (2, 0, 1)))


def dot(a, b):
    return jnp.dot(a, b, preferred_element_type=F32)


def dot_nt(a, b):
    return lax.dot_general(a, b, (((1,), (1,)), ((), ())), preferred_element_type=F32)


def iota(shape, dim):
    return lax.broadcasted_iota(I32, shape, dim)


def hot(mask):
    return jnp.where(mask, 1.0, 0.0).astype(BF)


def step_body(
    own, w_one_hbm, w_two_hbm, w_self_hbm, src, dst, rows, count, labels,
    logits_t, loss, grad_one, grad_two,
    w_one, w_two, w_self, adj, adj_t, norm, picks, picks_t,
    send, got_one, got_two, got_three, avg, avg_one_t, avg_two_t,
    pre, hidden, acc, table_acc, grad, grad_pre, keep,
    small_out, counts, totals,
    parts, near, half, r1a, r1b, r1c, q_a, q_b, q_c, r2a, r2b, r2c, t_a, t_b, t_c, r3a, r3b, r3c,
    w_sems, a_send, a_recv, s_send, s_recv, p_send, p_recv, x_send, x_recv,
):
    me = [lax.axis_index(a) for a in DOM]
    mine = ((me[0] * 4 + me[1]) * 4 + me[2]) * 2 + me[3]
    core = me[3]

    loads = [
        pltpu.make_async_copy(w_one_hbm, w_one, w_sems.at[0]),
        pltpu.make_async_copy(w_two_hbm, w_two, w_sems.at[1]),
        pltpu.make_async_copy(w_self_hbm, w_self, w_sems.at[2]),
    ]
    for load in loads:
        load.start()

    def relative(k):
        d0 = k % 4
        d1 = (k // 4 + d0) % 4
        d2 = (k // 16 + d1) % 4
        to = [lax.rem(m + s, n) for m, s, n in zip(me, (d0, d1, d2, k // 64), SIZES)]
        return to, ((to[0] * 4 + to[1]) * 4 + to[2]) * 2 + to[3]

    barrier = pltpu.get_barrier_semaphore()

    def greet(k, carry):
        to, _ = relative(k)
        pl.semaphore_signal(barrier, inc=1, device_id=tuple(to), device_id_type=MESH)
        return carry

    lax.fori_loop(1, PEERS, greet, 0)

    spot = iota((FAR, PEERS), 0)
    peer_hot = spot // SLOTS == iota((FAR, PEERS), 1)
    by_peer = dot(hot(peer_hot), rows[...].astype(F32).astype(BF))
    slot = iota((FAR, SLOTS), 0) % SLOTS
    chosen = jnp.sum(jnp.where(slot == iota((FAR, SLOTS), 1), by_peer, 0.0), axis=1, keepdims=True)
    live = jnp.sum(
        jnp.where(peer_hot, jnp.broadcast_to(count[...], (FAR, PEERS)), 0).astype(F32),
        axis=1, keepdims=True,
    )
    row_of = jnp.where(
        (iota((FAR, 1), 0) % SLOTS).astype(F32) < live, chosen, -1.0
    ).astype(I32)
    picks[...] = hot(row_of == iota((FAR, N), 1))

    def pack(values):
        send[...] = dot(picks[...], values).astype(BF).reshape(PEERS, SLOTS, D)

    pack(own[...])
    small_out[0] = jnp.broadcast_to(
        jnp.sum(jnp.where(labels[...] >= 0, 1.0, 0.0), axis=1, keepdims=True), (1, 128)
    )
    pl.semaphore_wait(barrier, PEERS - 1)

    def exchange(got, which, small, small_got):
        def one(k, carry):
            to, peer = relative(k)
            pltpu.make_async_remote_copy(
                src_ref=send.at[peer], dst_ref=got.at[mine], send_sem=a_send.at[which],
                recv_sem=a_recv.at[which], device_id=tuple(to), device_id_type=MESH,
            ).start()
            if small is not None:
                pltpu.make_async_remote_copy(
                    src_ref=small_out.at[small], dst_ref=small_got.at[mine],
                    send_sem=s_send.at[small], recv_sem=s_recv.at[small],
                    device_id=tuple(to), device_id_type=MESH,
                ).start()
            return carry

        lax.fori_loop(1, PEERS, one, 0)
        got[mine] = send[mine]
        if small is not None:
            small_got[mine] = small_out[small]

    rest = pl.ds(0, PEERS - 1)

    def exchange_wait(got, which):
        pltpu.make_async_copy(send.at[rest], got.at[rest], a_send.at[which]).wait()
        pltpu.make_async_copy(send.at[rest], got.at[rest], a_recv.at[which]).wait()

    def small_wait(which):
        pltpu.make_async_copy(counts.at[rest], totals.at[rest], s_send.at[which]).wait()
        pltpu.make_async_copy(counts.at[rest], totals.at[rest], s_recv.at[which]).wait()

    exchange(got_one, 0, 0, counts)

    def relation(r, carry):
        for b in range(2):
            at = slice(b * 128, (b + 1) * 128)
            dst_hot = hot(dst[r, b : b + 1, :] == iota((128, 256), 0))
            src_hot = hot(src[r, b : b + 1, :] == iota((TABLE, 256), 0))
            adj[r, at, :] = dot_nt(dst_hot, src_hot).astype(BF)
            adj_t[r, :, at] = dot_nt(src_hot, dst_hot).astype(BF)
            live_edges = jnp.sum(dst_hot.astype(F32), axis=1, keepdims=True)
            norm[r, at, :] = jnp.broadcast_to(1.0 / jnp.maximum(live_edges, 1.0), (128, 128))
        return carry

    lax.fori_loop(0, REL, relation, 0)
    picks_t[...] = picks[...].T
    avg_one_t[REL * D :, :] = own[...].T
    for load in loads:
        load.wait()
    pre[...] = dot(own[...], w_one[REL])
    small_wait(0)
    labelled_count = jnp.sum(counts[:, :, 0:1])
    exchange_wait(got_one, 0)

    def averaged(r, values, got):
        far = got[...].reshape(FAR, D)
        sums = dot(adj[r, :, :N], values[...]) + dot(adj[r, :, N:], far)
        return (sums * norm[r, :, :1]).astype(BF)

    def first(r, carry):
        a = averaged(r, own, got_one)
        avg[r] = a
        pre[...] += dot(a, w_one[r])
        return carry

    lax.fori_loop(0, REL, first, 0)
    hidden[...] = jnp.maximum(pre[...], 0.0).astype(BF)
    pack(hidden[...])
    exchange(got_two, 1, None, None)

    def turn(r, out):
        out[pl.ds(pl.multiple_of(r * D, D), D), :] = avg[r].T
        return out

    def turn_one(r, carry):
        turn(r, avg_one_t)
        return carry

    lax.fori_loop(0, REL, turn_one, 0)
    avg_two_t[REL * D :, :] = hidden[...].T
    acc[...] = dot_nt(hidden[...], w_self[...])
    label_row = jnp.broadcast_to(labels[...], (128, N))
    lab = label_row.T[:, :1]
    exchange_wait(got_two, 1)

    def second(r, carry):
        a = averaged(r, hidden, got_two)
        avg[r] = a
        acc[...] += dot_nt(a, w_two[r])
        return carry

    lax.fori_loop(0, REL, second, 0)
    out = acc[...]
    labelled = lab >= 0
    top = jnp.max(out, axis=1, keepdims=True)
    log_total = jnp.log(jnp.sum(jnp.exp(out - top), axis=1, keepdims=True)) + top
    label_hot = jnp.where(lab == iota((N, C), 1), 1.0, 0.0)
    picked = jnp.sum(out * label_hot, axis=1, keepdims=True)
    soft = jnp.exp(out - log_total)
    mask = jnp.where(labelled, 1.0, 0.0)
    grad[...] = jnp.zeros_like(grad)
    grad[:, :C] = (loss_scale * (soft - label_hot) * mask / labelled_count).astype(BF)
    small_out[1] = jnp.broadcast_to(
        jnp.sum(jnp.where(labelled, log_total - picked, 0.0), axis=0, keepdims=True), (1, 128)
    )
    table_acc[...] = jnp.zeros_like(table_acc)

    def spread(r, carry):
        s = (dot(grad[:, :C], w_two[r]) * norm[r, :, :1]).astype(BF)
        table_acc[...] += dot(adj_t[r], s)
        return carry

    lax.fori_loop(0, REL, spread, 0)
    send[...] = table_acc[N:, :].astype(BF).reshape(PEERS, SLOTS, D)
    exchange(got_three, 2, 1, totals)

    partner = (me[0], me[1], me[2], 1 - core)

    def chunks(x, h, left, right, lanes):
        start = pl.multiple_of((x * 2 + h) * BLOCK, BLOCK)
        value = dot(left[pl.ds(start, BLOCK), :], right[...]).astype(BF)
        for j in range(16):
            to = (x, h * 2 + j // 8, (j // 2) % 4, j % 2)
            parts[(*to, slice(None), lanes)] = value[ROWS * j : ROWS * (j + 1), :]

    def to_partner(x, lanes, sem):
        return pltpu.make_async_remote_copy(
            src_ref=parts.at[x, :, :, 1 - core, :, lanes], dst_ref=near.at[x, :, :, :, lanes],
            send_sem=p_send.at[sem], recv_sem=p_recv.at[sem], device_id=partner,
            device_id_type=MESH,
        )

    def add_near(x, z, lanes):
        half[x, z, :, :, lanes] = (
            parts[x, z, :, core, :, lanes].astype(F32) + near[x, z, :, :, lanes].astype(F32)
        ).astype(BF)

    two_lanes = pl.ds(D, CP)
    one_lanes = pl.ds(0, D)

    def turn_two(r, carry):
        turn(r, avg_two_t)
        return carry

    lax.fori_loop(0, REL, turn_two, 0)

    def two_chunks(i, carry):
        chunks(i // 2, i % 2, avg_two_t, grad, two_lanes)
        return carry

    lax.fori_loop(0, 8, two_chunks, 0)
    two_copy = to_partner(slice(None), two_lanes, 4)
    two_copy.start()
    keep[:, :C] = out
    logits_t[...] = keep[...].T[:C, :]
    table_acc[:N, :] += dot(grad[:, :C], w_self[...])
    two_copy.wait()

    def add_two(i, carry):
        add_near(i // 4, i % 4, two_lanes)
        return carry

    lax.fori_loop(0, 16, add_two, 0)

    first_got = (r1a, r1b, r1c)
    first_sum = (q_a, q_b, q_c)
    second_got = (r2a, r2b, r2c)
    second_sum = (t_a, t_b, t_c)
    third_got = (r3a, r3b, r3c)

    def hop(s, phase, j):
        lane, width, order = STREAMS[s]
        axis = order[phase]
        k = lax.rem(me[axis] + j, 4)
        to = list(me)
        to[axis] = k
        if phase == 0:
            at = tuple(k if a == axis else slice(None) for a in range(3))
            ref = half.at[(*at, slice(None), pl.ds(lane, width))]
            got = first_got[s]
        elif phase == 1:
            left = sorted(order[1:])
            at = tuple(k if a == axis else slice(None) for a in left)
            ref = first_sum[s].at[at]
            got = second_got[s]
        else:
            ref = second_sum[s].at[k]
            got = third_got[s]
        sem = (s * 3 + phase) * 3 + j - 1
        return pltpu.make_async_remote_copy(
            src_ref=ref, dst_ref=got.at[j - 1], send_sem=x_send.at[sem], recv_sem=x_recv.at[sem],
            device_id=tuple(to), device_id_type=MESH,
        )

    exchange_wait(got_three, 2)
    for j in (2, 1, 3):
        hop(2, 0, j).start()

    grad_hidden = table_acc[:N, :] + dot(picks_t[...], got_three[...].reshape(FAR, D))
    grad_pre[...] = jnp.where(pre[...] > 0.0, grad_hidden, 0.0).astype(BF)

    for j in (1, 2, 3, 4):
        k = lax.rem(me[0] + j, 4)

        def one_chunks(i, carry):
            chunks(k, i, avg_one_t, grad_pre, one_lanes)
            return carry

        lax.fori_loop(0, 2, one_chunks, 0)
        to_partner(k, one_lanes, j - 1).start()
    for j in (1, 2, 3, 4):
        k = lax.rem(me[0] + j, 4)
        to_partner(k, one_lanes, j - 1).wait()

        def add_one(i, carry):
            add_near(k, i, one_lanes)
            return carry

        lax.fori_loop(0, 4, add_one, 0)
        if j < 4:
            hop(0, 0, j).start()
    for j in (2, 1, 3):
        hop(1, 0, j).start()

    def wide(ref, at):
        return ref[at].astype(F32)

    def sum_first(s):
        lane, width, order = STREAMS[s]
        for j in (1, 2, 3):
            hop(s, 0, j).wait()

        def body(i, carry):
            at = [None, None, None]
            left = sorted(order[1:])
            at[order[0]] = me[order[0]]
            at[left[0]] = i
            at[left[1]] = slice(None)
            total = half[(*at, slice(None), pl.ds(lane, width))].astype(F32)
            for j in range(3):
                total += first_got[s][j, i].astype(F32)
            first_sum[s][i] = total.astype(BF)
            return carry

        lax.fori_loop(0, 4, body, 0)
        for j in (2, 1, 3):
            hop(s, 1, j).start()

    def sum_second(s):
        order = STREAMS[s][2]
        for j in (1, 2, 3):
            hop(s, 1, j).wait()
        m = me[order[1]]
        if order[1] < order[2]:
            total = first_sum[s][m].astype(F32)
        else:
            total = first_sum[s][:, m].astype(F32)
        for j in range(3):
            total += second_got[s][j].astype(F32)
        second_sum[s][...] = total.astype(BF)
        for j in (2, 1, 3):
            hop(s, 2, j).start()

    def sum_third(s):
        order = STREAMS[s][2]
        for j in (1, 2, 3):
            hop(s, 2, j).wait()
        total = second_sum[s][me[order[2]]].astype(F32)
        for j in range(3):
            total += third_got[s][j].astype(F32)
        return total

    for s in (0, 1, 2):
        sum_first(s)
    for s in (0, 1, 2):
        sum_second(s)
    small_wait(1)
    loss[...] = jnp.broadcast_to(jnp.sum(totals[:, :, 0:1]) / labelled_count, (1, 1))
    grad_one[:, :256] = sum_third(0)
    grad_one[:, 256:] = sum_third(1)
    grad_two[...] = sum_third(2)[:, :C]


def sds(shape, dtype):
    return jax.ShapeDtypeStruct(shape, dtype)


def on_device(features, w_one, w_two, self_two, edge_src, edge_dst, send_rows, send_count, labels):
    vm = pl.BlockSpec(memory_space=pltpu.VMEM)
    hbm = pl.BlockSpec(memory_space=pl.ANY)
    V = pltpu.VMEM
    widths = [s[1] for s in STREAMS]
    scratch = [
        V((REL + 1, D, D), BF), V((REL, C, D), BF), V((C, D), BF),
        V((REL, N, TABLE), BF), V((REL, TABLE, N), BF), V((REL, N, 128), F32),
        V((FAR, N), BF), V((N, FAR), BF),
        V((PEERS, SLOTS, D), BF), V((PEERS, SLOTS, D), BF), V((PEERS, SLOTS, D), BF),
        V((PEERS, SLOTS, D), BF),
        V((REL, N, D), BF), V(((REL + 1) * D, N), BF), V(((REL + 1) * D, N), BF),
        V((N, D), F32), V((N, D), BF), V((N, C), F32), V((TABLE, D), F32),
        V((N, CP), BF), V((N, D), BF), V((N, CP), F32),
        V((2, 1, 128), F32), V((PEERS, 1, 128), F32), V((PEERS, 1, 128), F32),
        V((4, 4, 4, 2, ROWS, WIDE), BF), V((4, 4, 4, ROWS, WIDE), BF), V((4, 4, 4, ROWS, WIDE), BF),
        *[V((3, 4, 4, ROWS, w), BF) for w in widths],
        *[V((4, 4, ROWS, w), BF) for w in widths],
        *[V((3, 4, ROWS, w), BF) for w in widths],
        *[V((4, ROWS, w), BF) for w in widths],
        *[V((3, ROWS, w), BF) for w in widths],
        pltpu.SemaphoreType.DMA((3,)),
        pltpu.SemaphoreType.DMA((3,)), pltpu.SemaphoreType.DMA((3,)),
        pltpu.SemaphoreType.DMA((2,)), pltpu.SemaphoreType.DMA((2,)),
        pltpu.SemaphoreType.DMA((5,)), pltpu.SemaphoreType.DMA((5,)),
        pltpu.SemaphoreType.DMA((27,)), pltpu.SemaphoreType.DMA((27,)),
    ]
    logits_t, loss, grad_one, grad_two = pl.pallas_call(
        step_body,
        name="step",
        in_specs=[vm, hbm, hbm, hbm, vm, vm, vm, vm, vm],
        out_specs=[vm, vm, vm, vm],
        out_shape=[sds((C, N), F32), sds((1, 1), F32), sds((ROWS, D), F32), sds((ROWS, C), F32)],
        scratch_shapes=scratch,
        compiler_params=pltpu.CompilerParams(
            collective_id=0, has_side_effects=True, vmem_limit_bytes=62 * MB
        ),
    )(
        features, w_one, jnp.swapaxes(w_two, 1, 2), self_two.T, edge_src, edge_dst, send_rows[0],
        send_count, labels.reshape(1, N),
    )
    return (logits_t.T, loss[0, 0], grad_one, grad_two)


def solution(mesh):
    split = Mesh(mesh.devices.reshape(SIZES), DOM)
    return jax.shard_map(
        on_device,
        mesh=split,
        in_specs=(
            P(DOM, None),
            P(),
            P(),
            P(),
            P(None, DOM, None),
            P(None, DOM, None),
            P(DOM, None, None),
            P(DOM, None),
            P(DOM),
        ),
        out_specs=(P(DOM, None), P(), P(DOM, None), P(DOM, None)),
        check_vma=False,
    )
```

```python
import jax
import jax.numpy as jnp
from jax import lax
from jax.experimental import pallas as pl
from jax.experimental.pallas import tpu as pltpu
from jax.sharding import Mesh
from jax.sharding import PartitionSpec as P

DOM = ("dom_0", "dom_1", "dom_2", "dom_3")
SIZES = (4, 4, 4, 2)
BF = jnp.bfloat16
F32 = jnp.float32
I32 = jnp.int32
MESH = pl.DeviceIdType.MESH
loss_scale = 256.0
MB = 1 << 20

PEERS = 128
CHIPS = 64
SLOTS = 8
REL = 8
N = 256
D = 512
C = 349
CP = 384
FAR = PEERS * SLOTS
TABLE = N + FAR
ROWS = 36
WIDE = D + CP
BLOCK = 16 * ROWS

STREAMS = ((0, 256, (0, 1, 2)), (256, 256, (1, 2, 0)), (512, 384, (2, 0, 1)))


def dot(a, b):
    return jnp.dot(a, b, preferred_element_type=F32)


def dot_nt(a, b):
    return lax.dot_general(a, b, (((1,), (1,)), ((), ())), preferred_element_type=F32)


def iota(shape, dim):
    return lax.broadcasted_iota(I32, shape, dim)


def hot(mask):
    return jnp.where(mask, 1.0, 0.0).astype(BF)


def phases():
    now = []

    def begin(name):
        if now:
            now.pop().__exit__(None, None, None)
        if name:
            now.append(jax.named_scope(name))
            now[0].__enter__()

    return begin


def step_body(
    own, w_one_hbm, w_two_hbm, w_self_hbm, src, dst, rows, count, labels,
    logits_t, loss, grad_one, grad_two,
    w_one, w_two, w_two_raw, turned, w_self, where_src, adj, adj_t, norm, picks, picks_t,
    send, got_one, got_two, sums, avg, avg_one_t, avg_two_t,
    pre, hidden, acc, own_grad, spreads, grad, grad_pre,
    small_out, counts, totals,
    parts, half, r1a, r1b, r1c, q_a, q_b, q_c, r2a, r2b, r2c, t_a, t_b, t_c, r3a, r3b, r3c,
    w_sems, a_send, a_recv, s_send, s_recv, p_send, p_recv, x_send, x_recv,
):
    begin = phases()
    me = [lax.axis_index(a) for a in DOM]
    mine = ((me[0] * 4 + me[1]) * 4 + me[2]) * 2 + me[3]
    core = me[3]

    begin("a_greet")
    loads = [
        pltpu.make_async_copy(w_one_hbm, w_one, w_sems.at[0]),
        pltpu.make_async_copy(w_self_hbm, w_self, w_sems.at[1]),
    ]

    def two_load(i):
        count = min(32, C - 32 * i)
        return pltpu.make_async_copy(
            w_two_hbm.at[pl.ds(32 * i, count)], w_two_raw.at[i % 4, pl.ds(0, count)],
            w_sems.at[2 + i % 4],
        )

    for load in loads + [two_load(i) for i in range(4)]:
        load.start()

    ahead = [[lax.rem(m + d, n) for d in range(n)] for m, n in zip(me, SIZES)]
    behind = [[lax.rem(m + n - d, n) for d in range(n)] for m, n in zip(me, SIZES)]

    def sixteen(hi, sign, body):
        q = lax.rem(hi, 4)
        d3 = lax.div(hi, 4)
        c = lax.rem(core + d3, 2)
        if sign > 0:
            ys = [lax.rem(me[2] + q + j, 4) for j in range(4)]
        else:
            ys = [lax.rem(me[2] + 8 - q - j, 4) for j in range(4)]
        near_axes = ahead if sign > 0 else behind
        for i in range(16):
            d0 = i % 4
            d1 = (i // 4 + d0) % 4
            if isinstance(hi, int) and hi == 0 and i == 0:
                continue
            body(hi * 16 + i, (near_axes[0][d0], near_axes[1][d1], ys[d1], c))

    def everyone(sign, body, start=0, stop=8):
        if start == 0:
            sixteen(0, sign, body)
            start = 1

        def loop(hi, carry):
            sixteen(hi, sign, body)
            return carry

        lax.fori_loop(start, stop, loop, 0)

    barrier = pltpu.get_barrier_semaphore()

    def greet(k, to):
        pl.semaphore_signal(barrier, inc=1, device_id=to, device_id_type=MESH)

    everyone(1, greet)

    begin("b_pack")
    spot = iota((FAR, 1), 0)
    block = spot >> 3
    e0 = block & 3
    e1 = ((block >> 2) + e0) & 3
    e2 = ((block >> 4) + e1) & 3
    peer = (
        (((me[0] + e0) & 3) << 5) + (((me[1] + e1) & 3) << 3) + (((me[2] + e2) & 3) << 1)
        + ((core + (block >> 6)) & 1)
    )
    peer_hot = peer == iota((FAR, PEERS), 1)
    by_peer = dot_nt(hot(peer_hot), rows[...].astype(F32).astype(BF))
    slot = spot & 7
    chosen = jnp.sum(jnp.where(slot == iota((FAR, SLOTS), 1), by_peer, 0.0), axis=1, keepdims=True)
    live = jnp.sum(
        jnp.where(peer_hot, jnp.broadcast_to(count[...], (FAR, PEERS)), 0).astype(F32),
        axis=1, keepdims=True,
    )
    row_of = jnp.where(slot.astype(F32) < live, chosen, -1.0).astype(I32)
    picks[...] = hot(row_of == iota((FAR, N), 1))

    def pack(values):
        send[...] = dot(picks[...], values).astype(BF).reshape(PEERS, SLOTS, D)

    pack(own[...])
    small_out[0] = jnp.broadcast_to(
        jnp.sum(jnp.where(labels[...] >= 0, 1.0, 0.0), axis=1, keepdims=True), (1, 128)
    )
    begin("c_barrier")
    pl.semaphore_wait(barrier, PEERS - 1)

    def sender(got, which, small, small_got):
        def one(k, to):
            pltpu.make_async_remote_copy(
                src_ref=send.at[k], dst_ref=got.at[k], send_sem=a_send.at[which],
                recv_sem=a_recv.at[which * 4 + k // 32], device_id=to, device_id_type=MESH,
            ).start()
            if small is not None:
                pltpu.make_async_remote_copy(
                    src_ref=small_out.at[small], dst_ref=small_got.at[k],
                    send_sem=s_send.at[small], recv_sem=s_recv.at[small],
                    device_id=to, device_id_type=MESH,
                ).start()

        return one

    def group_wait(got, which, g):
        part = pl.ds(0, 31 if g == 0 else 32)
        pltpu.make_async_copy(send.at[part], got.at[part], a_recv.at[which * 4 + g]).wait()

    rest = pl.ds(0, PEERS - 1)

    def sent_wait(got, which):
        pltpu.make_async_copy(send.at[rest], got.at[rest], a_send.at[which]).wait()

    def small_wait(which):
        pltpu.make_async_copy(counts.at[rest], totals.at[rest], s_send.at[which]).wait()
        pltpu.make_async_copy(counts.at[rest], totals.at[rest], s_recv.at[which]).wait()

    begin("d_send")
    everyone(1, sender(got_one, 0, 0, counts))
    got_one[0] = send[0]
    counts[0] = small_out[0]

    begin("e_adjacency")
    far_src = src[...] - N
    p = far_src >> 3
    o0 = (me[0] + 4 - (p >> 5)) & 3
    o1 = (me[1] + 4 - ((p >> 3) & 3)) & 3
    o2 = (me[2] + 4 - ((p >> 1) & 3)) & 3
    o3 = (core + 2 - (p & 1)) & 1
    block_of = o0 + (((o1 - o0) & 3) << 2) + (((o2 - o1) & 3) << 4) + (o3 << 6)
    where_src[...] = jnp.where(far_src >= 0, N + (block_of << 3) + (far_src & 7), src[...])

    def relation(r, carry):
        for b in range(2):
            at = slice(b * 128, (b + 1) * 128)
            dst_hot = hot(dst[r, b : b + 1, :] == iota((128, 256), 0))
            src_hot = hot(where_src[r, b : b + 1, :] == iota((TABLE, 256), 0))
            adj[r, at, :] = dot_nt(dst_hot, src_hot).astype(BF)
            live_edges = jnp.sum(dst_hot.astype(F32), axis=1, keepdims=True)
            norm[r, at, :] = jnp.broadcast_to(1.0 / jnp.maximum(live_edges, 1.0), (128, 128))
        return carry

    lax.fori_loop(0, REL, relation, 0)
    begin("f_local")

    def rows_of(got, g, count):
        return got[32 * g : 32 * (g + count)].reshape(256 * count, D)

    def columns(r, g, count):
        return adj[r, :, N + 256 * g : N + 256 * (g + count)]

    def gather_most(values, got, which):
        group_wait(got, which, 0)

        def near_rows(r, carry):
            sums[r] = dot(adj[r, :, :N], values[...]) + dot(columns(r, 0, 1), rows_of(got, 0, 1))
            return carry

        lax.fori_loop(0, REL, near_rows, 0)
        group_wait(got, which, 1)
        group_wait(got, which, 2)

        def middle_rows(r, carry):
            sums[r] += dot(columns(r, 1, 2), rows_of(got, 1, 2))
            return carry

        lax.fori_loop(0, REL, middle_rows, 0)

    def averaged(r, got):
        total = sums[r] + dot(columns(r, 3, 1), rows_of(got, 3, 1))
        return (total * norm[r, :, :1]).astype(BF)

    avg_one_t[REL * D :, :] = own[...].T
    for load in loads:
        load.wait()
    pre[...] = dot(own[...], w_one[REL])
    gather_most(own, got_one, 0)
    begin("g_wait")
    small_wait(0)
    labelled_count = jnp.sum(counts[:, :, 0:1])
    sent_wait(got_one, 0)
    group_wait(got_one, 0, 3)

    begin("h_first")

    def first(r, carry):
        a = averaged(r, got_one)
        avg[r] = a
        pre[...] += dot(a, w_one[r])
        return carry

    lax.fori_loop(0, REL, first, 0)
    hidden[...] = jnp.maximum(pre[...], 0.0).astype(BF)
    begin("i_pack")
    pack(hidden[...])
    everyone(1, sender(got_two, 1, None, None))
    got_two[0] = send[0]

    begin("j_turns")

    def turn(r, out):
        out[pl.ds(pl.multiple_of(r * D, D), D), :] = avg[r].T

    def relation_t(r, carry):
        for b in range(2):
            dst_hot = hot(dst[r, b : b + 1, :] == iota((128, 256), 0))
            src_hot = hot(where_src[r, b : b + 1, :] == iota((TABLE, 256), 0))
            lanes = pl.ds(pl.multiple_of(r * N + b * 128, 128), 128)
            adj_t[:, lanes] = dot_nt(src_hot, dst_hot).astype(BF)
        turn(r, avg_one_t)
        return carry

    lax.fori_loop(0, REL, relation_t, 0)
    begin("ja_weights")

    for i in range(11):
        two_load(i).wait()
        at = pl.ds(i * 32, 32)
        for j in range(4):
            lanes = slice(128 * j, 128 * (j + 1))
            turned[j % 2] = w_two_raw[i % 4, :, :, lanes].astype(F32).reshape(32 * REL, 128)
            for r in range(REL):
                w_two[r, at, lanes] = turned[j % 2, pl.ds(r, 32, stride=REL), :].astype(BF)
        if i + 4 < 11:
            two_load(i + 4).start()

    begin("jb_picks")
    picks_t[...] = picks[...].T
    avg_two_t[REL * D :, :] = hidden[...].T
    acc[:, :C] = dot_nt(hidden[...], w_self[...])
    lab = jnp.broadcast_to(labels[...], (128, N)).T[:, :1]
    begin("jc_gather")
    gather_most(hidden, got_two, 1)
    begin("k_wait")
    sent_wait(got_two, 1)
    group_wait(got_two, 1, 3)

    begin("l_second")

    def second(r, carry):
        a = averaged(r, got_two)
        avg[r] = a
        acc[:, :C] += dot_nt(a, w_two[r, :C, :])
        return carry

    lax.fori_loop(0, REL, second, 0)
    begin("m_soft")
    out = acc[:, :C]
    labelled = lab >= 0
    top = jnp.max(out, axis=1, keepdims=True)
    log_total = jnp.log(jnp.sum(jnp.exp(out - top), axis=1, keepdims=True)) + top
    label_hot = jnp.where(lab == iota((N, C), 1), 1.0, 0.0)
    picked = jnp.sum(out * label_hot, axis=1, keepdims=True)
    soft = jnp.exp(out - log_total)
    mask = jnp.where(labelled, 1.0, 0.0)
    grad[...] = jnp.zeros_like(grad)
    grad[:, :C] = (loss_scale * (soft - label_hot) * mask / labelled_count).astype(BF)
    small_out[1] = jnp.broadcast_to(
        jnp.sum(jnp.where(labelled, log_total - picked, 0.0), axis=0, keepdims=True), (1, 128)
    )

    begin("n_spread")

    def spread(r, carry):
        at = pl.ds(pl.multiple_of(r * N, N), N)
        spreads[at, :] = (dot(grad[:, :C], w_two[r, :C, :]) * norm[r, :, :1]).astype(BF)
        return carry

    lax.fori_loop(0, REL, spread, 0)
    begin("o_send")
    got_three = got_one
    back = sender(got_three, 2, 1, totals)
    for g in range(4):
        group = dot(adj_t[N + 256 * g : N + 256 * (g + 1), :], spreads[...])
        send[32 * g : 32 * (g + 1)] = group.astype(BF).reshape(32, SLOTS, D)
        everyone(-1, back, 2 * g, 2 * g + 2)
    got_three[0] = send[0]
    totals[0] = small_out[1]

    begin("p_two")
    partner = (me[0], me[1], me[2], 1 - core)

    def chunks(x, h, left, right, lanes):
        start = pl.multiple_of((x * 2 + h) * BLOCK, BLOCK)
        value = dot(left[pl.ds(start, BLOCK), :], right[...]).astype(BF)
        for j in range(16):
            to = (x, h * 2 + j // 8, (j // 2) % 4, j % 2)
            parts[(*to, slice(None), lanes)] = value[ROWS * j : ROWS * (j + 1), :]

    def to_partner(x, lanes, sem):
        return pltpu.make_async_remote_copy(
            src_ref=parts.at[x, :, :, 1 - core, :, lanes], dst_ref=half.at[x, :, :, :, lanes],
            send_sem=p_send.at[sem], recv_sem=p_recv.at[sem], device_id=partner,
            device_id_type=MESH,
        )

    def add_near(x, z, lanes):
        half[x, z, :, :, lanes] = (
            parts[x, z, :, core, :, lanes].astype(F32) + half[x, z, :, :, lanes].astype(F32)
        ).astype(BF)

    two_lanes = pl.ds(D, CP)
    one_lanes = pl.ds(0, D)

    def turn_two(r, carry):
        turn(r, avg_two_t)
        return carry

    lax.fori_loop(0, REL, turn_two, 0)

    def two_chunks(i, carry):
        chunks(i // 2, i % 2, avg_two_t, grad, two_lanes)
        return carry

    lax.fori_loop(0, 8, two_chunks, 0)
    two_copy = to_partner(slice(None), two_lanes, 4)
    two_copy.start()
    logits_t[...] = acc[...].T[:C, :]
    own_grad[...] = dot(adj_t[:N, :], spreads[...]) + dot(grad[:, :C], w_self[...])
    two_copy.wait()

    def add_two(i, carry):
        add_near(i // 4, i % 4, two_lanes)
        return carry

    lax.fori_loop(0, 16, add_two, 0)

    first_got = (r1a, r1b, r1c)
    first_sum = (q_a, q_b, q_c)
    second_got = (r2a, r2b, r2c)
    second_sum = (t_a, t_b, t_c)
    third_got = (r3a, r3b, r3c)

    def hop(s, phase, j):
        lane, width, order = STREAMS[s]
        axis = order[phase]
        k = lax.rem(me[axis] + j, 4)
        to = list(me)
        to[axis] = k
        if phase == 0:
            at = tuple(k if a == axis else slice(None) for a in range(3))
            ref = half.at[(*at, slice(None), pl.ds(lane, width))]
            got = first_got[s]
        elif phase == 1:
            left = sorted(order[1:])
            at = tuple(k if a == axis else slice(None) for a in left)
            ref = first_sum[s].at[at]
            got = second_got[s]
        else:
            ref = second_sum[s].at[k]
            got = third_got[s]
        sem = (s * 3 + phase) * 3 + j - 1
        return pltpu.make_async_remote_copy(
            src_ref=ref, dst_ref=got.at[j - 1], send_sem=x_send.at[sem], recv_sem=x_recv.at[sem],
            device_id=tuple(to), device_id_type=MESH,
        )

    begin("q_wait")
    sent_wait(got_three, 2)
    for g in range(4):
        group_wait(got_three, 2, g)
    for j in (2, 1, 3):
        hop(2, 0, j).start()

    begin("r_gradpre")
    grad_hidden = own_grad[...] + dot(picks_t[...], got_three[...].reshape(FAR, D))
    grad_pre[...] = jnp.where(pre[...] > 0.0, grad_hidden, 0.0).astype(BF)

    begin("s_one")
    for j in (1, 2, 3, 4):
        k = lax.rem(me[0] + j, 4)

        def one_chunks(i, carry):
            chunks(k, i, avg_one_t, grad_pre, one_lanes)
            return carry

        lax.fori_loop(0, 2, one_chunks, 0)
        to_partner(k, one_lanes, j - 1).start()
    begin("t_near")
    for j in (1, 2, 3, 4):
        k = lax.rem(me[0] + j, 4)
        to_partner(k, one_lanes, j - 1).wait()

        def add_one(i, carry):
            add_near(k, i, one_lanes)
            return carry

        lax.fori_loop(0, 4, add_one, 0)
        if j < 4:
            hop(0, 0, j).start()
    for j in (2, 1, 3):
        hop(1, 0, j).start()

    def wide(ref, at):
        return ref[at].astype(F32)

    def sum_first(s):
        lane, width, order = STREAMS[s]
        for j in (1, 2, 3):
            hop(s, 0, j).wait()

        def body(i, carry):
            at = [None, None, None]
            left = sorted(order[1:])
            at[order[0]] = me[order[0]]
            at[left[0]] = i
            at[left[1]] = slice(None)
            total = half[(*at, slice(None), pl.ds(lane, width))].astype(F32)
            for j in range(3):
                total += first_got[s][j, i].astype(F32)
            first_sum[s][i] = total.astype(BF)
            return carry

        lax.fori_loop(0, 4, body, 0)
        for j in (2, 1, 3):
            hop(s, 1, j).start()

    def sum_second(s):
        order = STREAMS[s][2]
        for j in (1, 2, 3):
            hop(s, 1, j).wait()
        m = me[order[1]]
        if order[1] < order[2]:
            total = first_sum[s][m].astype(F32)
        else:
            total = first_sum[s][:, m].astype(F32)
        for j in range(3):
            total += second_got[s][j].astype(F32)
        second_sum[s][...] = total.astype(BF)
        for j in (2, 1, 3):
            hop(s, 2, j).start()

    def sum_third(s):
        order = STREAMS[s][2]
        for j in (1, 2, 3):
            hop(s, 2, j).wait()
        total = second_sum[s][me[order[2]]].astype(F32)
        for j in range(3):
            total += third_got[s][j].astype(F32)
        return total

    begin("u_first")
    for s in (0, 1, 2):
        sum_first(s)
    begin("v_second")
    for s in (0, 1, 2):
        sum_second(s)
    begin("w_third")
    small_wait(1)
    loss[...] = jnp.broadcast_to(jnp.sum(totals[:, :, 0:1]) / labelled_count, (1, 1))
    grad_one[:, :256] = sum_third(0)
    grad_one[:, 256:] = sum_third(1)
    grad_two[...] = sum_third(2)[:, :C]
    begin(None)


def finish_body(a, b, c, d, a_out, b_out, c_out, d_out):
    a_out[...] = a[...]
    b_out[...] = b[...]
    c_out[...] = c[...]
    d_out[...] = d[...]


def sds(shape, dtype):
    return jax.ShapeDtypeStruct(shape, dtype)


def on_device(features, w_one, w_two, self_two, edge_src, edge_dst, send_rows, send_count, labels):
    vm = pl.BlockSpec(memory_space=pltpu.VMEM)
    hbm = pl.BlockSpec(memory_space=pl.ANY)
    V = pltpu.VMEM
    widths = [s[1] for s in STREAMS]
    scratch = [
        V((REL + 1, D, D), BF), V((REL, 352, D), BF), V((4, 32, REL, D), BF), V((2, 256, 128), F32),
        V((C, D), BF), V((REL, 2, N), I32),
        V((REL, N, TABLE), BF), V((TABLE, REL * N), BF), V((REL, N, 128), F32),
        V((FAR, N), BF), V((N, FAR), BF),
        V((PEERS, SLOTS, D), BF), V((PEERS, SLOTS, D), BF), V((PEERS, SLOTS, D), BF),
        V((REL, N, D), F32), V((REL, N, D), BF), V(((REL + 1) * D, N), BF), V(((REL + 1) * D, N), BF),
        V((N, D), F32), V((N, D), BF), V((N, CP), F32), V((N, D), F32),
        V((REL * N, D), BF),
        V((N, CP), BF), V((N, D), BF),
        V((2, 1, 128), F32), V((PEERS, 1, 128), F32), V((PEERS, 1, 128), F32),
        V((4, 4, 4, 2, ROWS, WIDE), BF), V((4, 4, 4, ROWS, WIDE), BF),
        *[V((3, 4, 4, ROWS, w), BF) for w in widths],
        *[V((4, 4, ROWS, w), BF) for w in widths],
        *[V((3, 4, ROWS, w), BF) for w in widths],
        *[V((4, ROWS, w), BF) for w in widths],
        *[V((3, ROWS, w), BF) for w in widths],
        pltpu.SemaphoreType.DMA((6,)),
        pltpu.SemaphoreType.DMA((3,)), pltpu.SemaphoreType.DMA((12,)),
        pltpu.SemaphoreType.DMA((2,)), pltpu.SemaphoreType.DMA((2,)),
        pltpu.SemaphoreType.DMA((5,)), pltpu.SemaphoreType.DMA((5,)),
        pltpu.SemaphoreType.DMA((27,)), pltpu.SemaphoreType.DMA((27,)),
    ]
    logits_t, loss, grad_one, grad_two = pl.pallas_call(
        step_body,
        name="step",
        in_specs=[vm, hbm, hbm, hbm, vm, vm, vm, vm, vm],
        out_specs=[vm, vm, vm, vm],
        out_shape=[sds((C, N), F32), sds((1, 1), F32), sds((ROWS, D), F32), sds((ROWS, C), F32)],
        scratch_shapes=scratch,
        compiler_params=pltpu.CompilerParams(
            collective_id=0, has_side_effects=True, vmem_limit_bytes=63 * MB
        ),
    )(
        features, w_one, jnp.transpose(w_two, (2, 0, 1)), self_two.T, edge_src, edge_dst,
        send_rows[0].T, send_count, labels.reshape(1, N),
    )
    logits_t, loss, grad_one, grad_two = pl.pallas_call(
        finish_body,
        name="finish",
        in_specs=[vm] * 4,
        out_specs=[vm] * 4,
        out_shape=[sds((C, N), F32), sds((1, 1), F32), sds((ROWS, D), F32), sds((ROWS, C), F32)],
        compiler_params=pltpu.CompilerParams(vmem_limit_bytes=4 * MB),
    )(logits_t, loss, grad_one, grad_two)
    return (logits_t.T, loss[0, 0], grad_one, grad_two)


def solution(mesh):
    split = Mesh(mesh.devices.reshape(SIZES), DOM)
    return jax.shard_map(
        on_device,
        mesh=split,
        in_specs=(
            P(DOM, None),
            P(),
            P(),
            P(),
            P(None, DOM, None),
            P(None, DOM, None),
            P(DOM, None, None),
            P(DOM, None),
            P(DOM),
        ),
        out_specs=(P(DOM, None), P(), P(DOM, None), P(DOM, None)),
        check_vma=False,
    )
```

```python
import jax
import jax.numpy as jnp
import numpy as np
from jax import lax
from jax.experimental import pallas as pl
from jax.experimental.pallas import tpu as pltpu
from jax.sharding import Mesh
from jax.sharding import PartitionSpec as P

DOM = ("dom_0", "dom_1", "dom_2", "dom_3")
SIZES = (4, 4, 4, 2)
BF = jnp.bfloat16
F32 = jnp.float32
I32 = jnp.int32
MESH = pl.DeviceIdType.MESH
loss_scale = 256.0
MB = 1 << 20

PEERS = 128
CHIPS = 64
SLOTS = 8
REL = 8
N = 256
D = 512
C = 349
CP = 384
FAR = PEERS * SLOTS
TABLE = N + FAR
ROWS = 36
WIDE = D + CP
BLOCK = 16 * ROWS

STREAMS = ((0, 256, (0, 1, 2)), (256, 256, (1, 2, 0)), (512, 384, (2, 0, 1)))


def hops(code):
    return sum(min(d, 4 - d) for d in digits(code)[:3])


def digits(code):
    return (code % 4, code // 4 % 4, code // 16 % 4, code // 64)


def block_order():
    spread = []
    for k in range(1, PEERS):
        d0 = k % 4
        d1 = (k // 4 + d0) % 4
        d2 = (k // 16 + d1) % 4
        spread.append(d0 + 4 * d1 + 16 * d2 + 64 * (k // 64))
    return [0] + sorted(spread, key=lambda code: -hops(code))


ORDER = block_order()


def dot(a, b):
    return jnp.dot(a, b, preferred_element_type=F32)


def dot_nt(a, b):
    return lax.dot_general(a, b, (((1,), (1,)), ((), ())), preferred_element_type=F32)


def iota(shape, dim):
    return lax.broadcasted_iota(I32, shape, dim)


def hot(mask):
    return jnp.where(mask, 1.0, 0.0).astype(BF)


def phases():
    now = []

    def begin(name):
        if now:
            now.pop().__exit__(None, None, None)
        if name:
            now.append(jax.named_scope(name))
            now[0].__enter__()

    return begin


def step_body(
    own, w_one_hbm, w_two_hbm, w_self_hbm, src, dst, rows, count, labels, codes,
    logits_t, loss, grad_one, grad_two,
    w_one, w_two, w_two_raw, turned, w_self, where_src, row_code, adj, adj_t, norm, picks, picks_t,
    send, got_one, got_two, sums, avg, avg_one_t, avg_two_t,
    pre, hidden, acc, own_grad, spreads, grad, grad_pre,
    small_out, counts, totals,
    parts, half, r1a, r1b, r1c, q_a, q_b, q_c, r2a, r2b, r2c, t_a, t_b, t_c, r3a, r3b, r3c,
    w_sems, a_send, a_recv, s_send, s_recv, p_send, p_recv, x_send, x_recv,
):
    begin = phases()
    me = [lax.axis_index(a) for a in DOM]
    mine = ((me[0] * 4 + me[1]) * 4 + me[2]) * 2 + me[3]
    core = me[3]

    begin("a_greet")
    loads = [
        pltpu.make_async_copy(w_one_hbm, w_one, w_sems.at[0]),
        pltpu.make_async_copy(w_self_hbm, w_self, w_sems.at[1]),
    ]

    def two_load(i):
        count = min(32, C - 32 * i)
        return pltpu.make_async_copy(
            w_two_hbm.at[pl.ds(32 * i, count)], w_two_raw.at[i % 4, pl.ds(0, count)],
            w_sems.at[2 + i % 4],
        )

    for load in loads + [two_load(i) for i in range(4)]:
        load.start()

    ahead = [[lax.rem(m + d, n) for d in range(n)] for m, n in zip(me, SIZES)]
    behind = [[lax.rem(m + n - d, n) for d in range(n)] for m, n in zip(me, SIZES)]

    def everyone(where, body, start=1, stop=PEERS):
        for k in range(start, stop):
            body(k, tuple(where[i][d] for i, d in enumerate(digits(ORDER[k]))))

    barrier = pltpu.get_barrier_semaphore()

    def greet(k, to):
        pl.semaphore_signal(barrier, inc=1, device_id=to, device_id_type=MESH)

    everyone(ahead, greet)

    begin("b_pack")
    row_code[...] = jnp.broadcast_to(codes[...], (TABLE, 128))
    spot = codes[N:, :] - N
    code = spot >> 3
    peer = (
        (((me[0] + code) & 3) << 5) + (((me[1] + (code >> 2)) & 3) << 3)
        + (((me[2] + (code >> 4)) & 3) << 1) + ((core + (code >> 6)) & 1)
    )
    peer_hot = peer == iota((FAR, PEERS), 1)
    by_peer = dot_nt(hot(peer_hot), rows[...].astype(F32).astype(BF))
    slot = spot & 7
    chosen = jnp.sum(jnp.where(slot == iota((FAR, SLOTS), 1), by_peer, 0.0), axis=1, keepdims=True)
    live = jnp.sum(
        jnp.where(peer_hot, jnp.broadcast_to(count[...], (FAR, PEERS)), 0).astype(F32),
        axis=1, keepdims=True,
    )
    row_of = jnp.where(slot.astype(F32) < live, chosen, -1.0).astype(I32)
    picks[...] = hot(row_of == iota((FAR, N), 1))

    def pack(values):
        send[...] = dot(picks[...], values).astype(BF).reshape(PEERS, SLOTS, D)

    pack(own[...])
    small_out[0] = jnp.broadcast_to(
        jnp.sum(jnp.where(labels[...] >= 0, 1.0, 0.0), axis=1, keepdims=True), (1, 128)
    )
    begin("c_barrier")
    pl.semaphore_wait(barrier, PEERS - 1)

    def sender(got, which, small, small_got):
        def one(k, to):
            pltpu.make_async_remote_copy(
                src_ref=send.at[k], dst_ref=got.at[k], send_sem=a_send.at[which],
                recv_sem=a_recv.at[which * 4 + k // 32], device_id=to, device_id_type=MESH,
            ).start()
            if small is not None:
                pltpu.make_async_remote_copy(
                    src_ref=small_out.at[small], dst_ref=small_got.at[k],
                    send_sem=s_send.at[small], recv_sem=s_recv.at[small],
                    device_id=to, device_id_type=MESH,
                ).start()

        return one

    def group_wait(got, which, g):
        part = pl.ds(0, 31 if g == 0 else 32)
        pltpu.make_async_copy(send.at[part], got.at[part], a_recv.at[which * 4 + g]).wait()

    rest = pl.ds(0, PEERS - 1)

    def sent_wait(got, which):
        pltpu.make_async_copy(send.at[rest], got.at[rest], a_send.at[which]).wait()

    def small_wait(which):
        pltpu.make_async_copy(counts.at[rest], totals.at[rest], s_send.at[which]).wait()
        pltpu.make_async_copy(counts.at[rest], totals.at[rest], s_recv.at[which]).wait()

    begin("d_send")
    everyone(ahead, sender(got_one, 0, 0, counts))
    got_one[0] = send[0]
    counts[0] = small_out[0]

    begin("e_adjacency")
    far_src = src[...] - N
    p = far_src >> 3
    o0 = (me[0] + 4 - (p >> 5)) & 3
    o1 = (me[1] + 4 - ((p >> 3) & 3)) & 3
    o2 = (me[2] + 4 - ((p >> 1) & 3)) & 3
    o3 = (core + 2 - (p & 1)) & 1
    code_of = o0 + (o1 << 2) + (o2 << 4) + (o3 << 6)
    where_src[...] = jnp.where(far_src >= 0, N + (code_of << 3) + (far_src & 7), src[...])

    def source_hot(r, b):
        halves = [
            hot(where_src[r, b : b + 1, 128 * i : 128 * (i + 1)] == row_code[...]) for i in range(2)
        ]
        return jnp.concatenate(halves, axis=1)

    def relation(r, carry):
        for b in range(2):
            at = slice(b * 128, (b + 1) * 128)
            dst_hot = hot(dst[r, b : b + 1, :] == iota((128, 256), 0))
            src_hot = source_hot(r, b)
            adj[r, at, :] = dot_nt(dst_hot, src_hot).astype(BF)
            live_edges = jnp.sum(dst_hot.astype(F32), axis=1, keepdims=True)
            norm[r, at, :] = jnp.broadcast_to(1.0 / jnp.maximum(live_edges, 1.0), (128, 128))
        return carry

    lax.fori_loop(0, REL, relation, 0)
    begin("f_local")

    def rows_of(got, g, count):
        return got[32 * g : 32 * (g + count)].reshape(256 * count, D)

    def columns(r, g, count):
        return adj[r, :, N + 256 * g : N + 256 * (g + count)]

    def gather_most(values, got, which):
        group_wait(got, which, 0)

        def near_rows(r, carry):
            sums[r] = dot(adj[r, :, :N], values[...]) + dot(columns(r, 0, 1), rows_of(got, 0, 1))
            return carry

        lax.fori_loop(0, REL, near_rows, 0)
        group_wait(got, which, 1)

        def middle_rows(r, carry):
            sums[r] += dot(columns(r, 1, 1), rows_of(got, 1, 1))
            return carry

        lax.fori_loop(0, REL, middle_rows, 0)

    def averaged(r, got):
        total = sums[r] + dot(columns(r, 2, 2), rows_of(got, 2, 2))
        return (total * norm[r, :, :1]).astype(BF)

    avg_one_t[REL * D :, :] = own[...].T
    for load in loads:
        load.wait()
    pre[...] = dot(own[...], w_one[REL])
    gather_most(own, got_one, 0)
    begin("g_wait")
    small_wait(0)
    labelled_count = jnp.sum(counts[:, :, 0:1])
    sent_wait(got_one, 0)
    group_wait(got_one, 0, 2)
    group_wait(got_one, 0, 3)

    begin("h_first")

    def first(r, carry):
        a = averaged(r, got_one)
        avg[r] = a
        pre[...] += dot(a, w_one[r])
        return carry

    lax.fori_loop(0, REL, first, 0)
    hidden[...] = jnp.maximum(pre[...], 0.0).astype(BF)
    begin("i_pack")
    pack(hidden[...])
    everyone(ahead, sender(got_two, 1, None, None))
    got_two[0] = send[0]

    begin("j_turns")

    def turn(r, out):
        out[pl.ds(pl.multiple_of(r * D, D), D), :] = avg[r].T

    def relation_t(r, carry):
        for b in range(2):
            dst_hot = hot(dst[r, b : b + 1, :] == iota((128, 256), 0))
            src_hot = source_hot(r, b)
            lanes = pl.ds(pl.multiple_of(r * N + b * 128, 128), 128)
            adj_t[:, lanes] = dot_nt(src_hot, dst_hot).astype(BF)
        turn(r, avg_one_t)
        return carry

    lax.fori_loop(0, REL, relation_t, 0)
    begin("ja_weights")

    for i in range(11):
        two_load(i).wait()
        at = pl.ds(i * 32, 32)
        for j in range(4):
            lanes = slice(128 * j, 128 * (j + 1))
            turned[j % 2] = w_two_raw[i % 4, :, :, lanes].astype(F32).reshape(32 * REL, 128)
            for r in range(REL):
                w_two[r, at, lanes] = turned[j % 2, pl.ds(r, 32, stride=REL), :].astype(BF)
        if i + 4 < 11:
            two_load(i + 4).start()

    begin("jb_picks")
    picks_t[...] = picks[...].T
    avg_two_t[REL * D :, :] = hidden[...].T
    acc[:, :C] = dot_nt(hidden[...], w_self[...])
    lab = jnp.broadcast_to(labels[...], (128, N)).T[:, :1]
    begin("jc_gather")
    gather_most(hidden, got_two, 1)
    begin("k_wait")
    sent_wait(got_two, 1)
    group_wait(got_two, 1, 2)
    group_wait(got_two, 1, 3)

    begin("l_second")

    def second(r, carry):
        a = averaged(r, got_two)
        avg[r] = a
        acc[:, :C] += dot_nt(a, w_two[r, :C, :])
        return carry

    lax.fori_loop(0, REL, second, 0)
    begin("m_soft")
    out = acc[:, :C]
    labelled = lab >= 0
    top = jnp.max(out, axis=1, keepdims=True)
    log_total = jnp.log(jnp.sum(jnp.exp(out - top), axis=1, keepdims=True)) + top
    label_hot = jnp.where(lab == iota((N, C), 1), 1.0, 0.0)
    picked = jnp.sum(out * label_hot, axis=1, keepdims=True)
    soft = jnp.exp(out - log_total)
    mask = jnp.where(labelled, 1.0, 0.0)
    grad[...] = jnp.zeros_like(grad)
    grad[:, :C] = (loss_scale * (soft - label_hot) * mask / labelled_count).astype(BF)
    small_out[1] = jnp.broadcast_to(
        jnp.sum(jnp.where(labelled, log_total - picked, 0.0), axis=0, keepdims=True), (1, 128)
    )

    begin("n_spread")

    def spread(r, carry):
        at = pl.ds(pl.multiple_of(r * N, N), N)
        spreads[at, :] = (dot(grad[:, :C], w_two[r, :C, :]) * norm[r, :, :1]).astype(BF)
        return carry

    lax.fori_loop(0, REL, spread, 0)
    begin("o_send")
    got_three = got_one
    back = sender(got_three, 2, 1, totals)
    for g in range(4):
        group = dot(adj_t[N + 256 * g : N + 256 * (g + 1), :], spreads[...])
        send[32 * g : 32 * (g + 1)] = group.astype(BF).reshape(32, SLOTS, D)
        everyone(behind, back, max(1, 32 * g), 32 * (g + 1))
    got_three[0] = send[0]
    totals[0] = small_out[1]

    begin("p_two")
    partner = (me[0], me[1], me[2], 1 - core)

    def chunks(x, h, left, right, lanes):
        start = pl.multiple_of((x * 2 + h) * BLOCK, BLOCK)
        value = dot(left[pl.ds(start, BLOCK), :], right[...]).astype(BF)
        for j in range(16):
            to = (x, h * 2 + j // 8, (j // 2) % 4, j % 2)
            parts[(*to, slice(None), lanes)] = value[ROWS * j : ROWS * (j + 1), :]

    def to_partner(x, lanes, sem):
        return pltpu.make_async_remote_copy(
            src_ref=parts.at[x, :, :, 1 - core, :, lanes], dst_ref=half.at[x, :, :, :, lanes],
            send_sem=p_send.at[sem], recv_sem=p_recv.at[sem], device_id=partner,
            device_id_type=MESH,
        )

    def add_near(x, z, lanes):
        half[x, z, :, :, lanes] = (
            parts[x, z, :, core, :, lanes].astype(F32) + half[x, z, :, :, lanes].astype(F32)
        ).astype(BF)

    two_lanes = pl.ds(D, CP)
    one_lanes = pl.ds(0, D)

    def turn_two(r, carry):
        turn(r, avg_two_t)
        return carry

    lax.fori_loop(0, REL, turn_two, 0)

    def two_chunks(i, carry):
        chunks(i // 2, i % 2, avg_two_t, grad, two_lanes)
        return carry

    lax.fori_loop(0, 8, two_chunks, 0)
    two_copy = to_partner(slice(None), two_lanes, 4)
    two_copy.start()
    logits_t[...] = acc[...].T[:C, :]
    own_grad[...] = dot(adj_t[:N, :], spreads[...]) + dot(grad[:, :C], w_self[...])
    two_copy.wait()

    def add_two(i, carry):
        add_near(i // 4, i % 4, two_lanes)
        return carry

    lax.fori_loop(0, 16, add_two, 0)

    first_got = (r1a, r1b, r1c)
    first_sum = (q_a, q_b, q_c)
    second_got = (r2a, r2b, r2c)
    second_sum = (t_a, t_b, t_c)
    third_got = (r3a, r3b, r3c)

    def to_axis(axis, step):
        to = list(me)
        to[axis] = lax.rem(me[axis] + step, 4)
        return tuple(to), to[axis]

    def cut(s, upper):
        lane, width, _ = STREAMS[s]
        low = 128 * (width // 256)
        return (lane + low, low, width - low) if upper else (lane, 0, low)

    def first_at(s, k, lane, size):
        at = tuple(k if a == STREAMS[s][2][0] else slice(None) for a in range(3))
        return (*at, slice(None), pl.ds(lane, size))

    def first_hop(s, kind, forward):
        axis = STREAMS[s][2][0]
        to, k = to_axis(axis, 1 if forward else 3)
        lane, inner, size = cut(s, forward if kind == "own" else not forward)
        if kind == "far":
            k = lax.rem(me[axis] + 2, 4)
            slot = 2
        else:
            slot = 0 if forward else 1
        sem = s * 12 + {"far": 0, "own": 2, "both": 4}[kind] + (0 if forward else 1)
        return pltpu.make_async_remote_copy(
            src_ref=half.at[first_at(s, k, lane, size)],
            dst_ref=first_got[s].at[slot, :, :, :, pl.ds(inner, size)],
            send_sem=x_send.at[sem], recv_sem=x_recv.at[sem], device_id=to, device_id_type=MESH,
        )

    def relay(s):
        axis = STREAMS[s][2][0]
        for forward in (True, False):
            first_hop(s, "far", forward).wait()
            _, k = to_axis(axis, 1 if forward else 3)
            lane, inner, size = cut(s, not forward)
            at = first_at(s, k, lane, size)
            half[at] = (
                half[at].astype(F32) + first_got[s][2, :, :, :, inner : inner + size].astype(F32)
            ).astype(BF)
            first_hop(s, "both", forward).start()

    def hop(s, phase, j):
        order = STREAMS[s][2]
        axis = order[phase]
        to, k = to_axis(axis, j)
        if phase == 1:
            at = tuple(k if a == axis else slice(None) for a in sorted(order[1:]))
            ref = first_sum[s].at[at]
            got = second_got[s]
        else:
            ref = second_sum[s].at[k]
            got = third_got[s]
        sem = s * 12 + 3 + phase * 3 + j - 1
        return pltpu.make_async_remote_copy(
            src_ref=ref, dst_ref=got.at[j - 1], send_sem=x_send.at[sem], recv_sem=x_recv.at[sem],
            device_id=to, device_id_type=MESH,
        )

    def first_start(s):
        for kind in ("far", "own"):
            for forward in (True, False):
                first_hop(s, kind, forward).start()

    first_start(2)
    begin("q_wait")
    sent_wait(got_three, 2)
    for g in range(4):
        group_wait(got_three, 2, g)

    begin("r_gradpre")
    grad_hidden = own_grad[...] + dot(picks_t[...], got_three[...].reshape(FAR, D))
    grad_pre[...] = jnp.where(pre[...] > 0.0, grad_hidden, 0.0).astype(BF)

    begin("s_one")

    def one_block(j):
        k = lax.rem(me[0] + j, 4)

        def one_chunks(i, carry):
            chunks(k, i, avg_one_t, grad_pre, one_lanes)
            return carry

        lax.fori_loop(0, 2, one_chunks, 0)
        to_partner(k, one_lanes, j).start()

    def one_near(j):
        k = lax.rem(me[0] + j, 4)
        to_partner(k, one_lanes, j).wait()

        def add_one(i, carry):
            add_near(k, i, one_lanes)
            return carry

        lax.fori_loop(0, 4, add_one, 0)
        if j == 2:
            first_hop(0, "far", True).start()
            first_hop(0, "far", False).start()
        elif j:
            first_hop(0, "own", j == 1).start()

    one_block(2)
    one_block(1)
    one_near(2)
    one_block(3)
    one_near(1)
    one_block(0)
    begin("t_near")
    relay(2)
    one_near(3)
    one_near(0)
    first_start(1)
    relay(0)
    relay(1)

    def sum_first(s):
        lane, width, order = STREAMS[s]
        for kind in ("own", "both"):
            for forward in (True, False):
                first_hop(s, kind, forward).wait()

        def body(i, carry):
            at = [None, None, None]
            left = sorted(order[1:])
            at[order[0]] = me[order[0]]
            at[left[0]] = i
            at[left[1]] = slice(None)
            total = half[(*at, slice(None), pl.ds(lane, width))].astype(F32)
            for j in range(2):
                total += first_got[s][j, i].astype(F32)
            first_sum[s][i] = total.astype(BF)
            return carry

        lax.fori_loop(0, 4, body, 0)
        for j in (2, 1, 3):
            hop(s, 1, j).start()

    def sum_second(s):
        order = STREAMS[s][2]
        for j in (1, 2, 3):
            hop(s, 1, j).wait()
        m = me[order[1]]
        if order[1] < order[2]:
            total = first_sum[s][m].astype(F32)
        else:
            total = first_sum[s][:, m].astype(F32)
        for j in range(3):
            total += second_got[s][j].astype(F32)
        second_sum[s][...] = total.astype(BF)
        for j in (2, 1, 3):
            hop(s, 2, j).start()

    def sum_third(s):
        order = STREAMS[s][2]
        for j in (1, 2, 3):
            hop(s, 2, j).wait()
        total = second_sum[s][me[order[2]]].astype(F32)
        for j in range(3):
            total += third_got[s][j].astype(F32)
        return total

    begin("u_first")
    for s in (2, 0, 1):
        sum_first(s)
    begin("v_second")
    for s in (2, 0, 1):
        sum_second(s)
    begin("w_third")
    small_wait(1)
    loss[...] = jnp.broadcast_to(jnp.sum(totals[:, :, 0:1]) / labelled_count, (1, 1))
    grad_one[:, :256] = sum_third(0)
    grad_one[:, 256:] = sum_third(1)
    grad_two[...] = sum_third(2)[:, :C]
    begin(None)


def finish_body(a, b, c, d, a_out, b_out, c_out, d_out):
    a_out[...] = a[...]
    b_out[...] = b[...]
    c_out[...] = c[...]
    d_out[...] = d[...]


def sds(shape, dtype):
    return jax.ShapeDtypeStruct(shape, dtype)


def on_device(features, w_one, w_two, self_two, edge_src, edge_dst, send_rows, send_count, labels):
    vm = pl.BlockSpec(memory_space=pltpu.VMEM)
    hbm = pl.BlockSpec(memory_space=pl.ANY)
    V = pltpu.VMEM
    widths = [s[1] for s in STREAMS]
    scratch = [
        V((REL + 1, D, D), BF), V((REL, 352, D), BF), V((4, 32, REL, D), BF), V((2, 256, 128), F32),
        V((C, D), BF), V((REL, 2, N), I32), V((TABLE, 128), I32),
        V((REL, N, TABLE), BF), V((TABLE, REL * N), BF), V((REL, N, 128), F32),
        V((FAR, N), BF), V((N, FAR), BF),
        V((PEERS, SLOTS, D), BF), V((PEERS, SLOTS, D), BF), V((PEERS, SLOTS, D), BF),
        V((REL, N, D), F32), V((REL, N, D), BF), V(((REL + 1) * D, N), BF), V(((REL + 1) * D, N), BF),
        V((N, D), F32), V((N, D), BF), V((N, CP), F32), V((N, D), F32),
        V((REL * N, D), BF),
        V((N, CP), BF), V((N, D), BF),
        V((2, 1, 128), F32), V((PEERS, 1, 128), F32), V((PEERS, 1, 128), F32),
        V((4, 4, 4, 2, ROWS, WIDE), BF), V((4, 4, 4, ROWS, WIDE), BF),
        *[V((3, 4, 4, ROWS, w), BF) for w in widths],
        *[V((4, 4, ROWS, w), BF) for w in widths],
        *[V((3, 4, ROWS, w), BF) for w in widths],
        *[V((4, ROWS, w), BF) for w in widths],
        *[V((3, ROWS, w), BF) for w in widths],
        pltpu.SemaphoreType.DMA((6,)),
        pltpu.SemaphoreType.DMA((3,)), pltpu.SemaphoreType.DMA((12,)),
        pltpu.SemaphoreType.DMA((2,)), pltpu.SemaphoreType.DMA((2,)),
        pltpu.SemaphoreType.DMA((5,)), pltpu.SemaphoreType.DMA((5,)),
        pltpu.SemaphoreType.DMA((36,)), pltpu.SemaphoreType.DMA((36,)),
    ]
    codes = np.concatenate(
        [np.arange(N)] + [N + SLOTS * code + np.arange(SLOTS) for code in ORDER]
    ).astype(np.int32)
    logits_t, loss, grad_one, grad_two = pl.pallas_call(
        step_body,
        name="step",
        in_specs=[vm, hbm, hbm, hbm, vm, vm, vm, vm, vm, vm],
        out_specs=[vm, vm, vm, vm],
        out_shape=[sds((C, N), F32), sds((1, 1), F32), sds((ROWS, D), F32), sds((ROWS, C), F32)],
        scratch_shapes=scratch,
        compiler_params=pltpu.CompilerParams(
            collective_id=0, has_side_effects=True, vmem_limit_bytes=63 * MB
        ),
    )(
        features, w_one, jnp.transpose(w_two, (2, 0, 1)), self_two.T, edge_src, edge_dst,
        send_rows[0].T, send_count, labels.reshape(1, N),
        jnp.asarray(codes).reshape(TABLE, 1),
    )
    logits_t, loss, grad_one, grad_two = pl.pallas_call(
        finish_body,
        name="finish",
        in_specs=[vm] * 4,
        out_specs=[vm] * 4,
        out_shape=[sds((C, N), F32), sds((1, 1), F32), sds((ROWS, D), F32), sds((ROWS, C), F32)],
        compiler_params=pltpu.CompilerParams(vmem_limit_bytes=4 * MB),
    )(logits_t, loss, grad_one, grad_two)
    return (logits_t.T, loss[0, 0], grad_one, grad_two)


def solution(mesh):
    split = Mesh(mesh.devices.reshape(SIZES), DOM)
    return jax.shard_map(
        on_device,
        mesh=split,
        in_specs=(
            P(DOM, None),
            P(),
            P(),
            P(),
            P(None, DOM, None),
            P(None, DOM, None),
            P(DOM, None, None),
            P(DOM, None),
            P(DOM),
        ),
        out_specs=(P(DOM, None), P(), P(DOM, None), P(DOM, None)),
        check_vma=False,
    )
```

```python
import jax
import jax.numpy as jnp
import numpy as np
from jax import lax
from jax.experimental import pallas as pl
from jax.experimental.pallas import tpu as pltpu
from jax.sharding import Mesh
from jax.sharding import PartitionSpec as P

DOM = ("dom_0", "dom_1", "dom_2", "dom_3")
SIZES = (4, 4, 4, 2)
BF = jnp.bfloat16
F32 = jnp.float32
I32 = jnp.int32
MESH = pl.DeviceIdType.MESH
loss_scale = 256.0
MB = 1 << 20
VLIM = 63
UNROLL = 4

PEERS = 128
CHIPS = 64
SLOTS = 8
REL = 8
N = 256
D = 512
C = 349
CP = 384
FAR = PEERS * SLOTS
TABLE = N + FAR
ROWS = 36
WIDE = D + CP
BLOCK = 16 * ROWS

STREAMS = (
    (0, 0, 36, (0, 1, 2)),
    (384, 0, 16, (0, 1, 2)),
    (128, 0, 36, (1, 2, 0)),
    (384, 16, 20, (1, 2, 0)),
    (256, 0, 36, (2, 0, 1)),
    (512, 0, 36, (0, 1, 2)),
    (640, 0, 36, (1, 2, 0)),
    (768, 0, 36, (2, 0, 1)),
)
ONE_X, ONE_REST, TWO = (0, 1), (2, 3, 4), (5, 6, 7)


def hops(code):
    return sum(min(d, 4 - d) for d in digits(code)[:3])


def digits(code):
    return (code % 4, code // 4 % 4, code // 16 % 4, code // 64)


def block_order():
    spread = []
    for k in range(1, PEERS):
        d0 = k % 4
        d1 = (k // 4 + d0) % 4
        d2 = (k // 16 + d1) % 4
        spread.append(d0 + 4 * d1 + 16 * d2 + 64 * (k // 64))
    return [0] + sorted(spread, key=lambda code: -hops(code))


ORDER = block_order()


def dot(a, b):
    return jnp.dot(a, b, preferred_element_type=F32)


def dot_nt(a, b):
    return lax.dot_general(a, b, (((1,), (1,)), ((), ())), preferred_element_type=F32)


def iota(shape, dim):
    return lax.broadcasted_iota(I32, shape, dim)


def hot(mask):
    return jnp.where(mask, 1.0, 0.0).astype(BF)


def phases():
    now = []

    def begin(name):
        if now:
            now.pop().__exit__(None, None, None)
        if name:
            now.append(jax.named_scope(name))
            now[0].__enter__()

    return begin


def step_body(
    own_hbm, w_one_hbm, w_two_hbm, w_self_hbm, src_hbm, dst_hbm, rows_hbm, count_hbm, labels_hbm,
    codes_hbm,
    logits_t, loss, grad_one, grad_two,
    own, src, dst, rows, count, labels, w_one, w_two, w_two_raw, turned, w_self, where_src, row_code, adj, adj_t, norm, picks, picks_t,
    send, got_one, got_two, sums, avg, avg_one_t, avg_two_t,
    pre, hidden, acc, logits_v, own_grad, spreads, grad, grad_pre,
    small_out, counts, totals,
    parts, half, *rest_refs,
):
    begin = phases()
    count_s = len(STREAMS)
    first_got, first_sum, second_got, second_sum, third_got = (
        rest_refs[i * count_s : (i + 1) * count_s] for i in range(5)
    )
    w_sems, a_send, a_recv, s_send, s_recv, p_send, p_recv, x_send, x_recv = rest_refs[5 * count_s :]
    me = [lax.axis_index(a) for a in DOM]
    mine = ((me[0] * 4 + me[1]) * 4 + me[2]) * 2 + me[3]
    core = me[3]

    begin("a_greet")
    loads = [
        pltpu.make_async_copy(w_one_hbm, w_one, w_sems.at[0]),
        pltpu.make_async_copy(w_self_hbm, w_self, w_sems.at[1]),
    ]

    def two_load(i):
        count = min(32, C - 32 * i)
        return pltpu.make_async_copy(
            w_two_hbm.at[pl.ds(32 * i, count)], w_two_raw.at[i % 4, pl.ds(0, count)],
            w_sems.at[2 + i % 4],
        )

    inputs = [
        pltpu.make_async_copy(a, b, w_sems.at[6 + i])
        for i, (a, b) in enumerate(
            (
                (codes_hbm, row_code), (rows_hbm, rows), (count_hbm, count), (own_hbm, own),
                (labels_hbm, labels), (src_hbm, src), (dst_hbm, dst),
            )
        )
    ]
    for load in inputs + loads + [two_load(i) for i in range(4)]:
        load.start()

    ahead = [[lax.rem(m + d, n) for d in range(n)] for m, n in zip(me, SIZES)]
    behind = [[lax.rem(m + n - d, n) for d in range(n)] for m, n in zip(me, SIZES)]

    def everyone(where, body, start=1, stop=PEERS):
        for k in range(start, stop):
            body(k, tuple(where[i][d] for i, d in enumerate(digits(ORDER[k]))))

    barrier = pltpu.get_barrier_semaphore()

    def greet(k, to):
        pl.semaphore_signal(barrier, inc=1, device_id=to, device_id_type=MESH)

    everyone(ahead, greet)

    begin("b_pack")
    for load in inputs:
        load.wait()
    spot = row_code[N:, :1] - N
    code = spot >> 3
    peer = (
        (((me[0] + code) & 3) << 5) + (((me[1] + (code >> 2)) & 3) << 3)
        + (((me[2] + (code >> 4)) & 3) << 1) + ((core + (code >> 6)) & 1)
    )
    peer_hot = peer == iota((FAR, PEERS), 1)
    by_peer = dot_nt(hot(peer_hot), rows[...].astype(F32).astype(BF))
    slot = spot & 7
    chosen = jnp.sum(jnp.where(slot == iota((FAR, SLOTS), 1), by_peer, 0.0), axis=1, keepdims=True)
    live = jnp.sum(
        jnp.where(peer_hot, jnp.broadcast_to(count[...], (FAR, PEERS)), 0).astype(F32),
        axis=1, keepdims=True,
    )
    row_of = jnp.where(slot.astype(F32) < live, chosen, -1.0).astype(I32)
    picks[...] = hot(row_of == iota((FAR, N), 1))

    def pack(values):
        send[...] = dot(picks[...], values).astype(BF).reshape(PEERS, SLOTS, D)

    pack(own[...])
    small_out[0] = jnp.broadcast_to(
        jnp.sum(jnp.where(labels[...] >= 0, 1.0, 0.0), axis=1, keepdims=True), (1, 128)
    )
    begin("c_barrier")
    pl.semaphore_wait(barrier, PEERS - 1)

    def sender(got, which):
        def one(k, to):
            pltpu.make_async_remote_copy(
                src_ref=send.at[k], dst_ref=got.at[k], send_sem=a_send.at[which],
                recv_sem=a_recv.at[which * 4 + k // 32], device_id=to, device_id_type=MESH,
            ).start()

        return one

    def small_sender(small, small_got):
        def one(k, to):
            pltpu.make_async_remote_copy(
                src_ref=small_out.at[small], dst_ref=small_got.at[k],
                send_sem=s_send.at[small], recv_sem=s_recv.at[small],
                device_id=to, device_id_type=MESH,
            ).start()

        return one

    def group_wait(got, which, g):
        part = pl.ds(0, 31 if g == 0 else 32)
        pltpu.make_async_copy(send.at[part], got.at[part], a_recv.at[which * 4 + g]).wait()

    rest = pl.ds(0, PEERS - 1)

    def sent_wait(got, which):
        pltpu.make_async_copy(send.at[rest], got.at[rest], a_send.at[which]).wait()

    def small_wait(which):
        pltpu.make_async_copy(counts.at[rest], totals.at[rest], s_send.at[which]).wait()
        pltpu.make_async_copy(counts.at[rest], totals.at[rest], s_recv.at[which]).wait()

    begin("d_send")
    everyone(ahead, sender(got_one, 0))
    got_one[0] = send[0]

    begin("e_adjacency")
    far_src = src[...] - N
    p = far_src >> 3
    o0 = (me[0] + 4 - (p >> 5)) & 3
    o1 = (me[1] + 4 - ((p >> 3) & 3)) & 3
    o2 = (me[2] + 4 - ((p >> 1) & 3)) & 3
    o3 = (core + 2 - (p & 1)) & 1
    code_of = o0 + (o1 << 2) + (o2 << 4) + (o3 << 6)
    where_src[...] = jnp.where(far_src >= 0, N + (code_of << 3) + (far_src & 7), src[...])

    def source_hot(r, b):
        halves = [
            hot(where_src[r, b : b + 1, 128 * i : 128 * (i + 1)] == row_code[...]) for i in range(2)
        ]
        return jnp.concatenate(halves, axis=1)

    def relation(r, carry):
        for b in range(2):
            at = slice(b * 128, (b + 1) * 128)
            dst_hot = hot(dst[r, b : b + 1, :] == iota((128, 256), 0))
            src_hot = source_hot(r, b)
            adj[r, at, :] = dot_nt(dst_hot, src_hot).astype(BF)
            live_edges = jnp.sum(dst_hot.astype(F32), axis=1, keepdims=True)
            norm[r, at, :] = jnp.broadcast_to(1.0 / jnp.maximum(live_edges, 1.0), (128, 128))
        return carry

    lax.fori_loop(0, REL, relation, 0, unroll=UNROLL)
    everyone(ahead, small_sender(0, counts))
    counts[0] = small_out[0]
    begin("f_local")

    def rows_of(got, g, count):
        return got[32 * g : 32 * (g + count)].reshape(256 * count, D)

    def columns(r, g, count):
        return adj[r, :, N + 256 * g : N + 256 * (g + count)]

    def gather_most(values, got, which):
        group_wait(got, which, 0)

        def near_rows(r, carry):
            sums[r] = dot(adj[r, :, :N], values[...]) + dot(columns(r, 0, 1), rows_of(got, 0, 1))
            return carry

        lax.fori_loop(0, REL, near_rows, 0, unroll=UNROLL)
        group_wait(got, which, 1)

        def middle_rows(r, carry):
            sums[r] += dot(columns(r, 1, 1), rows_of(got, 1, 1))
            return carry

        lax.fori_loop(0, REL, middle_rows, 0, unroll=UNROLL)

    def averaged(r, got):
        total = sums[r] + dot(columns(r, 2, 2), rows_of(got, 2, 2))
        return (total * norm[r, :, :1]).astype(BF)

    avg_one_t[REL * D :, :] = own[...].T
    for load in loads:
        load.wait()
    pre[...] = dot(own[...], w_one[REL])
    gather_most(own, got_one, 0)
    begin("g_wait")
    sent_wait(got_one, 0)
    group_wait(got_one, 0, 2)
    group_wait(got_one, 0, 3)

    begin("h_first")

    def first(r, carry):
        a = averaged(r, got_one)
        avg[r] = a
        pre[...] += dot(a, w_one[r])
        return carry

    lax.fori_loop(0, REL, first, 0, unroll=UNROLL)
    hidden[...] = jnp.maximum(pre[...], 0.0).astype(BF)
    begin("i_pack")
    pack(hidden[...])
    everyone(ahead, sender(got_two, 1))
    got_two[0] = send[0]

    begin("j_turns")

    def turn(r, out):
        out[pl.ds(pl.multiple_of(r * D, D), D), :] = avg[r].T

    def relation_t(r, carry):
        for b in range(2):
            dst_hot = hot(dst[r, b : b + 1, :] == iota((128, 256), 0))
            src_hot = source_hot(r, b)
            lanes = pl.ds(pl.multiple_of(r * N + b * 128, 128), 128)
            adj_t[:, lanes] = dot_nt(src_hot, dst_hot).astype(BF)
        turn(r, avg_one_t)
        return carry

    lax.fori_loop(0, REL, relation_t, 0, unroll=UNROLL)
    begin("ja_weights")

    for i in range(11):
        two_load(i).wait()
        at = pl.ds(i * 32, 32)
        for j in range(4):
            lanes = slice(128 * j, 128 * (j + 1))
            turned[j % 2] = w_two_raw[i % 4, :, :, lanes].astype(F32).reshape(32 * REL, 128)
            for r in range(REL):
                w_two[r, at, lanes] = turned[j % 2, pl.ds(r, 32, stride=REL), :].astype(BF)
        if i + 4 < 11:
            two_load(i + 4).start()

    begin("jb_picks")
    picks_t[...] = picks[...].T
    avg_two_t[REL * D :, :] = hidden[...].T
    acc[:, :C] = dot_nt(hidden[...], w_self[...])
    lab = jnp.broadcast_to(labels[...], (128, N)).T[:, :1]
    begin("jc_gather")
    gather_most(hidden, got_two, 1)
    begin("k_wait")
    small_wait(0)
    labelled_count = jnp.sum(counts[:, :, 0:1])
    sent_wait(got_two, 1)
    group_wait(got_two, 1, 2)
    group_wait(got_two, 1, 3)

    begin("l_second")

    def second(r, carry):
        a = averaged(r, got_two)
        avg[r] = a
        acc[:, :C] += dot_nt(a, w_two[r, :C, :])
        return carry

    lax.fori_loop(0, REL, second, 0, unroll=UNROLL)
    begin("m_soft")
    out = acc[:, :C]
    labelled = lab >= 0
    top = jnp.max(out, axis=1, keepdims=True)
    log_total = jnp.log(jnp.sum(jnp.exp(out - top), axis=1, keepdims=True)) + top
    label_hot = jnp.where(lab == iota((N, C), 1), 1.0, 0.0)
    picked = jnp.sum(out * label_hot, axis=1, keepdims=True)
    soft = jnp.exp(out - log_total)
    mask = jnp.where(labelled, 1.0, 0.0)
    grad[...] = jnp.zeros_like(grad)
    grad[:, :C] = (loss_scale * (soft - label_hot) * mask / labelled_count).astype(BF)
    small_out[1] = jnp.broadcast_to(
        jnp.sum(jnp.where(labelled, log_total - picked, 0.0), axis=0, keepdims=True), (1, 128)
    )

    begin("n_spread")

    def spread(r, carry):
        at = pl.ds(pl.multiple_of(r * N, N), N)
        spreads[at, :] = (dot(grad[:, :C], w_two[r, :C, :]) * norm[r, :, :1]).astype(BF)
        return carry

    lax.fori_loop(0, REL, spread, 0, unroll=UNROLL)
    begin("o_send")
    got_three = got_one
    back = sender(got_three, 2)
    for g in range(4):
        group = dot(adj_t[N + 256 * g : N + 256 * (g + 1), :], spreads[...])
        send[32 * g : 32 * (g + 1)] = group.astype(BF).reshape(32, SLOTS, D)
        everyone(behind, back, max(1, 32 * g), 32 * (g + 1))
    got_three[0] = send[0]

    begin("p_two")
    partner = (me[0], me[1], me[2], 1 - core)

    def chunks(x, h, left, right, lanes):
        start = pl.multiple_of((x * 2 + h) * BLOCK, BLOCK)
        value = dot(left[pl.ds(start, BLOCK), :], right[...]).astype(BF)
        for j in range(16):
            to = (x, h * 2 + j // 8, (j // 2) % 4, j % 2)
            parts[(*to, slice(None), lanes)] = value[ROWS * j : ROWS * (j + 1), :]

    def to_partner(x, lanes, sem):
        return pltpu.make_async_remote_copy(
            src_ref=parts.at[x, :, :, 1 - core, :, lanes], dst_ref=half.at[x, :, :, :, lanes],
            send_sem=p_send.at[sem], recv_sem=p_recv.at[sem], device_id=partner,
            device_id_type=MESH,
        )

    def add_near(x, z, lanes):
        half[x, z, :, :, lanes] = (
            parts[x, z, :, core, :, lanes].astype(F32) + half[x, z, :, :, lanes].astype(F32)
        ).astype(BF)

    two_lanes = pl.ds(D, CP)
    one_lanes = pl.ds(0, D)

    def turn_two(r, carry):
        turn(r, avg_two_t)
        return carry

    lax.fori_loop(0, REL, turn_two, 0)

    def two_chunks(i, carry):
        chunks(i // 2, i % 2, avg_two_t, grad, two_lanes)
        return carry

    lax.fori_loop(0, 8, two_chunks, 0)
    two_copy = to_partner(slice(None), two_lanes, 4)
    two_copy.start()
    logits_v[...] = acc[...].T[:C, :]
    logits_copy = pltpu.make_async_copy(logits_v, logits_t, w_sems.at[13])
    logits_copy.start()
    own_grad[...] = dot(adj_t[:N, :], spreads[...]) + dot(grad[:, :C], w_self[...])
    two_copy.wait()

    def add_two(i, carry):
        add_near(i // 4, i % 4, two_lanes)
        return carry

    lax.fori_loop(0, 16, add_two, 0)

    everyone(ahead, small_sender(1, totals))
    totals[0] = small_out[1]

    def to_axis(axis, step):
        to = list(me)
        to[axis] = lax.rem(me[axis] + step, 4)
        return tuple(to), to[axis]

    def cut(s, upper):
        _, row, rows_s, _ = STREAMS[s]
        low = 16 if rows_s > 20 else 8
        return (row + low, low, rows_s - low) if upper else (row, 0, low)

    def first_at(s, k, row, size):
        lane, _, _, order = STREAMS[s]
        at = tuple(k if a == order[0] else slice(None) for a in range(3))
        return (*at, pl.ds(row, size), pl.ds(lane, 128))

    def first_hop(s, kind, forward):
        axis = STREAMS[s][3][0]
        to, k = to_axis(axis, 1 if forward else 3)
        row, inner, size = cut(s, forward if kind == "own" else not forward)
        if kind == "far":
            k = lax.rem(me[axis] + 2, 4)
            slot = 2
        else:
            slot = 0 if forward else 1
        sem = s * 12 + {"far": 0, "own": 2, "both": 4}[kind] + (0 if forward else 1)
        return pltpu.make_async_remote_copy(
            src_ref=half.at[first_at(s, k, row, size)],
            dst_ref=first_got[s].at[slot, :, :, pl.ds(inner, size), :],
            send_sem=x_send.at[sem], recv_sem=x_recv.at[sem], device_id=to, device_id_type=MESH,
        )

    def relay(s):
        axis = STREAMS[s][3][0]
        for forward in (True, False):
            first_hop(s, "far", forward).wait()
            _, k = to_axis(axis, 1 if forward else 3)
            row, inner, size = cut(s, not forward)
            at = first_at(s, k, row, size)
            half[at] = (
                half[at].astype(F32) + first_got[s][2, :, :, inner : inner + size, :].astype(F32)
            ).astype(BF)
            first_hop(s, "both", forward).start()

    def hop(s, phase, j):
        order = STREAMS[s][3]
        axis = order[phase]
        to, k = to_axis(axis, j)
        if phase == 1:
            at = tuple(k if a == axis else slice(None) for a in sorted(order[1:]))
            ref = first_sum[s].at[at]
            got = second_got[s]
        else:
            ref = second_sum[s].at[k]
            got = third_got[s]
        sem = s * 12 + 3 + phase * 3 + j - 1
        return pltpu.make_async_remote_copy(
            src_ref=ref, dst_ref=got.at[j - 1], send_sem=x_send.at[sem], recv_sem=x_recv.at[sem],
            device_id=to, device_id_type=MESH,
        )

    def first_start(s):
        for kind in ("far", "own"):
            for forward in (True, False):
                first_hop(s, kind, forward).start()

    for s in TWO:
        first_start(s)
    begin("q_wait")
    sent_wait(got_three, 2)
    for g in range(4):
        group_wait(got_three, 2, g)

    begin("r_gradpre")
    grad_hidden = own_grad[...] + dot(picks_t[...], got_three[...].reshape(FAR, D))
    grad_pre[...] = jnp.where(pre[...] > 0.0, grad_hidden, 0.0).astype(BF)

    begin("s_one")

    def one_block(j):
        k = lax.rem(me[0] + j, 4)

        def one_chunks(i, carry):
            chunks(k, i, avg_one_t, grad_pre, one_lanes)
            return carry

        lax.fori_loop(0, 2, one_chunks, 0)
        to_partner(k, one_lanes, j).start()

    def one_near(j):
        k = lax.rem(me[0] + j, 4)
        to_partner(k, one_lanes, j).wait()

        def add_one(i, carry):
            add_near(k, i, one_lanes)
            return carry

        lax.fori_loop(0, 4, add_one, 0)
        for s in ONE_X:
            if j == 2:
                first_hop(s, "far", True).start()
                first_hop(s, "far", False).start()
            elif j:
                first_hop(s, "own", j == 1).start()

    one_block(2)
    one_block(1)
    for s in TWO:
        relay(s)
    one_near(2)
    one_block(3)
    one_near(1)
    one_block(0)
    one_near(3)
    one_near(0)
    begin("t_near")
    for s in ONE_REST:
        first_start(s)
    begin("ta_relay")
    for s in ONE_X + ONE_REST:
        relay(s)

    def sum_first(s):
        lane, row, rows_s, order = STREAMS[s]
        for kind in ("own", "both"):
            for forward in (True, False):
                first_hop(s, kind, forward).wait()

        def body(i, carry):
            at = [None, None, None]
            left = sorted(order[1:])
            at[order[0]] = me[order[0]]
            at[left[0]] = i
            at[left[1]] = slice(None)
            total = half[(*at, pl.ds(row, rows_s), pl.ds(lane, 128))].astype(F32)
            for j in range(2):
                total += first_got[s][j, i].astype(F32)
            first_sum[s][i] = total.astype(BF)
            return carry

        lax.fori_loop(0, 4, body, 0)
        for j in (2, 1, 3):
            hop(s, 1, j).start()

    def sum_second(s):
        order = STREAMS[s][3]
        for j in (1, 2, 3):
            hop(s, 1, j).wait()
        m = me[order[1]]
        if order[1] < order[2]:
            total = first_sum[s][m].astype(F32)
        else:
            total = first_sum[s][:, m].astype(F32)
        for j in range(3):
            total += second_got[s][j].astype(F32)
        second_sum[s][...] = total.astype(BF)
        for j in (2, 1, 3):
            hop(s, 2, j).start()

    def sum_third(s):
        order = STREAMS[s][3]
        for j in (1, 2, 3):
            hop(s, 2, j).wait()
        total = second_sum[s][me[order[2]]].astype(F32)
        for j in range(3):
            total += third_got[s][j].astype(F32)
        return total

    begin("u_first")
    for s in TWO:
        sum_first(s)
    begin("ua_first")
    for s in ONE_X + ONE_REST:
        sum_first(s)
    begin("v_second")
    for s in TWO + ONE_X + ONE_REST:
        sum_second(s)
    begin("w_third")
    small_wait(1)
    loss[...] = jnp.broadcast_to(jnp.sum(totals[:, :, 0:1]) / labelled_count, (1, 128))
    logits_copy.wait()
    for s in TWO + ONE_X + ONE_REST:
        lane, row, rows_s, _ = STREAMS[s]
        total = sum_third(s)
        if lane < D:
            grad_one[row : row + rows_s, lane : lane + 128] = total
        else:
            lane -= D
            size = min(128, C - lane)
            grad_two[:, lane : lane + size] = total[:, :size]
    begin(None)


def finish_body(a, b, c, d, a_out, b_out, c_out, d_out, b_row, sems):
    copies = [
        pltpu.make_async_copy(x, y, sems.at[i])
        for i, (x, y) in enumerate(((a, a_out), (b, b_row), (c, c_out), (d, d_out)))
    ]
    for copy in copies:
        copy.start()
    for copy in copies:
        copy.wait()
    b_out[...] = b_row[:, :1]


def sds(shape, dtype):
    return jax.ShapeDtypeStruct(shape, dtype)


def on_device(features, w_one, w_two, self_two, edge_src, edge_dst, send_rows, send_count, labels):
    vm = pl.BlockSpec(memory_space=pltpu.VMEM)
    hbm = pl.BlockSpec(memory_space=pl.ANY)
    V = pltpu.VMEM
    rows = [s[2] for s in STREAMS]
    scratch = [
        V((N, D), BF), V((REL, 2, N), I32), V((REL, 2, N), I32), V((SLOTS, PEERS), I32),
        V((1, PEERS), I32), V((1, N), I32),
        V((REL + 1, D, D), BF), V((REL, 352, D), BF), V((4, 32, REL, D), BF), V((2, 256, 128), F32),
        V((C, D), BF), V((REL, 2, N), I32), V((TABLE, 128), I32),
        V((REL, N, TABLE), BF), V((TABLE, REL * N), BF), V((REL, N, 128), F32),
        V((FAR, N), BF), V((N, FAR), BF),
        V((PEERS, SLOTS, D), BF), V((PEERS, SLOTS, D), BF), V((PEERS, SLOTS, D), BF),
        V((REL, N, D), F32), V((REL, N, D), BF), V(((REL + 1) * D, N), BF), V(((REL + 1) * D, N), BF),
        V((N, D), F32), V((N, D), BF), V((N, CP), F32), V((C, N), F32), V((N, D), F32),
        V((REL * N, D), BF),
        V((N, CP), BF), V((N, D), BF),
        V((2, 1, 128), F32), V((PEERS, 1, 128), F32), V((PEERS, 1, 128), F32),
        V((4, 4, 4, 2, ROWS, WIDE), BF), V((4, 4, 4, ROWS, WIDE), BF),
        *[V((3, 4, 4, r, 128), BF) for r in rows],
        *[V((4, 4, r, 128), BF) for r in rows],
        *[V((3, 4, r, 128), BF) for r in rows],
        *[V((4, r, 128), BF) for r in rows],
        *[V((3, r, 128), BF) for r in rows],
        pltpu.SemaphoreType.DMA((14,)),
        pltpu.SemaphoreType.DMA((3,)), pltpu.SemaphoreType.DMA((12,)),
        pltpu.SemaphoreType.DMA((2,)), pltpu.SemaphoreType.DMA((2,)),
        pltpu.SemaphoreType.DMA((5,)), pltpu.SemaphoreType.DMA((5,)),
        pltpu.SemaphoreType.DMA((96,)), pltpu.SemaphoreType.DMA((96,)),
    ]
    codes = np.concatenate(
        [np.arange(N)] + [N + SLOTS * code + np.arange(SLOTS) for code in ORDER]
    ).astype(np.int32)
    logits_t, loss, grad_one, grad_two = pl.pallas_call(
        step_body,
        name="step",
        in_specs=[hbm] * 10,
        out_specs=[hbm, vm, vm, vm],
        out_shape=[sds((C, N), F32), sds((1, 128), F32), sds((ROWS, D), F32), sds((ROWS, C), F32)],
        scratch_shapes=scratch,
        compiler_params=pltpu.CompilerParams(
            collective_id=0, has_side_effects=True, vmem_limit_bytes=int(VLIM * MB)
        ),
    )(
        features, w_one, jnp.transpose(w_two, (2, 0, 1)), self_two.T, edge_src, edge_dst,
        send_rows[0].T, send_count, labels.reshape(1, N),
        jnp.asarray(np.repeat(codes[:, None], 128, axis=1)),
    )
    logits_t, loss, grad_one, grad_two = pl.pallas_call(
        finish_body,
        name="finish",
        in_specs=[hbm] * 4,
        out_specs=[vm] * 4,
        out_shape=[sds((C, N), F32), sds((1, 1), F32), sds((ROWS, D), F32), sds((ROWS, C), F32)],
        scratch_shapes=[V((1, 128), F32), pltpu.SemaphoreType.DMA((4,))],
        compiler_params=pltpu.CompilerParams(vmem_limit_bytes=63 * MB),
    )(logits_t, loss, grad_one, grad_two)
    return (logits_t.T, loss[0, 0], grad_one, grad_two)


def solution(mesh):
    split = Mesh(mesh.devices.reshape(SIZES), DOM)
    return jax.shard_map(
        on_device,
        mesh=split,
        in_specs=(
            P(DOM, None),
            P(),
            P(),
            P(),
            P(None, DOM, None),
            P(None, DOM, None),
            P(DOM, None, None),
            P(DOM, None),
            P(DOM),
        ),
        out_specs=(P(DOM, None), P(), P(DOM, None), P(DOM, None)),
        check_vma=False,
    )
```

```python
import jax
import jax.numpy as jnp
import numpy as np
from jax import lax
from jax.experimental import pallas as pl
from jax.experimental.pallas import tpu as pltpu
from jax.sharding import Mesh
from jax.sharding import PartitionSpec as P

DOM = ("dom_0", "dom_1", "dom_2", "dom_3")
SIZES = (4, 4, 4, 2)
BF = jnp.bfloat16
F32 = jnp.float32
I32 = jnp.int32
MESH = pl.DeviceIdType.MESH
loss_scale = 256.0
MB = 1 << 20
VLIM = 63
UNROLL = 4

PEERS = 128
CHIPS = 64
SLOTS = 8
REL = 8
N = 256
D = 512
C = 349
CP = 384
FAR = PEERS * SLOTS
TABLE = N + FAR
ROWS = 36
WIDE = D + CP
BLOCK = 16 * ROWS

STREAMS = (
    (0, 0, 36, (0, 1, 2)),
    (384, 0, 24, (0, 1, 2)),
    (128, 0, 36, (1, 2, 0)),
    (384, 24, 12, (1, 2, 0)),
    (256, 0, 36, (2, 0, 1)),
    (512, 0, 36, (0, 1, 2)),
    (640, 0, 36, (1, 2, 0)),
    (768, 0, 36, (2, 0, 1)),
)
ONE_X, ONE_REST, TWO = (0, 1), (2, 3, 4), (5, 6, 7)
READY = (5, 6, 7, 0, 1, 4, 2, 3)


def hops(code):
    return sum(min(d, 4 - d) for d in digits(code)[:3])


def digits(code):
    return (code % 4, code // 4 % 4, code // 16 % 4, code // 64)


def block_order():
    spread = []
    for k in range(1, PEERS):
        d0 = k % 4
        d1 = (k // 4 + d0) % 4
        d2 = (k // 16 + d1) % 4
        spread.append(d0 + 4 * d1 + 16 * d2 + 64 * (k // 64))
    return [0] + sorted(spread, key=lambda code: -hops(code))


ORDER = block_order()


def dot(a, b):
    return jnp.dot(a, b, preferred_element_type=F32)


def dot_nt(a, b):
    return lax.dot_general(a, b, (((1,), (1,)), ((), ())), preferred_element_type=F32)


def iota(shape, dim):
    return lax.broadcasted_iota(I32, shape, dim)


def hot(mask):
    return jnp.where(mask, 1.0, 0.0).astype(BF)


def phases():
    now = []

    def begin(name):
        if now:
            now.pop().__exit__(None, None, None)
        if name:
            now.append(jax.named_scope(name))
            now[0].__enter__()

    return begin


def step_body(
    own_hbm, w_one_hbm, w_two_hbm, w_self_hbm, src_hbm, dst_hbm, rows_hbm, count_hbm, labels_hbm,
    codes_hbm,
    logits_t, loss, grad_one, grad_two,
    own, src, dst, rows, count, labels, w_one, w_two, w_two_raw, turned, w_self, where_src, row_code, adj, adj_t, norm, picks, picks_t,
    send, got_one, got_two, sums, avg, avg_one_t, avg_two_t,
    pre, hidden, acc, logits_v, loss_v, one_v, two_v, own_grad, spreads, grad, grad_pre,
    small_out, counts, totals,
    parts, half, *rest_refs,
):
    begin = phases()
    count_s = len(STREAMS)
    first_got, first_sum, second_got, second_sum, third_got = (
        rest_refs[i * count_s : (i + 1) * count_s] for i in range(5)
    )
    w_sems, a_send, a_recv, s_send, s_recv, p_send, p_recv, x_send, x_recv = rest_refs[5 * count_s :]
    me = [lax.axis_index(a) for a in DOM]
    mine = ((me[0] * 4 + me[1]) * 4 + me[2]) * 2 + me[3]
    core = me[3]

    begin("a_greet")
    loads = [
        pltpu.make_async_copy(w_one_hbm, w_one, w_sems.at[0]),
        pltpu.make_async_copy(w_self_hbm, w_self, w_sems.at[1]),
    ]

    def two_load(i):
        count = min(32, C - 32 * i)
        return pltpu.make_async_copy(
            w_two_hbm.at[pl.ds(32 * i, count)], w_two_raw.at[i % 4, pl.ds(0, count)],
            w_sems.at[2 + i % 4],
        )

    inputs = [
        pltpu.make_async_copy(a, b, w_sems.at[6 + i])
        for i, (a, b) in enumerate(
            (
                (codes_hbm, row_code), (rows_hbm, rows), (count_hbm, count), (own_hbm, own),
                (labels_hbm, labels), (src_hbm, src), (dst_hbm, dst),
            )
        )
    ]
    for load in inputs + loads + [two_load(i) for i in range(4)]:
        load.start()

    ahead = [[lax.rem(m + d, n) for d in range(n)] for m, n in zip(me, SIZES)]
    behind = [[lax.rem(m + n - d, n) for d in range(n)] for m, n in zip(me, SIZES)]

    def everyone(where, body, start=1, stop=PEERS):
        for k in range(start, stop):
            body(k, tuple(where[i][d] for i, d in enumerate(digits(ORDER[k]))))

    barrier = pltpu.get_barrier_semaphore()

    def greet(k, to):
        pl.semaphore_signal(barrier, inc=1, device_id=to, device_id_type=MESH)

    everyone(ahead, greet)

    begin("b_pack")
    for load in inputs:
        load.wait()
    spot = row_code[N:, :1] - N
    code = spot >> 3
    peer = (
        (((me[0] + code) & 3) << 5) + (((me[1] + (code >> 2)) & 3) << 3)
        + (((me[2] + (code >> 4)) & 3) << 1) + ((core + (code >> 6)) & 1)
    )
    peer_hot = peer == iota((FAR, PEERS), 1)
    by_peer = dot_nt(hot(peer_hot), rows[...].astype(F32).astype(BF))
    slot = spot & 7
    chosen = jnp.sum(jnp.where(slot == iota((FAR, SLOTS), 1), by_peer, 0.0), axis=1, keepdims=True)
    live = jnp.sum(
        jnp.where(peer_hot, jnp.broadcast_to(count[...], (FAR, PEERS)), 0).astype(F32),
        axis=1, keepdims=True,
    )
    row_of = jnp.where(slot.astype(F32) < live, chosen, -1.0).astype(I32)
    picks[...] = hot(row_of == iota((FAR, N), 1))

    def pack(values):
        send[...] = dot(picks[...], values).astype(BF).reshape(PEERS, SLOTS, D)

    pack(own[...])
    small_out[0] = jnp.broadcast_to(
        jnp.sum(jnp.where(labels[...] >= 0, 1.0, 0.0), axis=1, keepdims=True), (1, 128)
    )
    begin("c_barrier")
    pl.semaphore_wait(barrier, PEERS - 1)

    def sender(got, which):
        def one(k, to):
            pltpu.make_async_remote_copy(
                src_ref=send.at[k], dst_ref=got.at[k], send_sem=a_send.at[which],
                recv_sem=a_recv.at[which * 4 + k // 32], device_id=to, device_id_type=MESH,
            ).start()

        return one

    def small_sender(small, small_got):
        def one(k, to):
            pltpu.make_async_remote_copy(
                src_ref=small_out.at[small], dst_ref=small_got.at[k],
                send_sem=s_send.at[small], recv_sem=s_recv.at[small],
                device_id=to, device_id_type=MESH,
            ).start()

        return one

    def group_wait(got, which, g):
        part = pl.ds(0, 31 if g == 0 else 32)
        pltpu.make_async_copy(send.at[part], got.at[part], a_recv.at[which * 4 + g]).wait()

    rest = pl.ds(0, PEERS - 1)

    def sent_wait(got, which):
        pltpu.make_async_copy(send.at[rest], got.at[rest], a_send.at[which]).wait()

    def small_wait(which):
        pltpu.make_async_copy(counts.at[rest], totals.at[rest], s_send.at[which]).wait()
        pltpu.make_async_copy(counts.at[rest], totals.at[rest], s_recv.at[which]).wait()

    begin("d_send")
    everyone(ahead, sender(got_one, 0))
    got_one[0] = send[0]

    begin("e_adjacency")
    far_src = src[...] - N
    p = far_src >> 3
    o0 = (me[0] + 4 - (p >> 5)) & 3
    o1 = (me[1] + 4 - ((p >> 3) & 3)) & 3
    o2 = (me[2] + 4 - ((p >> 1) & 3)) & 3
    o3 = (core + 2 - (p & 1)) & 1
    code_of = o0 + (o1 << 2) + (o2 << 4) + (o3 << 6)
    where_src[...] = jnp.where(far_src >= 0, N + (code_of << 3) + (far_src & 7), src[...])

    def source_hot(r, b):
        halves = [
            hot(where_src[r, b : b + 1, 128 * i : 128 * (i + 1)] == row_code[...]) for i in range(2)
        ]
        return jnp.concatenate(halves, axis=1)

    def relation(r, carry):
        for b in range(2):
            at = slice(b * 128, (b + 1) * 128)
            dst_hot = hot(dst[r, b : b + 1, :] == iota((128, 256), 0))
            src_hot = source_hot(r, b)
            adj[r, at, :] = dot_nt(dst_hot, src_hot).astype(BF)
            live_edges = jnp.sum(dst_hot.astype(F32), axis=1, keepdims=True)
            norm[r, at, :] = jnp.broadcast_to(1.0 / jnp.maximum(live_edges, 1.0), (128, 128))
        return carry

    lax.fori_loop(0, REL, relation, 0, unroll=UNROLL)
    everyone(ahead, small_sender(0, counts))
    counts[0] = small_out[0]
    begin("f_local")

    def rows_of(got, g, count):
        return got[32 * g : 32 * (g + count)].reshape(256 * count, D)

    def columns(r, g, count):
        return adj[r, :, N + 256 * g : N + 256 * (g + count)]

    def gather_most(values, got, which):
        group_wait(got, which, 0)

        def near_rows(r, carry):
            sums[r] = dot(adj[r, :, :N], values[...]) + dot(columns(r, 0, 1), rows_of(got, 0, 1))
            return carry

        lax.fori_loop(0, REL, near_rows, 0, unroll=UNROLL)
        group_wait(got, which, 1)

        def middle_rows(r, carry):
            sums[r] += dot(columns(r, 1, 1), rows_of(got, 1, 1))
            return carry

        lax.fori_loop(0, REL, middle_rows, 0, unroll=UNROLL)

    def averaged(r, got):
        total = sums[r] + dot(columns(r, 2, 2), rows_of(got, 2, 2))
        return (total * norm[r, :, :1]).astype(BF)

    avg_one_t[REL * D :, :] = own[...].T
    for load in loads:
        load.wait()
    pre[...] = dot(own[...], w_one[REL])
    gather_most(own, got_one, 0)
    begin("g_wait")
    sent_wait(got_one, 0)
    group_wait(got_one, 0, 2)
    group_wait(got_one, 0, 3)

    begin("h_first")

    def first(r, carry):
        a = averaged(r, got_one)
        avg[r] = a
        pre[...] += dot(a, w_one[r])
        return carry

    lax.fori_loop(0, REL, first, 0, unroll=UNROLL)
    hidden[...] = jnp.maximum(pre[...], 0.0).astype(BF)
    begin("i_pack")
    pack(hidden[...])
    everyone(ahead, sender(got_two, 1))
    got_two[0] = send[0]

    begin("j_turns")

    def turn(r, out):
        out[pl.ds(pl.multiple_of(r * D, D), D), :] = avg[r].T

    def relation_t(r, carry):
        for b in range(2):
            dst_hot = hot(dst[r, b : b + 1, :] == iota((128, 256), 0))
            src_hot = source_hot(r, b)
            lanes = pl.ds(pl.multiple_of(r * N + b * 128, 128), 128)
            adj_t[:, lanes] = dot_nt(src_hot, dst_hot).astype(BF)
        turn(r, avg_one_t)
        return carry

    lax.fori_loop(0, REL, relation_t, 0, unroll=UNROLL)
    begin("ja_weights")

    for i in range(11):
        two_load(i).wait()
        at = pl.ds(i * 32, 32)
        for j in range(4):
            lanes = slice(128 * j, 128 * (j + 1))
            turned[j % 2] = w_two_raw[i % 4, :, :, lanes].astype(F32).reshape(32 * REL, 128)
            for r in range(REL):
                w_two[r, at, lanes] = turned[j % 2, pl.ds(r, 32, stride=REL), :].astype(BF)
        if i + 4 < 11:
            two_load(i + 4).start()

    begin("jb_picks")
    picks_t[...] = picks[...].T
    avg_two_t[REL * D :, :] = hidden[...].T
    acc[:, :C] = dot_nt(hidden[...], w_self[...])
    lab = jnp.broadcast_to(labels[...], (128, N)).T[:, :1]
    begin("jc_gather")
    gather_most(hidden, got_two, 1)
    begin("k_wait")
    small_wait(0)
    labelled_count = jnp.sum(counts[:, :, 0:1])
    sent_wait(got_two, 1)
    group_wait(got_two, 1, 2)
    group_wait(got_two, 1, 3)

    begin("l_second")

    def second(r, carry):
        a = averaged(r, got_two)
        avg[r] = a
        acc[:, :C] += dot_nt(a, w_two[r, :C, :])
        return carry

    lax.fori_loop(0, REL, second, 0, unroll=UNROLL)
    begin("m_soft")
    out = acc[:, :C]
    labelled = lab >= 0
    top = jnp.max(out, axis=1, keepdims=True)
    log_total = jnp.log(jnp.sum(jnp.exp(out - top), axis=1, keepdims=True)) + top
    label_hot = jnp.where(lab == iota((N, C), 1), 1.0, 0.0)
    picked = jnp.sum(out * label_hot, axis=1, keepdims=True)
    soft = jnp.exp(out - log_total)
    mask = jnp.where(labelled, 1.0, 0.0)
    grad[...] = jnp.zeros_like(grad)
    grad[:, :C] = (loss_scale * (soft - label_hot) * mask / labelled_count).astype(BF)
    small_out[1] = jnp.broadcast_to(
        jnp.sum(jnp.where(labelled, log_total - picked, 0.0), axis=0, keepdims=True), (1, 128)
    )

    begin("n_spread")

    def spread(r, carry):
        at = pl.ds(pl.multiple_of(r * N, N), N)
        spreads[at, :] = (dot(grad[:, :C], w_two[r, :C, :]) * norm[r, :, :1]).astype(BF)
        return carry

    lax.fori_loop(0, REL, spread, 0, unroll=UNROLL)
    begin("o_send")
    got_three = got_one
    back = sender(got_three, 2)
    for g in range(4):
        group = dot(adj_t[N + 256 * g : N + 256 * (g + 1), :], spreads[...])
        send[32 * g : 32 * (g + 1)] = group.astype(BF).reshape(32, SLOTS, D)
        everyone(behind, back, max(1, 32 * g), 32 * (g + 1))
    got_three[0] = send[0]

    begin("p_two")
    partner = (me[0], me[1], me[2], 1 - core)

    def chunks(x, h, left, right, lanes):
        start = pl.multiple_of((x * 2 + h) * BLOCK, BLOCK)
        value = dot(left[pl.ds(start, BLOCK), :], right[...]).astype(BF)
        for j in range(16):
            to = (x, h * 2 + j // 8, (j // 2) % 4, j % 2)
            parts[(*to, slice(None), lanes)] = value[ROWS * j : ROWS * (j + 1), :]

    def to_partner(x, lanes, sem):
        return pltpu.make_async_remote_copy(
            src_ref=parts.at[x, :, :, 1 - core, :, lanes], dst_ref=half.at[x, :, :, :, lanes],
            send_sem=p_send.at[sem], recv_sem=p_recv.at[sem], device_id=partner,
            device_id_type=MESH,
        )

    def add_near(x, z, lanes):
        half[x, z, :, :, lanes] += parts[x, z, :, core, :, lanes]

    two_lanes = pl.ds(D, CP)
    one_lanes = pl.ds(0, D)

    def turn_two(r, carry):
        turn(r, avg_two_t)
        return carry

    lax.fori_loop(0, REL, turn_two, 0)

    for x in range(4):

        def two_chunks(i, carry):
            chunks(x, i, avg_two_t, grad, two_lanes)
            return carry

        lax.fori_loop(0, 2, two_chunks, 0)
        to_partner(x, two_lanes, 4 + x).start()
    logits_v[...] = acc[...].T[:C, :]
    logits_copy = pltpu.make_async_copy(logits_v, logits_t, w_sems.at[13])
    logits_copy.start()
    own_grad[...] = dot(adj_t[:N, :], spreads[...]) + dot(grad[:, :C], w_self[...])
    for x in range(4):
        to_partner(x, two_lanes, 4 + x).wait()

        def add_two(i, carry):
            add_near(x, i, two_lanes)
            return carry

        lax.fori_loop(0, 4, add_two, 0, unroll=2)

    everyone(ahead, small_sender(1, totals))
    totals[0] = small_out[1]

    def to_axis(axis, step):
        to = list(me)
        to[axis] = lax.rem(me[axis] + step, 4)
        return tuple(to), to[axis]

    def cut(s, upper):
        _, row, rows_s, _ = STREAMS[s]
        low = 16 if rows_s > 12 else 8
        return (row + low, low, rows_s - low) if upper else (row, 0, low)

    def first_at(s, k, row, size):
        lane, _, _, order = STREAMS[s]
        at = tuple(k if a == order[0] else slice(None) for a in range(3))
        return (*at, pl.ds(row, size), pl.ds(lane, 128))

    def first_hop(s, kind, forward):
        axis = STREAMS[s][3][0]
        to, k = to_axis(axis, 1 if forward else 3)
        row, inner, size = cut(s, forward if kind == "own" else not forward)
        if kind == "far":
            k = lax.rem(me[axis] + 2, 4)
            slot = 2
        else:
            slot = 0 if forward else 1
        sem = s * 12 + {"far": 0, "own": 2, "both": 4}[kind] + (0 if forward else 1)
        return pltpu.make_async_remote_copy(
            src_ref=half.at[first_at(s, k, row, size)],
            dst_ref=first_got[s].at[slot, :, :, pl.ds(inner, size), :],
            send_sem=x_send.at[sem], recv_sem=x_recv.at[sem], device_id=to, device_id_type=MESH,
        )

    def relay(s):
        axis = STREAMS[s][3][0]
        for forward in (True, False):
            first_hop(s, "far", forward).wait()
            _, k = to_axis(axis, 1 if forward else 3)
            row, inner, size = cut(s, not forward)
            at = first_at(s, k, row, size)
            half[at] += first_got[s][2, :, :, inner : inner + size, :]
            first_hop(s, "both", forward).start()

    def hop(s, phase, j):
        order = STREAMS[s][3]
        axis = order[phase]
        to, k = to_axis(axis, j)
        if phase == 1:
            at = tuple(k if a == axis else slice(None) for a in sorted(order[1:]))
            ref = first_sum[s].at[at]
            got = second_got[s]
        else:
            ref = second_sum[s].at[k]
            got = third_got[s]
        sem = s * 12 + 3 + phase * 3 + j - 1
        return pltpu.make_async_remote_copy(
            src_ref=ref, dst_ref=got.at[j - 1], send_sem=x_send.at[sem], recv_sem=x_recv.at[sem],
            device_id=to, device_id_type=MESH,
        )

    def first_start(s):
        for kind in ("far", "own"):
            for forward in (True, False):
                first_hop(s, kind, forward).start()

    for s in TWO:
        first_start(s)
    begin("q_wait")
    sent_wait(got_three, 2)
    for g in range(4):
        group_wait(got_three, 2, g)

    begin("r_gradpre")
    grad_hidden = own_grad[...] + dot(picks_t[...], got_three[...].reshape(FAR, D))
    grad_pre[...] = jnp.where(pre[...] > 0.0, grad_hidden, 0.0).astype(BF)

    begin("s_one")

    def one_block(j):
        k = lax.rem(me[0] + j, 4)

        def one_chunks(i, carry):
            chunks(k, i, avg_one_t, grad_pre, one_lanes)
            return carry

        lax.fori_loop(0, 2, one_chunks, 0)
        to_partner(k, one_lanes, j).start()

    def one_near(j):
        k = lax.rem(me[0] + j, 4)
        to_partner(k, one_lanes, j).wait()

        def add_one(i, carry):
            add_near(k, i, one_lanes)
            return carry

        lax.fori_loop(0, 4, add_one, 0, unroll=2)
        for s in ONE_X:
            if j == 2:
                first_hop(s, "far", True).start()
                first_hop(s, "far", False).start()
            elif j:
                first_hop(s, "own", j == 1).start()

    one_block(2)
    one_block(1)
    for s in TWO:
        relay(s)
    one_block(3)
    one_near(2)
    one_block(0)
    one_near(1)
    one_near(3)
    one_near(0)
    begin("t_near")
    for s in ONE_REST:
        first_start(s)
    begin("ta_relay")
    for s in READY[3:]:
        relay(s)

    def sum_first(s):
        lane, row, rows_s, order = STREAMS[s]
        for kind in ("own", "both"):
            for forward in (True, False):
                first_hop(s, kind, forward).wait()

        def body(i, carry):
            at = [None, None, None]
            left = sorted(order[1:])
            at[order[0]] = me[order[0]]
            at[left[0]] = i
            at[left[1]] = slice(None)
            total = half[(*at, pl.ds(row, rows_s), pl.ds(lane, 128))].astype(F32)
            for j in range(2):
                total += first_got[s][j, i].astype(F32)
            first_sum[s][i] = total.astype(BF)
            return carry

        lax.fori_loop(0, 4, body, 0)
        for j in (2, 1, 3):
            hop(s, 1, j).start()

    def sum_second(s):
        order = STREAMS[s][3]
        for j in (1, 2, 3):
            hop(s, 1, j).wait()
        m = me[order[1]]
        if order[1] < order[2]:
            total = first_sum[s][m].astype(F32)
        else:
            total = first_sum[s][:, m].astype(F32)
        for j in range(3):
            total += second_got[s][j].astype(F32)
        second_sum[s][...] = total.astype(BF)
        for j in (2, 1, 3):
            hop(s, 2, j).start()

    def sum_third(s):
        order = STREAMS[s][3]
        for j in (1, 2, 3):
            hop(s, 2, j).wait()
        total = second_sum[s][me[order[2]]].astype(F32)
        for j in range(3):
            total += third_got[s][j].astype(F32)
        return total

    begin("u_first")
    for s in READY:
        sum_first(s)
    begin("v_second")
    for s in READY:
        sum_second(s)
    begin("w_third")
    small_wait(1)
    loss_v[...] = jnp.broadcast_to(jnp.sum(totals[:, :, 0:1]) / labelled_count, (1, 128))
    results = [logits_copy]

    def result(value, out, at):
        copy = pltpu.make_async_copy(value, out, w_sems.at[at])
        copy.start()
        results.append(copy)

    result(loss_v, loss, 14)
    for i, s in enumerate(READY):
        lane, row, rows_s, _ = STREAMS[s]
        total = sum_third(s)
        if lane < D:
            one_v[row : row + rows_s, lane : lane + 128] = total
        else:
            lane -= D
            size = min(128, C - lane)
            two_v[:, lane : lane + size] = total[:, :size]
        if i == 2:
            result(two_v, grad_two, 15)
    result(one_v, grad_one, 16)
    for copy in results:
        copy.wait()
    begin(None)


def finish_body(a, b, c, d, a_out, b_out, c_out, d_out, b_row, sems):
    copies = [
        pltpu.make_async_copy(x, y, sems.at[i])
        for i, (x, y) in enumerate(((a, a_out), (b, b_row), (c, c_out), (d, d_out)))
    ]
    for copy in copies:
        copy.start()
    for copy in copies:
        copy.wait()
    b_out[...] = b_row[:, :1]


def sds(shape, dtype):
    return jax.ShapeDtypeStruct(shape, dtype)


def on_device(features, w_one, w_two, self_two, edge_src, edge_dst, send_rows, send_count, labels):
    vm = pl.BlockSpec(memory_space=pltpu.VMEM)
    hbm = pl.BlockSpec(memory_space=pl.ANY)
    V = pltpu.VMEM
    rows = [s[2] for s in STREAMS]
    scratch = [
        V((N, D), BF), V((REL, 2, N), I32), V((REL, 2, N), I32), V((SLOTS, PEERS), I32),
        V((1, PEERS), I32), V((1, N), I32),
        V((REL + 1, D, D), BF), V((REL, 352, D), BF), V((4, 32, REL, D), BF), V((2, 256, 128), F32),
        V((C, D), BF), V((REL, 2, N), I32), V((TABLE, 128), I32),
        V((REL, N, TABLE), BF), V((TABLE, REL * N), BF), V((REL, N, 128), F32),
        V((FAR, N), BF), V((N, FAR), BF),
        V((PEERS, SLOTS, D), BF), V((PEERS, SLOTS, D), BF), V((PEERS, SLOTS, D), BF),
        V((REL, N, D), F32), V((REL, N, D), BF), V(((REL + 1) * D, N), BF), V(((REL + 1) * D, N), BF),
        V((N, D), F32), V((N, D), BF), V((N, CP), F32), V((C, N), F32), V((1, 128), F32), V((ROWS, D), F32), V((ROWS, C), F32),
        V((N, D), F32),
        V((REL * N, D), BF),
        V((N, CP), BF), V((N, D), BF),
        V((2, 1, 128), F32), V((PEERS, 1, 128), F32), V((PEERS, 1, 128), F32),
        V((4, 4, 4, 2, ROWS, WIDE), BF), V((4, 4, 4, ROWS, WIDE), BF),
        *[V((3, 4, 4, r, 128), BF) for r in rows],
        *[V((4, 4, r, 128), BF) for r in rows],
        *[V((3, 4, r, 128), BF) for r in rows],
        *[V((4, r, 128), BF) for r in rows],
        *[V((3, r, 128), BF) for r in rows],
        pltpu.SemaphoreType.DMA((17,)),
        pltpu.SemaphoreType.DMA((3,)), pltpu.SemaphoreType.DMA((12,)),
        pltpu.SemaphoreType.DMA((2,)), pltpu.SemaphoreType.DMA((2,)),
        pltpu.SemaphoreType.DMA((8,)), pltpu.SemaphoreType.DMA((8,)),
        pltpu.SemaphoreType.DMA((96,)), pltpu.SemaphoreType.DMA((96,)),
    ]
    codes = np.concatenate(
        [np.arange(N)] + [N + SLOTS * code + np.arange(SLOTS) for code in ORDER]
    ).astype(np.int32)
    logits_t, loss, grad_one, grad_two = pl.pallas_call(
        step_body,
        name="step",
        in_specs=[hbm] * 10,
        out_specs=[hbm] * 4,
        out_shape=[sds((C, N), F32), sds((1, 128), F32), sds((ROWS, D), F32), sds((ROWS, C), F32)],
        scratch_shapes=scratch,
        compiler_params=pltpu.CompilerParams(
            collective_id=0, has_side_effects=True, vmem_limit_bytes=int(VLIM * MB)
        ),
    )(
        features, w_one, jnp.transpose(w_two, (2, 0, 1)), self_two.T, edge_src, edge_dst,
        send_rows[0].T, send_count, labels.reshape(1, N),
        jnp.asarray(np.repeat(codes[:, None], 128, axis=1)),
    )
    logits_t, loss, grad_one, grad_two = pl.pallas_call(
        finish_body,
        name="finish",
        in_specs=[hbm] * 4,
        out_specs=[vm] * 4,
        out_shape=[sds((C, N), F32), sds((1, 1), F32), sds((ROWS, D), F32), sds((ROWS, C), F32)],
        scratch_shapes=[V((1, 128), F32), pltpu.SemaphoreType.DMA((4,))],
        compiler_params=pltpu.CompilerParams(vmem_limit_bytes=63 * MB),
    )(logits_t, loss, grad_one, grad_two)
    return (logits_t.T, loss[0, 0], grad_one, grad_two)


def solution(mesh):
    split = Mesh(mesh.devices.reshape(SIZES), DOM)
    return jax.shard_map(
        on_device,
        mesh=split,
        in_specs=(
            P(DOM, None),
            P(),
            P(),
            P(),
            P(None, DOM, None),
            P(None, DOM, None),
            P(DOM, None, None),
            P(DOM, None),
            P(DOM),
        ),
        out_specs=(P(DOM, None), P(), P(DOM, None), P(DOM, None)),
        check_vma=False,
    )
```

```python
import jax
import jax.numpy as jnp
import numpy as np
from jax import lax
from jax.experimental import pallas as pl
from jax.experimental.pallas import tpu as pltpu
from jax.sharding import Mesh
from jax.sharding import PartitionSpec as P

DOM = ("dom_0", "dom_1", "dom_2", "dom_3")
SIZES = (4, 4, 4, 2)
BF = jnp.bfloat16
F32 = jnp.float32
I32 = jnp.int32
MESH = pl.DeviceIdType.MESH
loss_scale = 256.0
MB = 1 << 20
VLIM = 63
UNROLL = 4

PEERS = 128
CHIPS = 64
SLOTS = 8
REL = 8
N = 256
D = 512
C = 349
CP = 384
FAR = PEERS * SLOTS
TABLE = N + FAR
ROWS = 36
WIDE = D + CP
BLOCK = 16 * ROWS

STREAMS = (
    (0, 0, 36, (0, 1, 2)),
    (384, 0, 24, (0, 1, 2)),
    (128, 0, 36, (1, 2, 0)),
    (384, 24, 12, (1, 2, 0)),
    (256, 0, 36, (2, 0, 1)),
    (512, 0, 36, (0, 1, 2)),
    (640, 0, 36, (1, 2, 0)),
    (768, 0, 36, (2, 0, 1)),
)
ONE_X, ONE_REST, TWO = (0, 1), (2, 3, 4), (5, 6, 7)
READY = (5, 6, 7, 0, 1, 4, 2, 3)


def hops(code):
    return sum(min(d, 4 - d) for d in digits(code)[:3])


def digits(code):
    return (code % 4, code // 4 % 4, code // 16 % 4, code // 64)


def block_order():
    spread = []
    for k in range(1, PEERS):
        d0 = k % 4
        d1 = (k // 4 + d0) % 4
        d2 = (k // 16 + d1) % 4
        spread.append(d0 + 4 * d1 + 16 * d2 + 64 * (k // 64))
    return [0] + sorted(spread, key=lambda code: -hops(code))


ORDER = block_order()


def dot(a, b):
    return jnp.dot(a, b, preferred_element_type=F32)


def dot_nt(a, b):
    return lax.dot_general(a, b, (((1,), (1,)), ((), ())), preferred_element_type=F32)


def iota(shape, dim):
    return lax.broadcasted_iota(I32, shape, dim)


def hot(mask):
    return jnp.where(mask, 1.0, 0.0).astype(BF)


def phases():
    now = []

    def begin(name):
        if now:
            now.pop().__exit__(None, None, None)
        if name:
            now.append(jax.named_scope(name))
            now[0].__enter__()

    return begin


def step_body(
    own_hbm, w_one_hbm, w_two_hbm, w_self_hbm, src_hbm, dst_hbm, rows_hbm, count_hbm, labels_hbm,
    codes_hbm,
    logits_t, loss, grad_one, grad_two,
    own, src, dst, rows, count, labels, w_one, w_two, w_two_raw, turned, w_self, where_src, row_code, adj, adj_t, norm, picks, picks_t,
    send, got_one, got_two, sums, avg, avg_one_t, avg_two_t,
    pre, hidden, acc, logits_v, loss_v, one_v, two_v, own_grad, spreads, grad, grad_pre,
    small_out, counts, totals,
    parts, half, *rest_refs,
):
    begin = phases()
    count_s = len(STREAMS)
    first_got, first_sum, second_got, second_sum, third_got = (
        rest_refs[i * count_s : (i + 1) * count_s] for i in range(5)
    )
    w_sems, a_send, a_recv, s_send, s_recv, p_send, p_recv, x_send, x_recv = rest_refs[5 * count_s :]
    me = [lax.axis_index(a) for a in DOM]
    mine = ((me[0] * 4 + me[1]) * 4 + me[2]) * 2 + me[3]
    core = me[3]

    begin("a_greet")
    loads = [
        pltpu.make_async_copy(w_one_hbm, w_one, w_sems.at[0]),
        pltpu.make_async_copy(w_self_hbm, w_self, w_sems.at[1]),
    ]

    def two_load(i):
        count = min(32, C - 32 * i)
        return pltpu.make_async_copy(
            w_two_hbm.at[pl.ds(32 * i, count)], w_two_raw.at[i % 4, pl.ds(0, count)],
            w_sems.at[2 + i % 4],
        )

    inputs = [
        pltpu.make_async_copy(a, b, w_sems.at[6 + i])
        for i, (a, b) in enumerate(
            (
                (codes_hbm, row_code), (rows_hbm, rows), (count_hbm, count), (own_hbm, own),
                (labels_hbm, labels), (src_hbm, src), (dst_hbm, dst),
            )
        )
    ]
    for load in inputs + loads + [two_load(i) for i in range(4)]:
        load.start()

    ahead = [[lax.rem(m + d, n) for d in range(n)] for m, n in zip(me, SIZES)]
    behind = [[lax.rem(m + n - d, n) for d in range(n)] for m, n in zip(me, SIZES)]

    def everyone(where, body, start=1, stop=PEERS):
        for k in range(start, stop):
            body(k, tuple(where[i][d] for i, d in enumerate(digits(ORDER[k]))))

    barrier = pltpu.get_barrier_semaphore()

    def greet(k, to):
        pl.semaphore_signal(barrier, inc=1, device_id=to, device_id_type=MESH)

    everyone(ahead, greet)

    begin("b_pack")
    for load in inputs:
        load.wait()
    spot = row_code[N:, :1] - N
    code = spot >> 3
    peer = (
        (((me[0] + code) & 3) << 5) + (((me[1] + (code >> 2)) & 3) << 3)
        + (((me[2] + (code >> 4)) & 3) << 1) + ((core + (code >> 6)) & 1)
    )
    peer_hot = peer == iota((FAR, PEERS), 1)
    by_peer = dot_nt(hot(peer_hot), rows[...].astype(F32).astype(BF))
    slot = spot & 7
    chosen = jnp.sum(jnp.where(slot == iota((FAR, SLOTS), 1), by_peer, 0.0), axis=1, keepdims=True)
    live = jnp.sum(
        jnp.where(peer_hot, jnp.broadcast_to(count[...], (FAR, PEERS)), 0).astype(F32),
        axis=1, keepdims=True,
    )
    row_of = jnp.where(slot.astype(F32) < live, chosen, -1.0).astype(I32)
    picks[...] = hot(row_of == iota((FAR, N), 1))

    def pack(values):
        send[...] = dot(picks[...], values).astype(BF).reshape(PEERS, SLOTS, D)

    pack(own[...])
    small_out[0] = jnp.broadcast_to(
        jnp.sum(jnp.where(labels[...] >= 0, 1.0, 0.0), axis=1, keepdims=True), (1, 128)
    )
    begin("c_barrier")
    pl.semaphore_wait(barrier, PEERS - 1)

    def sender(got, which):
        def one(k, to):
            pltpu.make_async_remote_copy(
                src_ref=send.at[k], dst_ref=got.at[k], send_sem=a_send.at[which],
                recv_sem=a_recv.at[which * 4 + k // 32], device_id=to, device_id_type=MESH,
            ).start()

        return one

    def small_sender(small, small_got):
        def one(k, to):
            pltpu.make_async_remote_copy(
                src_ref=small_out.at[small], dst_ref=small_got.at[k],
                send_sem=s_send.at[small], recv_sem=s_recv.at[small],
                device_id=to, device_id_type=MESH,
            ).start()

        return one

    def group_wait(got, which, g):
        part = pl.ds(0, 31 if g == 0 else 32)
        pltpu.make_async_copy(send.at[part], got.at[part], a_recv.at[which * 4 + g]).wait()

    rest = pl.ds(0, PEERS - 1)

    def sent_wait(got, which):
        pltpu.make_async_copy(send.at[rest], got.at[rest], a_send.at[which]).wait()

    def small_wait(which):
        pltpu.make_async_copy(counts.at[rest], totals.at[rest], s_send.at[which]).wait()
        pltpu.make_async_copy(counts.at[rest], totals.at[rest], s_recv.at[which]).wait()

    begin("d_send")
    everyone(ahead, sender(got_one, 0))
    got_one[0] = send[0]

    begin("e_adjacency")
    far_src = src[...] - N
    p = far_src >> 3
    o0 = (me[0] + 4 - (p >> 5)) & 3
    o1 = (me[1] + 4 - ((p >> 3) & 3)) & 3
    o2 = (me[2] + 4 - ((p >> 1) & 3)) & 3
    o3 = (core + 2 - (p & 1)) & 1
    code_of = o0 + (o1 << 2) + (o2 << 4) + (o3 << 6)
    where_src[...] = jnp.where(far_src >= 0, N + (code_of << 3) + (far_src & 7), src[...])

    def source_hot(r, b):
        halves = [
            hot(where_src[r, b : b + 1, 128 * i : 128 * (i + 1)] == row_code[...]) for i in range(2)
        ]
        return jnp.concatenate(halves, axis=1)

    def relation(r, carry):
        for b in range(2):
            at = slice(b * 128, (b + 1) * 128)
            dst_hot = hot(dst[r, b : b + 1, :] == iota((128, 256), 0))
            src_hot = source_hot(r, b)
            adj[r, at, :] = dot_nt(dst_hot, src_hot).astype(BF)
            live_edges = jnp.sum(dst_hot.astype(F32), axis=1, keepdims=True)
            norm[r, at, :] = jnp.broadcast_to(1.0 / jnp.maximum(live_edges, 1.0), (128, 128))
        return carry

    lax.fori_loop(0, REL, relation, 0)
    everyone(ahead, small_sender(0, counts))
    counts[0] = small_out[0]
    begin("f_local")

    def rows_of(got, g, count):
        return got[32 * g : 32 * (g + count)].reshape(256 * count, D)

    def columns(r, g, count):
        return adj[r, :, N + 256 * g : N + 256 * (g + count)]

    def gather_most(values, got, which):
        group_wait(got, which, 0)

        def near_rows(r, carry):
            sums[r] = dot(adj[r, :, :N], values[...]) + dot(columns(r, 0, 1), rows_of(got, 0, 1))
            return carry

        lax.fori_loop(0, REL, near_rows, 0, unroll=2)
        group_wait(got, which, 1)

        def middle_rows(r, carry):
            sums[r] += dot(columns(r, 1, 1), rows_of(got, 1, 1))
            return carry

        lax.fori_loop(0, REL, middle_rows, 0, unroll=2)

    def averaged(r, got):
        total = sums[r] + dot(columns(r, 2, 2), rows_of(got, 2, 2))
        return (total * norm[r, :, :1]).astype(BF)

    avg_one_t[REL * D :, :] = own[...].T
    for load in loads:
        load.wait()
    pre[...] = dot(own[...], w_one[REL])
    gather_most(own, got_one, 0)
    begin("g_wait")
    sent_wait(got_one, 0)
    group_wait(got_one, 0, 2)
    group_wait(got_one, 0, 3)

    begin("h_first")

    def first(r, carry):
        a = averaged(r, got_one)
        avg[r] = a
        pre[...] += dot(a, w_one[r])
        return carry

    lax.fori_loop(0, REL, first, 0, unroll=UNROLL)
    hidden[...] = jnp.maximum(pre[...], 0.0).astype(BF)
    begin("i_pack")
    pack(hidden[...])
    everyone(ahead, sender(got_two, 1))
    got_two[0] = send[0]

    begin("j_turns")

    def turn(r, out):
        out[pl.ds(pl.multiple_of(r * D, D), D), :] = avg[r].T

    def relation_t(r, carry):
        for b in range(2):
            dst_hot = hot(dst[r, b : b + 1, :] == iota((128, 256), 0))
            src_hot = source_hot(r, b)
            lanes = pl.ds(pl.multiple_of(r * N + b * 128, 128), 128)
            adj_t[:, lanes] = dot_nt(src_hot, dst_hot).astype(BF)
        turn(r, avg_one_t)
        return carry

    lax.fori_loop(0, REL, relation_t, 0)
    begin("ja_weights")

    for i in range(11):
        two_load(i).wait()
        at = pl.ds(i * 32, 32)
        for j in range(4):
            lanes = slice(128 * j, 128 * (j + 1))
            turned[j % 2] = w_two_raw[i % 4, :, :, lanes].astype(F32).reshape(32 * REL, 128)
            for r in range(REL):
                w_two[r, at, lanes] = turned[j % 2, pl.ds(r, 32, stride=REL), :].astype(BF)
        if i + 4 < 11:
            two_load(i + 4).start()

    begin("jb_picks")
    picks_t[...] = picks[...].T
    avg_two_t[REL * D :, :] = hidden[...].T
    acc[:, :C] = dot_nt(hidden[...], w_self[...])
    lab = jnp.broadcast_to(labels[...], (128, N)).T[:, :1]
    begin("jc_gather")
    gather_most(hidden, got_two, 1)
    begin("k_wait")
    small_wait(0)
    labelled_count = jnp.sum(counts[:, :, 0:1])
    sent_wait(got_two, 1)
    group_wait(got_two, 1, 2)
    group_wait(got_two, 1, 3)

    begin("l_second")

    def second(r, carry):
        a = averaged(r, got_two)
        avg[r] = a
        acc[:, :C] += dot_nt(a, w_two[r, :C, :])
        return carry

    lax.fori_loop(0, REL, second, 0, unroll=UNROLL)
    begin("m_soft")
    out = acc[:, :C]
    labelled = lab >= 0
    top = jnp.max(out, axis=1, keepdims=True)
    log_total = jnp.log(jnp.sum(jnp.exp(out - top), axis=1, keepdims=True)) + top
    label_hot = jnp.where(lab == iota((N, C), 1), 1.0, 0.0)
    picked = jnp.sum(out * label_hot, axis=1, keepdims=True)
    soft = jnp.exp(out - log_total)
    mask = jnp.where(labelled, 1.0, 0.0)
    grad[...] = jnp.zeros_like(grad)
    grad[:, :C] = (loss_scale * (soft - label_hot) * mask / labelled_count).astype(BF)
    small_out[1] = jnp.broadcast_to(
        jnp.sum(jnp.where(labelled, log_total - picked, 0.0), axis=0, keepdims=True), (1, 128)
    )

    begin("n_spread")

    def spread(r, carry):
        at = pl.ds(pl.multiple_of(r * N, N), N)
        spreads[at, :] = (dot(grad[:, :C], w_two[r, :C, :]) * norm[r, :, :1]).astype(BF)
        return carry

    lax.fori_loop(0, REL, spread, 0, unroll=UNROLL)
    begin("o_send")
    got_three = got_one
    back = sender(got_three, 2)
    for g in range(4):
        group = dot(adj_t[N + 256 * g : N + 256 * (g + 1), :], spreads[...])
        send[32 * g : 32 * (g + 1)] = group.astype(BF).reshape(32, SLOTS, D)
        everyone(behind, back, max(1, 32 * g), 32 * (g + 1))
    got_three[0] = send[0]

    begin("p_two")
    partner = (me[0], me[1], me[2], 1 - core)

    def chunks(x, h, left, right, lanes):
        start = pl.multiple_of((x * 2 + h) * BLOCK, BLOCK)
        value = dot(left[pl.ds(start, BLOCK), :], right[...]).astype(BF)
        for j in range(16):
            to = (x, h * 2 + j // 8, (j // 2) % 4, j % 2)
            parts[(*to, slice(None), lanes)] = value[ROWS * j : ROWS * (j + 1), :]

    def to_partner(x, lanes, sem):
        return pltpu.make_async_remote_copy(
            src_ref=parts.at[x, :, :, 1 - core, :, lanes], dst_ref=half.at[x, :, :, :, lanes],
            send_sem=p_send.at[sem], recv_sem=p_recv.at[sem], device_id=partner,
            device_id_type=MESH,
        )

    def add_near(x, z, lanes):
        half[x, z, :, :, lanes] += parts[x, z, :, core, :, lanes]

    two_lanes = pl.ds(D, CP)
    one_lanes = pl.ds(0, D)

    def turn_two(r, carry):
        turn(r, avg_two_t)
        return carry

    lax.fori_loop(0, REL, turn_two, 0)

    for x in range(4):

        def two_chunks(i, carry):
            chunks(x, i, avg_two_t, grad, two_lanes)
            return carry

        lax.fori_loop(0, 2, two_chunks, 0)
        to_partner(x, two_lanes, 4 + x).start()
    logits_v[...] = acc[...].T[:C, :]
    logits_copy = pltpu.make_async_copy(logits_v, logits_t, w_sems.at[13])
    logits_copy.start()
    own_grad[...] = dot(adj_t[:N, :], spreads[...]) + dot(grad[:, :C], w_self[...])
    for x in range(4):
        to_partner(x, two_lanes, 4 + x).wait()

        def add_two(i, carry):
            add_near(x, i, two_lanes)
            return carry

        lax.fori_loop(0, 4, add_two, 0, unroll=2)

    everyone(ahead, small_sender(1, totals))
    totals[0] = small_out[1]

    def to_axis(axis, step):
        to = list(me)
        to[axis] = lax.rem(me[axis] + step, 4)
        return tuple(to), to[axis]

    def cut(s, upper):
        _, row, rows_s, _ = STREAMS[s]
        low = 16 if rows_s > 12 else 8
        return (row + low, low, rows_s - low) if upper else (row, 0, low)

    def first_at(s, k, row, size):
        lane, _, _, order = STREAMS[s]
        at = tuple(k if a == order[0] else slice(None) for a in range(3))
        return (*at, pl.ds(row, size), pl.ds(lane, 128))

    def first_hop(s, kind, forward):
        axis = STREAMS[s][3][0]
        to, k = to_axis(axis, 1 if forward else 3)
        row, inner, size = cut(s, forward if kind == "own" else not forward)
        if kind == "far":
            k = lax.rem(me[axis] + 2, 4)
            slot = 2
        else:
            slot = 0 if forward else 1
        sem = s * 12 + {"far": 0, "own": 2, "both": 4}[kind] + (0 if forward else 1)
        return pltpu.make_async_remote_copy(
            src_ref=half.at[first_at(s, k, row, size)],
            dst_ref=first_got[s].at[slot, :, :, pl.ds(inner, size), :],
            send_sem=x_send.at[sem], recv_sem=x_recv.at[sem], device_id=to, device_id_type=MESH,
        )

    def relay(s):
        axis = STREAMS[s][3][0]
        for forward in (True, False):
            first_hop(s, "far", forward).wait()
            _, k = to_axis(axis, 1 if forward else 3)
            row, inner, size = cut(s, not forward)
            at = first_at(s, k, row, size)
            half[at] += first_got[s][2, :, :, inner : inner + size, :]
            first_hop(s, "both", forward).start()

    def hop(s, phase, j):
        order = STREAMS[s][3]
        axis = order[phase]
        to, k = to_axis(axis, j)
        if phase == 1:
            at = tuple(k if a == axis else slice(None) for a in sorted(order[1:]))
            ref = first_sum[s].at[at]
            got = second_got[s]
        else:
            ref = second_sum[s].at[k]
            got = third_got[s]
        sem = s * 12 + 3 + phase * 3 + j - 1
        return pltpu.make_async_remote_copy(
            src_ref=ref, dst_ref=got.at[j - 1], send_sem=x_send.at[sem], recv_sem=x_recv.at[sem],
            device_id=to, device_id_type=MESH,
        )

    def first_start(s):
        for kind in ("far", "own"):
            for forward in (True, False):
                first_hop(s, kind, forward).start()

    for s in TWO:
        first_start(s)
    begin("q_wait")
    sent_wait(got_three, 2)
    for g in range(4):
        group_wait(got_three, 2, g)

    begin("r_gradpre")
    grad_hidden = own_grad[...] + dot(picks_t[...], got_three[...].reshape(FAR, D))
    grad_pre[...] = jnp.where(pre[...] > 0.0, grad_hidden, 0.0).astype(BF)

    begin("s_one")

    def one_block(j):
        k = lax.rem(me[0] + j, 4)

        def one_chunks(i, carry):
            chunks(k, i, avg_one_t, grad_pre, one_lanes)
            return carry

        lax.fori_loop(0, 2, one_chunks, 0)
        to_partner(k, one_lanes, j).start()

    def one_near(j):
        k = lax.rem(me[0] + j, 4)
        to_partner(k, one_lanes, j).wait()

        def add_one(i, carry):
            add_near(k, i, one_lanes)
            return carry

        lax.fori_loop(0, 4, add_one, 0, unroll=2)
        for s in ONE_X:
            if j == 2:
                first_hop(s, "far", True).start()
                first_hop(s, "far", False).start()
            elif j:
                first_hop(s, "own", j == 1).start()

    one_block(2)
    one_block(1)
    for s in TWO:
        relay(s)
    one_block(3)
    one_near(2)
    one_block(0)
    one_near(1)
    one_near(3)
    one_near(0)
    begin("t_near")
    for s in ONE_REST:
        first_start(s)
    begin("ta_relay")
    for s in READY[3:]:
        relay(s)

    def sum_first(s):
        lane, row, rows_s, order = STREAMS[s]
        for kind in ("own", "both"):
            for forward in (True, False):
                first_hop(s, kind, forward).wait()

        def body(i, carry):
            at = [None, None, None]
            left = sorted(order[1:])
            at[order[0]] = me[order[0]]
            at[left[0]] = i
            at[left[1]] = slice(None)
            total = half[(*at, pl.ds(row, rows_s), pl.ds(lane, 128))].astype(F32)
            for j in range(2):
                total += first_got[s][j, i].astype(F32)
            first_sum[s][i] = total.astype(BF)
            return carry

        lax.fori_loop(0, 4, body, 0)
        for j in (2, 1, 3):
            hop(s, 1, j).start()

    def sum_second(s):
        order = STREAMS[s][3]
        for j in (1, 2, 3):
            hop(s, 1, j).wait()
        m = me[order[1]]
        if order[1] < order[2]:
            total = first_sum[s][m].astype(F32)
        else:
            total = first_sum[s][:, m].astype(F32)
        for j in range(3):
            total += second_got[s][j].astype(F32)
        second_sum[s][...] = total.astype(BF)
        for j in (2, 1, 3):
            hop(s, 2, j).start()

    def sum_third(s):
        order = STREAMS[s][3]
        for j in (1, 2, 3):
            hop(s, 2, j).wait()
        total = second_sum[s][me[order[2]]].astype(F32)
        for j in range(3):
            total += third_got[s][j].astype(F32)
        return total

    begin("u_first")
    for s in READY:
        sum_first(s)
    begin("v_second")
    for s in READY:
        sum_second(s)
    begin("w_third")
    small_wait(1)
    loss_v[...] = jnp.broadcast_to(jnp.sum(totals[:, :, 0:1]) / labelled_count, (1, 128))
    results = [logits_copy]

    def result(value, out, at):
        copy = pltpu.make_async_copy(value, out, w_sems.at[at])
        copy.start()
        results.append(copy)

    result(loss_v, loss, 14)
    for i, s in enumerate(READY):
        lane, row, rows_s, _ = STREAMS[s]
        total = sum_third(s)
        if lane < D:
            one_v[row : row + rows_s, lane : lane + 128] = total
        else:
            lane -= D
            size = min(128, C - lane)
            two_v[:, lane : lane + size] = total[:, :size]
        if i == 2:
            result(two_v, grad_two, 15)
    result(one_v, grad_one, 16)
    for copy in results:
        copy.wait()
    begin(None)


def finish_body(a, b, c, d, a_out, b_out, c_out, d_out, b_row, sems):
    copies = [
        pltpu.make_async_copy(x, y, sems.at[i])
        for i, (x, y) in enumerate(((a, a_out), (b, b_row), (c, c_out), (d, d_out)))
    ]
    for copy in copies:
        copy.start()
    for copy in copies:
        copy.wait()
    b_out[...] = b_row[:, :1]


def sds(shape, dtype):
    return jax.ShapeDtypeStruct(shape, dtype)


def on_device(features, w_one, w_two, self_two, edge_src, edge_dst, send_rows, send_count, labels):
    vm = pl.BlockSpec(memory_space=pltpu.VMEM)
    hbm = pl.BlockSpec(memory_space=pl.ANY)
    V = pltpu.VMEM
    rows = [s[2] for s in STREAMS]
    scratch = [
        V((N, D), BF), V((REL, 2, N), I32), V((REL, 2, N), I32), V((SLOTS, PEERS), I32),
        V((1, PEERS), I32), V((1, N), I32),
        V((REL + 1, D, D), BF), V((REL, 352, D), BF), V((4, 32, REL, D), BF), V((2, 256, 128), F32),
        V((C, D), BF), V((REL, 2, N), I32), V((TABLE, 128), I32),
        V((REL, N, TABLE), BF), V((TABLE, REL * N), BF), V((REL, N, 128), F32),
        V((FAR, N), BF), V((N, FAR), BF),
        V((PEERS, SLOTS, D), BF), V((PEERS, SLOTS, D), BF), V((PEERS, SLOTS, D), BF),
        V((REL, N, D), F32), V((REL, N, D), BF), V(((REL + 1) * D, N), BF), V(((REL + 1) * D, N), BF),
        V((N, D), F32), V((N, D), BF), V((N, CP), F32), V((C, N), F32), V((1, 128), F32), V((ROWS, D), F32), V((ROWS, C), F32),
        V((N, D), F32),
        V((REL * N, D), BF),
        V((N, CP), BF), V((N, D), BF),
        V((2, 1, 128), F32), V((PEERS, 1, 128), F32), V((PEERS, 1, 128), F32),
        V((4, 4, 4, 2, ROWS, WIDE), BF), V((4, 4, 4, ROWS, WIDE), BF),
        *[V((3, 4, 4, r, 128), BF) for r in rows],
        *[V((4, 4, r, 128), BF) for r in rows],
        *[V((3, 4, r, 128), BF) for r in rows],
        *[V((4, r, 128), BF) for r in rows],
        *[V((3, r, 128), BF) for r in rows],
        pltpu.SemaphoreType.DMA((17,)),
        pltpu.SemaphoreType.DMA((3,)), pltpu.SemaphoreType.DMA((12,)),
        pltpu.SemaphoreType.DMA((2,)), pltpu.SemaphoreType.DMA((2,)),
        pltpu.SemaphoreType.DMA((8,)), pltpu.SemaphoreType.DMA((8,)),
        pltpu.SemaphoreType.DMA((96,)), pltpu.SemaphoreType.DMA((96,)),
    ]
    codes = np.concatenate(
        [np.arange(N)] + [N + SLOTS * code + np.arange(SLOTS) for code in ORDER]
    ).astype(np.int32)
    logits_t, loss, grad_one, grad_two = pl.pallas_call(
        step_body,
        name="step",
        in_specs=[hbm] * 10,
        out_specs=[hbm] * 4,
        out_shape=[sds((C, N), F32), sds((1, 128), F32), sds((ROWS, D), F32), sds((ROWS, C), F32)],
        scratch_shapes=scratch,
        compiler_params=pltpu.CompilerParams(
            collective_id=0, has_side_effects=True, vmem_limit_bytes=int(VLIM * MB)
        ),
    )(
        features, w_one, jnp.transpose(w_two, (2, 0, 1)), self_two.T, edge_src, edge_dst,
        send_rows[0].T, send_count, labels.reshape(1, N),
        jnp.asarray(np.repeat(codes[:, None], 128, axis=1)),
    )
    logits_t, loss, grad_one, grad_two = pl.pallas_call(
        finish_body,
        name="finish",
        in_specs=[hbm] * 4,
        out_specs=[vm] * 4,
        out_shape=[sds((C, N), F32), sds((1, 1), F32), sds((ROWS, D), F32), sds((ROWS, C), F32)],
        scratch_shapes=[V((1, 128), F32), pltpu.SemaphoreType.DMA((4,))],
        compiler_params=pltpu.CompilerParams(vmem_limit_bytes=63 * MB),
    )(logits_t, loss, grad_one, grad_two)
    return (logits_t.T, loss[0, 0], grad_one, grad_two)


def solution(mesh):
    split = Mesh(mesh.devices.reshape(SIZES), DOM)
    return jax.shard_map(
        on_device,
        mesh=split,
        in_specs=(
            P(DOM, None),
            P(),
            P(),
            P(),
            P(None, DOM, None),
            P(None, DOM, None),
            P(DOM, None, None),
            P(DOM, None),
            P(DOM),
        ),
        out_specs=(P(DOM, None), P(), P(DOM, None), P(DOM, None)),
        check_vma=False,
    )
```

```python
import jax
import jax.numpy as jnp
import numpy as np
from jax import lax
from jax.experimental import pallas as pl
from jax.experimental.pallas import tpu as pltpu
from jax.sharding import Mesh
from jax.sharding import PartitionSpec as P

DOM = ("dom_0", "dom_1", "dom_2", "dom_3")
SIZES = (4, 4, 4, 2)
BF = jnp.bfloat16
F32 = jnp.float32
I32 = jnp.int32
MESH = pl.DeviceIdType.MESH
loss_scale = 256.0
MB = 1 << 20
VLIM = 63
UNROLL = 4

PEERS = 128
CHIPS = 64
SLOTS = 8
REL = 8
N = 256
D = 512
C = 349
CP = 384
FAR = PEERS * SLOTS
TABLE = N + FAR
ROWS = 36
WIDE = D + CP
BLOCK = 16 * ROWS

STREAMS = (
    (0, 0, 36, (0, 1, 2)),
    (384, 0, 24, (0, 1, 2)),
    (128, 0, 36, (1, 2, 0)),
    (384, 24, 12, (1, 2, 0)),
    (256, 0, 36, (2, 0, 1)),
    (512, 0, 36, (0, 1, 2)),
    (640, 0, 24, (1, 2, 0)),
    (768, 0, 36, (2, 0, 1)),
    (640, 24, 12, (2, 0, 1)),
)
ONE_X, ONE_REST, TWO = (0, 1), (2, 3, 4), (5, 6, 7, 8)
READY = (5, 6, 7, 8, 0, 1, 4, 2, 3)


def hops(code):
    return sum(min(d, 4 - d) for d in digits(code)[:3])


def digits(code):
    return (code % 4, code // 4 % 4, code // 16 % 4, code // 64)


def block_order():
    spread = []
    for k in range(1, PEERS):
        d0 = k % 4
        d1 = (k // 4 + d0) % 4
        d2 = (k // 16 + d1) % 4
        spread.append(d0 + 4 * d1 + 16 * d2 + 64 * (k // 64))
    return [0] + sorted(spread, key=lambda code: -hops(code))


ORDER = block_order()


def dot(a, b):
    return jnp.dot(a, b, preferred_element_type=F32)


def dot_nt(a, b):
    return lax.dot_general(a, b, (((1,), (1,)), ((), ())), preferred_element_type=F32)


def iota(shape, dim):
    return lax.broadcasted_iota(I32, shape, dim)


def hot(mask):
    return jnp.where(mask, 1.0, 0.0).astype(BF)


def phases():
    now = []

    def begin(name):
        if now:
            now.pop().__exit__(None, None, None)
        if name:
            now.append(jax.named_scope(name))
            now[0].__enter__()

    return begin


def step_body(
    own_hbm, w_one_hbm, w_two_hbm, w_self_hbm, src_hbm, dst_hbm, rows_hbm, count_hbm, labels_hbm,
    codes_hbm,
    logits_t, loss, grad_one, grad_two,
    own, src, dst, rows, count, labels, w_one, w_two, w_two_raw, turned, w_self, where_src, row_code, adj, adj_t, norm, picks, picks_t,
    send, got_one, got_two, sums, avg, avg_one_t, avg_two_t,
    pre, hidden, acc, logits_v, loss_v, one_v, two_v, own_grad, spreads, grad, grad_pre,
    small_out, counts, totals,
    parts, half, *rest_refs,
):
    begin = phases()
    count_s = len(STREAMS)
    first_got, first_sum, second_got, second_sum, third_got = (
        rest_refs[i * count_s : (i + 1) * count_s] for i in range(5)
    )
    w_sems, a_send, a_recv, s_send, s_recv, p_send, p_recv, x_send, x_recv = rest_refs[5 * count_s :]
    me = [lax.axis_index(a) for a in DOM]
    mine = ((me[0] * 4 + me[1]) * 4 + me[2]) * 2 + me[3]
    core = me[3]

    begin("a_greet")
    loads = [
        pltpu.make_async_copy(w_one_hbm, w_one, w_sems.at[0]),
        pltpu.make_async_copy(w_self_hbm, w_self, w_sems.at[1]),
    ]

    def two_load(i):
        count = min(32, C - 32 * i)
        return pltpu.make_async_copy(
            w_two_hbm.at[pl.ds(32 * i, count)], w_two_raw.at[i % 4, pl.ds(0, count)],
            w_sems.at[2 + i % 4],
        )

    inputs = [
        pltpu.make_async_copy(a, b, w_sems.at[6 + i])
        for i, (a, b) in enumerate(
            (
                (codes_hbm, row_code), (rows_hbm, rows), (count_hbm, count), (own_hbm, own),
                (labels_hbm, labels), (src_hbm, src), (dst_hbm, dst),
            )
        )
    ]
    for load in inputs + loads + [two_load(i) for i in range(4)]:
        load.start()

    ahead = [[lax.rem(m + d, n) for d in range(n)] for m, n in zip(me, SIZES)]
    behind = [[lax.rem(m + n - d, n) for d in range(n)] for m, n in zip(me, SIZES)]

    def everyone(where, body, start=1, stop=PEERS):
        for k in range(start, stop):
            body(k, tuple(where[i][d] for i, d in enumerate(digits(ORDER[k]))))

    barrier = pltpu.get_barrier_semaphore()

    def greet(k, to):
        pl.semaphore_signal(barrier, inc=1, device_id=to, device_id_type=MESH)

    everyone(ahead, greet)

    begin("b_pack")
    for load in inputs:
        load.wait()
    spot = row_code[N:, :1] - N
    code = spot >> 3
    peer = (
        (((me[0] + code) & 3) << 5) + (((me[1] + (code >> 2)) & 3) << 3)
        + (((me[2] + (code >> 4)) & 3) << 1) + ((core + (code >> 6)) & 1)
    )
    peer_hot = peer == iota((FAR, PEERS), 1)
    by_peer = dot_nt(hot(peer_hot), rows[...].astype(F32).astype(BF))
    slot = spot & 7
    chosen = jnp.sum(jnp.where(slot == iota((FAR, SLOTS), 1), by_peer, 0.0), axis=1, keepdims=True)
    live = jnp.sum(
        jnp.where(peer_hot, jnp.broadcast_to(count[...], (FAR, PEERS)), 0).astype(F32),
        axis=1, keepdims=True,
    )
    row_of = jnp.where(slot.astype(F32) < live, chosen, -1.0).astype(I32)
    picks[...] = hot(row_of == iota((FAR, N), 1))

    def pack(values):
        send[...] = dot(picks[...], values).astype(BF).reshape(PEERS, SLOTS, D)

    pack(own[...])
    small_out[0] = jnp.broadcast_to(
        jnp.sum(jnp.where(labels[...] >= 0, 1.0, 0.0), axis=1, keepdims=True), (1, 128)
    )
    begin("c_barrier")
    pl.semaphore_wait(barrier, PEERS - 1)

    def sender(got, which):
        def one(k, to):
            pltpu.make_async_remote_copy(
                src_ref=send.at[k], dst_ref=got.at[k], send_sem=a_send.at[which],
                recv_sem=a_recv.at[which * 4 + k // 32], device_id=to, device_id_type=MESH,
            ).start()

        return one

    def small_sender(small, small_got):
        def one(k, to):
            pltpu.make_async_remote_copy(
                src_ref=small_out.at[small], dst_ref=small_got.at[k],
                send_sem=s_send.at[small], recv_sem=s_recv.at[small],
                device_id=to, device_id_type=MESH,
            ).start()

        return one

    def group_wait(got, which, g):
        part = pl.ds(0, 31 if g == 0 else 32)
        pltpu.make_async_copy(send.at[part], got.at[part], a_recv.at[which * 4 + g]).wait()

    rest = pl.ds(0, PEERS - 1)

    def sent_wait(got, which):
        pltpu.make_async_copy(send.at[rest], got.at[rest], a_send.at[which]).wait()

    def small_wait(which):
        pltpu.make_async_copy(counts.at[rest], totals.at[rest], s_send.at[which]).wait()
        pltpu.make_async_copy(counts.at[rest], totals.at[rest], s_recv.at[which]).wait()

    begin("d_send")
    everyone(ahead, sender(got_one, 0))
    got_one[0] = send[0]

    begin("e_adjacency")
    far_src = src[...] - N
    p = far_src >> 3
    o0 = (me[0] + 4 - (p >> 5)) & 3
    o1 = (me[1] + 4 - ((p >> 3) & 3)) & 3
    o2 = (me[2] + 4 - ((p >> 1) & 3)) & 3
    o3 = (core + 2 - (p & 1)) & 1
    code_of = o0 + (o1 << 2) + (o2 << 4) + (o3 << 6)
    where_src[...] = jnp.where(far_src >= 0, N + (code_of << 3) + (far_src & 7), src[...])

    def source_hot(r, b):
        halves = [
            hot(where_src[r, b : b + 1, 128 * i : 128 * (i + 1)] == row_code[...]) for i in range(2)
        ]
        return jnp.concatenate(halves, axis=1)

    def relation(r, carry):
        for b in range(2):
            at = slice(b * 128, (b + 1) * 128)
            dst_hot = hot(dst[r, b : b + 1, :] == iota((128, 256), 0))
            src_hot = source_hot(r, b)
            adj[r, at, :] = dot_nt(dst_hot, src_hot).astype(BF)
            live_edges = jnp.sum(dst_hot.astype(F32), axis=1, keepdims=True)
            norm[r, at, :] = jnp.broadcast_to(1.0 / jnp.maximum(live_edges, 1.0), (128, 128))
        return carry

    lax.fori_loop(0, REL, relation, 0, unroll=UNROLL)
    everyone(ahead, small_sender(0, counts))
    counts[0] = small_out[0]
    begin("f_local")

    def rows_of(got, g, count):
        return got[32 * g : 32 * (g + count)].reshape(256 * count, D)

    def columns(r, g, count):
        return adj[r, :, N + 256 * g : N + 256 * (g + count)]

    def gather_most(values, got, which):
        group_wait(got, which, 0)

        def near_rows(r, carry):
            sums[r] = dot(adj[r, :, :N], values[...]) + dot(columns(r, 0, 1), rows_of(got, 0, 1))
            return carry

        lax.fori_loop(0, REL, near_rows, 0, unroll=UNROLL)
        group_wait(got, which, 1)

        def middle_rows(r, carry):
            sums[r] += dot(columns(r, 1, 1), rows_of(got, 1, 1))
            return carry

        lax.fori_loop(0, REL, middle_rows, 0, unroll=UNROLL)

    def averaged(r, got):
        total = sums[r] + dot(columns(r, 2, 2), rows_of(got, 2, 2))
        return (total * norm[r, :, :1]).astype(BF)

    avg_one_t[REL * D :, :] = own[...].T
    for load in loads:
        load.wait()
    pre[...] = dot(own[...], w_one[REL])
    gather_most(own, got_one, 0)
    begin("g_wait")
    sent_wait(got_one, 0)
    group_wait(got_one, 0, 2)
    group_wait(got_one, 0, 3)

    begin("h_first")

    def first(r, carry):
        a = averaged(r, got_one)
        avg[r] = a
        pre[...] += dot(a, w_one[r])
        return carry

    lax.fori_loop(0, REL, first, 0, unroll=UNROLL)
    hidden[...] = jnp.maximum(pre[...], 0.0).astype(BF)
    begin("i_pack")
    pack(hidden[...])
    everyone(ahead, sender(got_two, 1))
    got_two[0] = send[0]

    begin("j_turns")

    def turn(r, out):
        out[pl.ds(pl.multiple_of(r * D, D), D), :] = avg[r].T

    def relation_t(r, carry):
        for b in range(2):
            dst_hot = hot(dst[r, b : b + 1, :] == iota((128, 256), 0))
            src_hot = source_hot(r, b)
            lanes = pl.ds(pl.multiple_of(r * N + b * 128, 128), 128)
            adj_t[:, lanes] = dot_nt(src_hot, dst_hot).astype(BF)
        turn(r, avg_one_t)
        return carry

    lax.fori_loop(0, REL, relation_t, 0, unroll=UNROLL)
    begin("ja_weights")

    for i in range(11):
        two_load(i).wait()
        at = pl.ds(i * 32, 32)
        for j in range(4):
            lanes = slice(128 * j, 128 * (j + 1))
            turned[j % 2] = w_two_raw[i % 4, :, :, lanes].astype(F32).reshape(32 * REL, 128)
            for r in range(REL):
                w_two[r, at, lanes] = turned[j % 2, pl.ds(r, 32, stride=REL), :].astype(BF)
        if i + 4 < 11:
            two_load(i + 4).start()

    begin("jb_picks")
    picks_t[...] = picks[...].T
    avg_two_t[REL * D :, :] = hidden[...].T
    acc[:, :C] = dot_nt(hidden[...], w_self[...])
    lab = jnp.broadcast_to(labels[...], (128, N)).T[:, :1]
    begin("jc_gather")
    gather_most(hidden, got_two, 1)
    begin("k_wait")
    small_wait(0)
    labelled_count = jnp.sum(counts[:, :, 0:1])
    sent_wait(got_two, 1)
    group_wait(got_two, 1, 2)
    group_wait(got_two, 1, 3)

    begin("l_second")

    def second(r, carry):
        a = averaged(r, got_two)
        avg[r] = a
        acc[:, :C] += dot_nt(a, w_two[r, :C, :])
        return carry

    lax.fori_loop(0, REL, second, 0, unroll=UNROLL)
    begin("m_soft")
    out = acc[:, :C]
    labelled = lab >= 0
    top = jnp.max(out, axis=1, keepdims=True)
    log_total = jnp.log(jnp.sum(jnp.exp(out - top), axis=1, keepdims=True)) + top
    label_hot = jnp.where(lab == iota((N, C), 1), 1.0, 0.0)
    picked = jnp.sum(out * label_hot, axis=1, keepdims=True)
    soft = jnp.exp(out - log_total)
    mask = jnp.where(labelled, 1.0, 0.0)
    grad[...] = jnp.zeros_like(grad)
    grad[:, :C] = (loss_scale * (soft - label_hot) * mask / labelled_count).astype(BF)
    small_out[1] = jnp.broadcast_to(
        jnp.sum(jnp.where(labelled, log_total - picked, 0.0), axis=0, keepdims=True), (1, 128)
    )

    begin("n_spread")

    def spread(r, carry):
        at = pl.ds(pl.multiple_of(r * N, N), N)
        spreads[at, :] = (dot(grad[:, :C], w_two[r, :C, :]) * norm[r, :, :1]).astype(BF)
        return carry

    lax.fori_loop(0, REL, spread, 0, unroll=UNROLL)
    begin("o_send")
    got_three = got_one
    back = sender(got_three, 2)
    for g in range(4):
        group = dot(adj_t[N + 256 * g : N + 256 * (g + 1), :], spreads[...])
        send[32 * g : 32 * (g + 1)] = group.astype(BF).reshape(32, SLOTS, D)
        everyone(behind, back, max(1, 32 * g), 32 * (g + 1))
    got_three[0] = send[0]

    begin("p_two")
    partner = (me[0], me[1], me[2], 1 - core)

    def chunks(x, h, left, right, lanes):
        start = pl.multiple_of((x * 2 + h) * BLOCK, BLOCK)
        value = dot(left[pl.ds(start, BLOCK), :], right[...]).astype(BF)
        for j in range(16):
            to = (x, h * 2 + j // 8, (j // 2) % 4, j % 2)
            parts[(*to, slice(None), lanes)] = value[ROWS * j : ROWS * (j + 1), :]

    def to_partner(x, lanes, sem):
        return pltpu.make_async_remote_copy(
            src_ref=parts.at[x, :, :, 1 - core, :, lanes], dst_ref=half.at[x, :, :, :, lanes],
            send_sem=p_send.at[sem], recv_sem=p_recv.at[sem], device_id=partner,
            device_id_type=MESH,
        )

    def add_near(x, z, lanes):
        half[x, z, :, :, lanes] += parts[x, z, :, core, :, lanes]

    two_lanes = pl.ds(D, CP)
    one_lanes = pl.ds(0, D)

    def turn_two(r, carry):
        turn(r, avg_two_t)
        return carry

    lax.fori_loop(0, REL, turn_two, 0)

    for x in range(4):

        def two_chunks(i, carry):
            chunks(x, i, avg_two_t, grad, two_lanes)
            return carry

        lax.fori_loop(0, 2, two_chunks, 0)
        to_partner(x, two_lanes, 4 + x).start()
    logits_v[...] = acc[...].T[:C, :]
    logits_copy = pltpu.make_async_copy(logits_v, logits_t, w_sems.at[13])
    logits_copy.start()
    own_grad[...] = dot(adj_t[:N, :], spreads[...]) + dot(grad[:, :C], w_self[...])
    for x in range(4):
        to_partner(x, two_lanes, 4 + x).wait()

        def add_two(i, carry):
            add_near(x, i, two_lanes)
            return carry

        lax.fori_loop(0, 4, add_two, 0, unroll=2)

    everyone(ahead, small_sender(1, totals))
    totals[0] = small_out[1]

    def to_axis(axis, step):
        to = list(me)
        to[axis] = lax.rem(me[axis] + step, 4)
        return tuple(to), to[axis]

    def cut(s, upper):
        _, row, rows_s, _ = STREAMS[s]
        low = 16 if rows_s > 12 else 8
        return (row + low, low, rows_s - low) if upper else (row, 0, low)

    def first_at(s, k, row, size):
        lane, _, _, order = STREAMS[s]
        at = tuple(k if a == order[0] else slice(None) for a in range(3))
        return (*at, pl.ds(row, size), pl.ds(lane, 128))

    def first_hop(s, kind, forward):
        axis = STREAMS[s][3][0]
        to, k = to_axis(axis, 1 if forward else 3)
        row, inner, size = cut(s, forward if kind == "own" else not forward)
        if kind == "far":
            k = lax.rem(me[axis] + 2, 4)
            slot = 2
        else:
            slot = 0 if forward else 1
        sem = s * 12 + {"far": 0, "own": 2, "both": 4}[kind] + (0 if forward else 1)
        return pltpu.make_async_remote_copy(
            src_ref=half.at[first_at(s, k, row, size)],
            dst_ref=first_got[s].at[slot, :, :, pl.ds(inner, size), :],
            send_sem=x_send.at[sem], recv_sem=x_recv.at[sem], device_id=to, device_id_type=MESH,
        )

    def relay(s):
        axis = STREAMS[s][3][0]
        for forward in (True, False):
            first_hop(s, "far", forward).wait()
            _, k = to_axis(axis, 1 if forward else 3)
            row, inner, size = cut(s, not forward)
            at = first_at(s, k, row, size)
            half[at] += first_got[s][2, :, :, inner : inner + size, :]
            first_hop(s, "both", forward).start()

    def hop(s, phase, j):
        order = STREAMS[s][3]
        axis = order[phase]
        to, k = to_axis(axis, j)
        if phase == 1:
            at = tuple(k if a == axis else slice(None) for a in sorted(order[1:]))
            ref = first_sum[s].at[at]
            got = second_got[s]
        else:
            ref = second_sum[s].at[k]
            got = third_got[s]
        sem = s * 12 + 3 + phase * 3 + j - 1
        return pltpu.make_async_remote_copy(
            src_ref=ref, dst_ref=got.at[j - 1], send_sem=x_send.at[sem], recv_sem=x_recv.at[sem],
            device_id=to, device_id_type=MESH,
        )

    def first_start(s):
        for kind in ("far", "own"):
            for forward in (True, False):
                first_hop(s, kind, forward).start()

    for s in TWO:
        first_start(s)
    begin("q_wait")
    sent_wait(got_three, 2)
    for g in range(4):
        group_wait(got_three, 2, g)

    begin("r_gradpre")
    grad_hidden = own_grad[...] + dot(picks_t[...], got_three[...].reshape(FAR, D))
    grad_pre[...] = jnp.where(pre[...] > 0.0, grad_hidden, 0.0).astype(BF)

    begin("s_one")

    def one_block(j):
        k = lax.rem(me[0] + j, 4)

        def one_chunks(i, carry):
            chunks(k, i, avg_one_t, grad_pre, one_lanes)
            return carry

        lax.fori_loop(0, 2, one_chunks, 0)
        to_partner(k, one_lanes, j).start()

    def one_near(j):
        k = lax.rem(me[0] + j, 4)
        to_partner(k, one_lanes, j).wait()

        def add_one(i, carry):
            add_near(k, i, one_lanes)
            return carry

        lax.fori_loop(0, 4, add_one, 0, unroll=2)
        for s in ONE_X:
            if j == 2:
                first_hop(s, "far", True).start()
                first_hop(s, "far", False).start()
            elif j:
                first_hop(s, "own", j == 1).start()

    one_block(2)
    one_block(1)
    for s in TWO:
        relay(s)
    one_block(3)
    one_near(2)
    one_block(0)
    one_near(1)
    one_near(3)
    one_near(0)
    begin("t_near")
    for s in ONE_REST:
        first_start(s)
    begin("ta_relay")
    for s in READY[4:]:
        relay(s)

    def sum_first(s):
        lane, row, rows_s, order = STREAMS[s]
        for kind in ("own", "both"):
            for forward in (True, False):
                first_hop(s, kind, forward).wait()

        def body(i, carry):
            at = [None, None, None]
            left = sorted(order[1:])
            at[order[0]] = me[order[0]]
            at[left[0]] = i
            at[left[1]] = slice(None)
            total = half[(*at, pl.ds(row, rows_s), pl.ds(lane, 128))].astype(F32)
            for j in range(2):
                total += first_got[s][j, i].astype(F32)
            first_sum[s][i] = total.astype(BF)
            return carry

        lax.fori_loop(0, 4, body, 0)
        for j in (2, 1, 3):
            hop(s, 1, j).start()

    def sum_second(s):
        order = STREAMS[s][3]
        for j in (1, 2, 3):
            hop(s, 1, j).wait()
        m = me[order[1]]
        if order[1] < order[2]:
            total = first_sum[s][m].astype(F32)
        else:
            total = first_sum[s][:, m].astype(F32)
        for j in range(3):
            total += second_got[s][j].astype(F32)
        second_sum[s][...] = total.astype(BF)
        for j in (2, 1, 3):
            hop(s, 2, j).start()

    def sum_third(s):
        order = STREAMS[s][3]
        for j in (1, 2, 3):
            hop(s, 2, j).wait()
        total = second_sum[s][me[order[2]]].astype(F32)
        for j in range(3):
            total += third_got[s][j].astype(F32)
        return total

    begin("u_first")
    for s in READY:
        sum_first(s)
    begin("v_second")
    for s in READY:
        sum_second(s)
    begin("w_third")
    small_wait(1)
    loss_v[...] = jnp.broadcast_to(jnp.sum(totals[:, :, 0:1]) / labelled_count, (1, 128))
    results = [logits_copy]

    def result(value, out, at):
        copy = pltpu.make_async_copy(value, out, w_sems.at[at])
        copy.start()
        results.append(copy)

    result(loss_v, loss, 14)
    for i, s in enumerate(READY):
        lane, row, rows_s, _ = STREAMS[s]
        total = sum_third(s)
        if lane < D:
            one_v[row : row + rows_s, lane : lane + 128] = total
        else:
            lane -= D
            size = min(128, C - lane)
            two_v[row : row + rows_s, lane : lane + size] = total[:, :size]
        if i == 3:
            result(two_v, grad_two, 15)
    result(one_v, grad_one, 16)
    for copy in results:
        copy.wait()
    begin(None)


def finish_body(a, b, c, d, a_out, b_out, c_out, d_out, b_row, sems):
    copies = [
        pltpu.make_async_copy(x, y, sems.at[i])
        for i, (x, y) in enumerate(((a, a_out), (b, b_row), (c, c_out), (d, d_out)))
    ]
    for copy in copies:
        copy.start()
    for copy in copies:
        copy.wait()
    b_out[...] = b_row[:, :1]


def sds(shape, dtype):
    return jax.ShapeDtypeStruct(shape, dtype)


def on_device(features, w_one, w_two, self_two, edge_src, edge_dst, send_rows, send_count, labels):
    vm = pl.BlockSpec(memory_space=pltpu.VMEM)
    hbm = pl.BlockSpec(memory_space=pl.ANY)
    V = pltpu.VMEM
    rows = [s[2] for s in STREAMS]
    scratch = [
        V((N, D), BF), V((REL, 2, N), I32), V((REL, 2, N), I32), V((SLOTS, PEERS), I32),
        V((1, PEERS), I32), V((1, N), I32),
        V((REL + 1, D, D), BF), V((REL, 352, D), BF), V((4, 32, REL, D), BF), V((2, 256, 128), F32),
        V((C, D), BF), V((REL, 2, N), I32), V((TABLE, 128), I32),
        V((REL, N, TABLE), BF), V((TABLE, REL * N), BF), V((REL, N, 128), F32),
        V((FAR, N), BF), V((N, FAR), BF),
        V((PEERS, SLOTS, D), BF), V((PEERS, SLOTS, D), BF), V((PEERS, SLOTS, D), BF),
        V((REL, N, D), F32), V((REL, N, D), BF), V(((REL + 1) * D, N), BF), V(((REL + 1) * D, N), BF),
        V((N, D), F32), V((N, D), BF), V((N, CP), F32), V((C, N), F32), V((1, 128), F32), V((ROWS, D), F32), V((ROWS, C), F32),
        V((N, D), F32),
        V((REL * N, D), BF),
        V((N, CP), BF), V((N, D), BF),
        V((2, 1, 128), F32), V((PEERS, 1, 128), F32), V((PEERS, 1, 128), F32),
        V((4, 4, 4, 2, ROWS, WIDE), BF), V((4, 4, 4, ROWS, WIDE), BF),
        *[V((3, 4, 4, r, 128), BF) for r in rows],
        *[V((4, 4, r, 128), BF) for r in rows],
        *[V((3, 4, r, 128), BF) for r in rows],
        *[V((4, r, 128), BF) for r in rows],
        *[V((3, r, 128), BF) for r in rows],
        pltpu.SemaphoreType.DMA((17,)),
        pltpu.SemaphoreType.DMA((3,)), pltpu.SemaphoreType.DMA((12,)),
        pltpu.SemaphoreType.DMA((2,)), pltpu.SemaphoreType.DMA((2,)),
        pltpu.SemaphoreType.DMA((8,)), pltpu.SemaphoreType.DMA((8,)),
        pltpu.SemaphoreType.DMA((108,)), pltpu.SemaphoreType.DMA((108,)),
    ]
    codes = np.concatenate(
        [np.arange(N)] + [N + SLOTS * code + np.arange(SLOTS) for code in ORDER]
    ).astype(np.int32)
    logits_t, loss, grad_one, grad_two = pl.pallas_call(
        step_body,
        name="step",
        in_specs=[hbm] * 10,
        out_specs=[hbm] * 4,
        out_shape=[sds((C, N), F32), sds((1, 128), F32), sds((ROWS, D), F32), sds((ROWS, C), F32)],
        scratch_shapes=scratch,
        compiler_params=pltpu.CompilerParams(
            collective_id=0, has_side_effects=True, vmem_limit_bytes=int(VLIM * MB)
        ),
    )(
        features, w_one, jnp.transpose(w_two, (2, 0, 1)), self_two.T, edge_src, edge_dst,
        send_rows[0].T, send_count, labels.reshape(1, N),
        jnp.asarray(np.repeat(codes[:, None], 128, axis=1)),
    )
    logits_t, loss, grad_one, grad_two = pl.pallas_call(
        finish_body,
        name="finish",
        in_specs=[hbm] * 4,
        out_specs=[vm] * 4,
        out_shape=[sds((C, N), F32), sds((1, 1), F32), sds((ROWS, D), F32), sds((ROWS, C), F32)],
        scratch_shapes=[V((1, 128), F32), pltpu.SemaphoreType.DMA((4,))],
        compiler_params=pltpu.CompilerParams(vmem_limit_bytes=63 * MB),
    )(logits_t, loss, grad_one, grad_two)
    return (logits_t.T, loss[0, 0], grad_one, grad_two)


def solution(mesh):
    split = Mesh(mesh.devices.reshape(SIZES), DOM)
    return jax.shard_map(
        on_device,
        mesh=split,
        in_specs=(
            P(DOM, None),
            P(),
            P(),
            P(),
            P(None, DOM, None),
            P(None, DOM, None),
            P(DOM, None, None),
            P(DOM, None),
            P(DOM),
        ),
        out_specs=(P(DOM, None), P(), P(DOM, None), P(DOM, None)),
        check_vma=False,
    )
```
